8 devices in a mesh: batch: 1 (over z), tp: 2 (over y), sp: 4 (over x, core).
Axes of the slice: x: 2, y: 2, z: 1, core: 2. Of those that a mesh axis runs over, the one named last changes fastest.
Arguments:
- tokens: bfloat16 [8192, 1024], P(('batch', 'sp'))
- glob_pos: int32 [512], P('batch')
- rel_bias: float32 [16, 513], P('tp')
- w_query: bfloat16 [1024, 1024], P(None, 'tp')
- w_key: bfloat16 [1024, 1024], P(None, 'tp')
- w_value: bfloat16 [1024, 1024], P(None, 'tp')
- w_query_glob: bfloat16 [1024, 1024], P(None, 'tp')
- w_out: bfloat16 [1024, 1024], P('tp')
- w_up: bfloat16 [1024, 4096], P(None, 'tp')
- w_down: bfloat16 [4096, 1024], P('tp')
Outputs:
- output: bfloat16 [8192, 1024], P(('batch', 'sp'))
All inputs are finite; a program needn't handle non-finite values.
Results may differ from the reference program's by a relative error of at most 0.0116037.
Values are sent between devices in bfloat16 or wider.
A program may use at most 1 GiB of HBM per device.

```python
import math
import jax
import jax.numpy as jnp
from jax import lax

MODEL_DIM = 1024
NUM_HEADS = 16
HIDDEN_DIM = 4096
WINDOW = 256
NUM_GLOBAL = 512
SEQ_LEN = 8192


def setup_inputs(seed: int = 0, part: int = 0) -> dict:
    part_keys = jax.random.split(jax.random.fold_in(jax.random.key(seed), part), 2)
    shared_keys = jax.random.split(jax.random.key(seed + 1), 9)
    in_scale = MODEL_DIM ** -0.5
    out_scale = ((2 * WINDOW + NUM_GLOBAL) / (3.0 * MODEL_DIM)) ** 0.5
    glob_scale = (math.log(6.0 * SEQ_LEN / (2 * WINDOW + NUM_GLOBAL)) / MODEL_DIM) ** 0.5

    def draw_normal(rand_key, arr_shape, std_dev):
        return (std_dev * jax.random.normal(rand_key, arr_shape, jnp.float32)).astype(jnp.bfloat16)

    square = (MODEL_DIM, MODEL_DIM)
    glob_pos = jnp.sort(jax.random.permutation(part_keys[1], SEQ_LEN)[:NUM_GLOBAL]).astype(jnp.int32)
    return {
        "tokens": draw_normal(part_keys[0], (SEQ_LEN, MODEL_DIM), 1.0),
        "glob_pos": glob_pos,
        "rel_bias": 0.7 * jax.random.normal(shared_keys[0], (NUM_HEADS, 2 * WINDOW + 1), jnp.float32),
        "w_query": draw_normal(shared_keys[1], square, in_scale),
        "w_key": draw_normal(shared_keys[2], square, in_scale),
        "w_value": draw_normal(shared_keys[3], square, in_scale),
        "w_query_glob": draw_normal(shared_keys[4], square, glob_scale),
        "w_out": draw_normal(shared_keys[5], square, out_scale),
        "w_up": draw_normal(shared_keys[6], (MODEL_DIM, HIDDEN_DIM), in_scale),
        "w_down": draw_normal(shared_keys[7], (HIDDEN_DIM, MODEL_DIM), HIDDEN_DIM ** -0.5),
    }


def reference(tokens, glob_pos, rel_bias, w_query, w_key, w_value, w_query_glob, w_out, w_up, w_down):
    head_dim = MODEL_DIM // NUM_HEADS
    score_scale = head_dim ** -0.5
    n_blocks = SEQ_LEN // WINDOW
    heads_shape = (SEQ_LEN, NUM_HEADS, head_dim)

    def project(weight):
        product = jnp.dot(tokens, weight, preferred_element_type=jnp.float32)
        return product.astype(jnp.bfloat16).astype(jnp.float32).reshape(heads_shape)

    queries = project(w_query)
    keys_all = project(w_key)
    values_all = project(w_value)
    zero_pad = jnp.zeros((WINDOW, NUM_HEADS, head_dim), jnp.float32)
    keys_ext = jnp.concatenate([zero_pad, keys_all, zero_pad], axis=0)
    values_ext = jnp.concatenate([zero_pad, values_all, zero_pad], axis=0)
    glob_keys = keys_all[glob_pos]
    glob_values = values_all[glob_pos]
    rel_offs = jnp.arange(3 * WINDOW)[None, :] - jnp.arange(WINDOW)[:, None]
    in_band = (rel_offs >= 0) & (rel_offs <= 2 * WINDOW)
    band_bias = jnp.take(rel_bias, jnp.clip(rel_offs, 0, 2 * WINDOW), axis=1)

    def window_block(blk_index):
        blk_start = blk_index * WINDOW
        q_blk = lax.dynamic_slice_in_dim(queries, blk_start, WINDOW, axis=0)
        k_win = lax.dynamic_slice_in_dim(keys_ext, blk_start, 3 * WINDOW, axis=0)
        v_win = lax.dynamic_slice_in_dim(values_ext, blk_start, 3 * WINDOW, axis=0)
        query_pos = blk_start + jnp.arange(WINDOW)
        key_pos = blk_start - WINDOW + jnp.arange(3 * WINDOW)
        key_ok = (key_pos >= 0) & (key_pos < SEQ_LEN)
        win_scores = jnp.einsum("qhd,khd->hqk", q_blk, k_win) * score_scale + band_bias
        win_scores = jnp.where(in_band & key_ok[None, :], win_scores, -jnp.inf)
        far_mask = jnp.abs(query_pos[:, None] - glob_pos[None, :]) > WINDOW
        glob_scores = jnp.einsum("qhd,ghd->hqg", q_blk, glob_keys) * score_scale
        glob_scores = jnp.where(far_mask, glob_scores, -jnp.inf)
        scores = jnp.concatenate([win_scores, glob_scores], axis=-1)
        attn_probs = jax.nn.softmax(scores, axis=-1).astype(jnp.bfloat16).astype(jnp.float32)
        all_values = jnp.concatenate([v_win, glob_values], axis=0)
        return jnp.einsum("hqk,khd->qhd", attn_probs, all_values)

    win_out = lax.map(window_block, jnp.arange(n_blocks)).reshape(heads_shape)
    x_glob = tokens[glob_pos]
    q_glob = jnp.dot(x_glob, w_query_glob, preferred_element_type=jnp.float32)
    q_glob = q_glob.astype(jnp.bfloat16).astype(jnp.float32).reshape(NUM_GLOBAL // 8, 8, NUM_HEADS, head_dim)

    def glob_block(q_group):
        scores = jnp.einsum("ghd,khd->hgk", q_group, keys_all) * score_scale
        attn_probs = jax.nn.softmax(scores, axis=-1).astype(jnp.bfloat16).astype(jnp.float32)
        return jnp.einsum("hgk,khd->ghd", attn_probs, values_all)

    glob_out = lax.map(glob_block, q_glob).reshape(NUM_GLOBAL, NUM_HEADS, head_dim)
    heads_out = win_out.at[glob_pos].set(glob_out)
    attn_vec = heads_out.reshape(SEQ_LEN, MODEL_DIM).astype(jnp.bfloat16)
    attn_proj = jnp.dot(attn_vec, w_out, preferred_element_type=jnp.float32)
    hidden = (tokens.astype(jnp.float32) + attn_proj).astype(jnp.bfloat16)
    up_proj = jnp.dot(hidden, w_up, preferred_element_type=jnp.float32)
    act_vals = jax.nn.gelu(up_proj).astype(jnp.bfloat16)
    down_proj = jnp.dot(act_vals, w_down, preferred_element_type=jnp.float32)
    return (hidden.astype(jnp.float32) + down_proj).astype(jnp.bfloat16)
```

```python
import functools

import jax
import jax.numpy as jnp
from jax import lax
from jax.experimental import pallas as pl
from jax.experimental.pallas import tpu as pltpu
from jax.sharding import PartitionSpec as P

BF = jnp.bfloat16
F32 = jnp.float32
NEG = float("-inf")
QB = 128


def const_spec(shape):
    return pl.BlockSpec(shape, lambda *_: (0,) * len(shape), pipeline_mode=pl.Buffered(1))


def pair_rhs(q_pair):
    half = lax.broadcasted_iota(jnp.int32, q_pair.shape, 0) < q_pair.shape[0] // 2
    zero = jnp.zeros_like(q_pair)
    return jnp.concatenate([jnp.where(half, q_pair, zero), jnp.where(half, zero, q_pair)], axis=1)


def unpair(o_two):
    n = o_two.shape[1] // 2
    half = lax.broadcasted_iota(jnp.int32, (o_two.shape[0], n), 0) < o_two.shape[0] // 2
    return jnp.where(half, o_two[:, :n], o_two[:, n:])


def window_kernel(base, n_win, info_ref, q_ref, k_ref, vt_ref, kg_ref, vgt_ref, br_ref, gpos_ref, o_ref, bias, gmask, score):
    j = pl.program_id(0)
    blk = j + base
    row_start = info_ref[0]
    seq_len = info_ref[1]
    n_pairs = q_ref.shape[0] // 128
    n_glob = kg_ref.shape[0]

    @pl.when(j == 0)
    def _():
        for head in range(2 * n_pairs):
            lanes = slice((head % 2) * QB, (head % 2 + 1) * QB)
            for c in range(n_win):
                hi = 128 * (n_win - c)
                g = jnp.concatenate([br_ref[head:head + 1, hi:hi + 128], br_ref[head:head + 1, hi - 128:hi]], axis=1)
                rolled = pltpu.roll(jnp.broadcast_to(g, (128, 256)), 0, 1, stride=1, stride_axis=0)
                bias[head // 2, c, :, lanes] = rolled[:, :QB]
            bias[head // 2, n_win, :, lanes] = jnp.full((128, QB), NEG, F32)

    q_start = row_start + blk * QB
    q_pos = q_start + lax.broadcasted_iota(jnp.int32, (n_glob, QB), 1)
    gmask[...] = jnp.where(jnp.abs(q_pos - gpos_ref[...]) > (n_win - 1) * 64, 0.0, NEG)

    slots = []
    for c in range(n_win):
        key_start = q_start - (n_win - 1) * 64 + 128 * c
        slots.append(jnp.where((key_start >= 0) & (key_start < seq_len), c, n_win))
    n_chunk = n_win + n_glob // 128
    for p in range(n_pairs):
        lanes = slice(128 * p, 128 * p + 128)
        buf = p % 2
        rhs = pair_rhs(q_ref[lanes, :])
        top = None
        for c in range(n_chunk):
            if c < n_win:
                keys = k_ref[pl.ds(pl.multiple_of(blk * QB + 128 * c, 128), 128), lanes]
                extra = bias[p, slots[c]]
            else:
                rows = slice(128 * (c - n_win), 128 * (c - n_win) + 128)
                keys = kg_ref[rows, lanes]
                extra = jnp.concatenate([gmask[rows, :], gmask[rows, :]], axis=1)
            s = jnp.dot(keys, rhs, preferred_element_type=F32) + extra
            score[buf, 128 * c:128 * c + 128, :] = s
            part = jnp.max(s.reshape(16, 8, 2 * QB), axis=0)
            top = part if top is None else jnp.maximum(top, part)
        top = jnp.max(top, axis=0, keepdims=True)
        total = None
        for c in range(n_chunk):
            rows = slice(128 * c, 128 * c + 128)
            e = jnp.exp(score[buf, rows, :] - top)
            score[buf, rows, :] = e
            part = jnp.sum(e.reshape(16, 8, 2 * QB), axis=0)
            total = part if total is None else total + part
        inv = 1.0 / jnp.sum(total, axis=0, keepdims=True)
        w_len = 128 * n_win
        pw = (score[buf, :w_len, :] * inv).astype(BF)
        pg = (score[buf, w_len:, :] * inv).astype(BF)
        vt = vt_ref[lanes, pl.ds(pl.multiple_of(blk * QB, 128), w_len)]
        o_two = jnp.dot(vt, pw, preferred_element_type=F32) + jnp.dot(vgt_ref[lanes, :], pg, preferred_element_type=F32)
        o_ref[:, lanes] = jnp.transpose(unpair(o_two)).astype(BF)


def glob_kernel(q_ref, k_ref, vt_ref, o_ref, m_ref, l_ref, score):
    rows = k_ref.shape[0]
    rhs = pair_rhs(q_ref[...])
    top = None
    for c in range(rows // 256):
        s = jnp.dot(k_ref[256 * c:256 * c + 256, :], rhs, preferred_element_type=F32)
        score[256 * c:256 * c + 256, :] = s
        part = jnp.max(s.reshape(32, 8, 2 * QB), axis=0)
        top = part if top is None else jnp.maximum(top, part)
    top = jnp.max(top, axis=0, keepdims=True)
    total = None
    acc = None
    for c in range(rows // 256):
        e = jnp.exp(score[256 * c:256 * c + 256, :] - top)
        part = jnp.sum(e.reshape(32, 8, 2 * QB), axis=0)
        total = part if total is None else total + part
        o = jnp.dot(vt_ref[:, 256 * c:256 * c + 256], e.astype(BF), preferred_element_type=F32)
        acc = o if acc is None else acc + o
    o_ref[...] = unpair(acc)
    m_ref[0] = jnp.broadcast_to(top, (8, 2 * QB))
    l_ref[0] = jnp.broadcast_to(jnp.sum(total, axis=0, keepdims=True), (8, 2 * QB))


def mlp_kernel(info_ref, x_ref, oa_ref, ob_ref, wo_ref, wu_ref, wd_ref, *refs):
    wo_p, wu_p, wd_p, out_ref = refs[0:4], refs[4:8], refs[8:12], refs[12]
    piece = wu_p[0].shape[1]
    acc = x_ref[...].astype(F32) + jnp.dot(oa_ref[...], wo_ref[...], preferred_element_type=F32)
    for k in range(4):
        depth = wo_p[k].shape[0]
        cols = pl.ds(pl.multiple_of(info_ref[2 + k] * depth, depth), depth)
        acc = acc + jnp.dot(ob_ref[:, cols], wo_p[k][...], preferred_element_type=F32)
    h = acc.astype(BF)
    acc = h.astype(F32)
    for k in range(8):
        cols = slice(piece * (k % 4), piece * (k % 4) + piece)
        up = wu_ref[:, cols] if k < 4 else wu_p[k - 4][...]
        down = wd_ref[cols, :] if k < 4 else wd_p[k - 4][...]
        act = jax.nn.gelu(jnp.dot(h, up, preferred_element_type=F32)).astype(BF)
        acc = acc + jnp.dot(act, down, preferred_element_type=F32)
    out_ref[...] = acc.astype(BF)


def solution(mesh):
    n_seq = mesh.shape["sp"]
    to_right = [(s, s + 1) for s in range(n_seq - 1)]
    to_left = [(s + 1, s) for s in range(n_seq - 1)]
    flip = {"tp": [(0, 1), (1, 0)], 1: [(s, s ^ 1) for s in range(n_seq)], 2: [(s, s ^ 2) for s in range(n_seq)]}

    def swap_tp(v):
        return lax.ppermute(v, "tp", flip["tp"])

    def swap_core(v):
        return lax.ppermute(v, "sp", flip[1])

    def swap_x(v):
        return lax.ppermute(v, "sp", flip[2])

    def local_layer(tokens, glob_pos, rel_bias, w_query, w_key, w_value, w_query_glob, w_out, w_up, w_down):
        rows, dim = tokens.shape
        heads, span = rel_bias.shape
        window = (span - 1) // 2
        loc = w_query.shape[1]
        head_dim = loc // heads
        n_glob = glob_pos.shape[0]
        n_pairs = loc // 128
        n_win = 2 * window // 128 + 1
        scale = head_dim ** -0.5
        rank = lax.axis_index("sp")
        core = rank % 2
        row_start = rank * rows
        vmem = 60 * 1024 * 1024

        def dot(a, b, dims):
            return lax.dot_general(a, b, (dims, ((), ())), preferred_element_type=F32)

        def quarters(w, axis):
            size = w.shape[axis] // n_seq
            mine = swap_tp(lax.dynamic_slice_in_dim(w, rank * size, size, axis))
            across = swap_x(mine)
            return [mine, across, swap_core(mine), swap_core(across)]

        wo_p = quarters(w_out, 0)
        wu_p = quarters(w_up, 1)
        wd_p = quarters(w_down, 0)

        slot = glob_pos - row_start
        pick = (slot[:, None] == jnp.arange(rows)[None, :]).astype(BF)
        x_glob = dot(pick, tokens, ((1,), (0,))).astype(BF)
        x_glob = x_glob + swap_core(x_glob)
        half = n_glob // 2
        x_half = lax.dynamic_slice_in_dim(x_glob, core * half, half, 0)
        x_half = x_half + swap_x(x_half)
        x_other = swap_core(x_half)
        first = core == 0
        x_glob = jnp.concatenate([jnp.where(first, x_half, x_other), jnp.where(first, x_other, x_half)], axis=0)

        q_t = dot(w_query, tokens, ((0,), (1,))).astype(BF) * BF(scale)
        k_loc = dot(tokens, w_key, ((1,), (0,))).astype(BF)
        v_t = dot(w_value, tokens, ((0,), (1,))).astype(BF)
        kg = dot(x_glob, w_key, ((1,), (0,))).astype(BF)
        vg_t = dot(w_value, x_glob, ((0,), (1,))).astype(BF)
        qg_t = dot(w_query_glob, x_glob, ((0,), (1,))).astype(BF) * BF(scale)

        k_ext = jnp.concatenate([
            lax.ppermute(k_loc[rows - window:], "sp", to_right), k_loc, lax.ppermute(k_loc[:window], "sp", to_left)], axis=0)
        v_ext = jnp.concatenate([
            lax.ppermute(v_t[:, rows - window:], "sp", to_right), v_t, lax.ppermute(v_t[:, :window], "sp", to_left)], axis=1)

        n_tiles = n_glob // QB
        part_o, part_m, part_l = pl.pallas_call(
            glob_kernel,
            name="glob_attn",
            grid=(n_pairs, n_tiles),
            in_specs=[
                pl.BlockSpec((128, QB), lambda p, t: (p, t)),
                pl.BlockSpec((rows, 128), lambda p, t: (0, p)),
                pl.BlockSpec((128, rows), lambda p, t: (p, 0)),
            ],
            out_specs=[
                pl.BlockSpec((128, QB), lambda p, t: (p, t)),
                pl.BlockSpec((1, 8, 2 * QB), lambda p, t: (p * n_tiles + t, 0, 0)),
                pl.BlockSpec((1, 8, 2 * QB), lambda p, t: (p * n_tiles + t, 0, 0)),
            ],
            out_shape=[
                jax.ShapeDtypeStruct((loc, n_glob), F32),
                jax.ShapeDtypeStruct((n_pairs * n_tiles, 8, 2 * QB), F32),
                jax.ShapeDtypeStruct((n_pairs * n_tiles, 8, 2 * QB), F32),
            ],
            scratch_shapes=[pltpu.VMEM((rows, 2 * QB), F32)],
            compiler_params=pltpu.CompilerParams(vmem_limit_bytes=vmem),
            cost_estimate=pl.CostEstimate(flops=16 * 10**9, bytes_accessed=8 * 2**20, transcendentals=heads * n_glob * rows),
        )(qg_t, k_loc, v_t)

        def stat(s):
            s = s[:, 0, :].reshape(n_pairs, n_tiles, 2, QB)
            return s.transpose(0, 2, 1, 3).reshape(heads, n_glob)

        stats = jnp.stack([stat(part_m), stat(part_l)])
        for swap in (swap_core, swap_x):
            o_far, s_far = swap(part_o), swap(stats)
            top = jnp.maximum(stats[0], s_far[0])
            mine, theirs = jnp.exp(stats[0] - top), jnp.exp(s_far[0] - top)
            stats = jnp.stack([top, stats[1] * mine + s_far[1] * theirs])
            shape = (heads, head_dim, n_glob)
            part_o = (part_o.reshape(shape) * mine[:, None] + o_far.reshape(shape) * theirs[:, None]).reshape(loc, n_glob)
        glob_o = (part_o.reshape(heads, head_dim, n_glob) / stats[1][:, None]).astype(BF).reshape(loc, n_glob)

        br = jnp.pad(rel_bias[:, ::-1], ((0, 0), (128, 127)), constant_values=NEG)
        info = jnp.stack([row_start, jnp.int32(rows * n_seq), rank, rank ^ 2, rank ^ 1, rank ^ 3]).astype(jnp.int32)
        n_ext = rows + 2 * window
        n_calls = 2
        blocks = rows // QB // n_calls
        is_glob = (slot[:, None] == jnp.arange(rows)[None, :]).any(axis=0)
        o_mine, o_peer = [], []
        for call in range(n_calls):
            base = call * blocks
            o_win = pl.pallas_call(
                functools.partial(window_kernel, base, n_win),
                name="window_attn",
                grid=(blocks,),
                in_specs=[
                    pl.BlockSpec(memory_space=pltpu.SMEM),
                    pl.BlockSpec((loc, QB), functools.partial(lambda b, j: (0, j + b), base)),
                    const_spec((n_ext, loc)),
                    const_spec((loc, n_ext)),
                    const_spec((n_glob, loc)),
                    const_spec((loc, n_glob)),
                    const_spec((heads, span + 255)),
                    const_spec((n_glob, 1)),
                ],
                out_specs=pl.BlockSpec((QB, loc), lambda j: (j, 0)),
                out_shape=jax.ShapeDtypeStruct((blocks * QB, loc), BF),
                scratch_shapes=[
                    pltpu.VMEM((n_pairs, n_win + 1, 128, 2 * QB), F32),
                    pltpu.VMEM((n_glob, QB), F32),
                    pltpu.VMEM((2, n_win * 128 + n_glob, 2 * QB), F32),
                ],
                compiler_params=pltpu.CompilerParams(vmem_limit_bytes=vmem),
                cost_estimate=pl.CostEstimate(flops=16 * 10**9, bytes_accessed=8 * 2**20, transcendentals=heads * n_glob * rows),
            )(info, q_t, k_ext, v_ext, kg, vg_t, br, glob_pos[:, None])
            part = slice(base * QB, (base + blocks) * QB)
            glob_rows = dot(pick[:, part], glob_o, ((0,), (1,))).astype(BF)
            o_fix = jnp.where(is_glob[part, None], glob_rows, o_win)
            o_mine.append(o_fix)
            o_peer.append(swap_tp(o_fix))
        oa = jnp.concatenate(o_mine, axis=0)
        ob = jnp.concatenate(o_peer, axis=0)

        mb = 256
        hid = w_up.shape[1]
        piece = hid // n_seq
        return pl.pallas_call(
            mlp_kernel,
            name="mlp",
            grid=(rows // mb,),
            in_specs=[
                pl.BlockSpec(memory_space=pltpu.SMEM),
                pl.BlockSpec((mb, dim), lambda j: (j, 0)),
                pl.BlockSpec((mb, loc), lambda j: (j, 0)),
                pl.BlockSpec((mb, loc), lambda j: (j, 0)),
                const_spec((loc, dim)),
                const_spec((dim, hid)),
                const_spec((hid, dim)),
                *[const_spec((loc // n_seq, dim))] * 4,
                *[const_spec((dim, piece))] * 4,
                *[const_spec((piece, dim))] * 4,
            ],
            out_specs=pl.BlockSpec((mb, dim), lambda j: (j, 0)),
            out_shape=jax.ShapeDtypeStruct((rows, dim), BF),
            compiler_params=pltpu.CompilerParams(vmem_limit_bytes=vmem),
            cost_estimate=pl.CostEstimate(flops=38 * 10**9, bytes_accessed=30 * 2**20, transcendentals=rows * hid * 2),
        )(info, tokens, oa, ob, w_out, w_up, w_down, *wo_p, *wu_p, *wd_p)

    row_spec = P(("batch", "sp"), None)
    col_spec = P(None, "tp")
    head_spec = P("tp", None)
    in_specs = (row_spec, P("batch"), head_spec, col_spec, col_spec, col_spec, col_spec, head_spec, col_spec, head_spec)
    return jax.shard_map(local_layer, mesh=mesh, in_specs=in_specs, out_specs=row_spec, check_vma=False)
```

```python
import functools

import jax
import jax.numpy as jnp
from jax import lax
from jax.experimental import pallas as pl
from jax.experimental.pallas import tpu as pltpu
from jax.sharding import PartitionSpec as P

BF = jnp.bfloat16
F32 = jnp.float32
NEG = float("-inf")
QB = 128
MESH = pl.DeviceIdType.MESH


def const_spec(shape):
    return pl.BlockSpec(shape, lambda *_: (0,) * len(shape), pipeline_mode=pl.Buffered(1))


def pair_rhs(q_pair):
    half = lax.broadcasted_iota(jnp.int32, q_pair.shape, 0) < q_pair.shape[0] // 2
    zero = jnp.zeros_like(q_pair)
    return jnp.concatenate([jnp.where(half, q_pair, zero), jnp.where(half, zero, q_pair)], axis=1)


def unpair(o_two):
    n = o_two.shape[1] // 2
    half = lax.broadcasted_iota(jnp.int32, (o_two.shape[0], n), 0) < o_two.shape[0] // 2
    return jnp.where(half, o_two[:, :n], o_two[:, n:])


def window_kernel(base, n_win, info_ref, q_ref, k_ref, vt_ref, kg_ref, vgt_ref, br_ref, gpos_ref, o_ref, bias, gmask, score):
    j = pl.program_id(0)
    blk = j + base
    row_start = info_ref[0]
    seq_len = info_ref[1]
    n_pairs = q_ref.shape[0] // 128
    n_glob = kg_ref.shape[0]

    @pl.when(j == 0)
    def _():
        for head in range(2 * n_pairs):
            lanes = slice((head % 2) * QB, (head % 2 + 1) * QB)
            for c in range(n_win):
                hi = 128 * (n_win - c)
                g = jnp.concatenate([br_ref[head:head + 1, hi:hi + 128], br_ref[head:head + 1, hi - 128:hi]], axis=1)
                rolled = pltpu.roll(jnp.broadcast_to(g, (128, 256)), 0, 1, stride=1, stride_axis=0)
                bias[head // 2, c, :, lanes] = rolled[:, :QB]
            bias[head // 2, n_win, :, lanes] = jnp.full((128, QB), NEG, F32)

    q_start = row_start + blk * QB
    q_pos = q_start + lax.broadcasted_iota(jnp.int32, (n_glob, QB), 1)
    gmask[...] = jnp.where(jnp.abs(q_pos - gpos_ref[...]) > (n_win - 1) * 64, 0.0, NEG)

    slots = []
    for c in range(n_win):
        key_start = q_start - (n_win - 1) * 64 + 128 * c
        slots.append(jnp.where((key_start >= 0) & (key_start < seq_len), c, n_win))
    n_chunk = n_win + n_glob // 128
    for p in range(n_pairs):
        lanes = slice(128 * p, 128 * p + 128)
        buf = p % 2
        rhs = pair_rhs(q_ref[lanes, :])
        top = None
        for c in range(n_chunk):
            if c < n_win:
                keys = k_ref[pl.ds(pl.multiple_of(blk * QB + 128 * c, 128), 128), lanes]
                extra = bias[p, slots[c]]
            else:
                rows = slice(128 * (c - n_win), 128 * (c - n_win) + 128)
                keys = kg_ref[rows, lanes]
                extra = jnp.concatenate([gmask[rows, :], gmask[rows, :]], axis=1)
            s = jnp.dot(keys, rhs, preferred_element_type=F32) + extra
            score[buf, 128 * c:128 * c + 128, :] = s
            part = jnp.max(s.reshape(16, 8, 2 * QB), axis=0)
            top = part if top is None else jnp.maximum(top, part)
        top = jnp.max(top, axis=0, keepdims=True)
        total = None
        for c in range(n_chunk):
            rows = slice(128 * c, 128 * c + 128)
            e = jnp.exp(score[buf, rows, :] - top)
            score[buf, rows, :] = e
            part = jnp.sum(e.reshape(16, 8, 2 * QB), axis=0)
            total = part if total is None else total + part
        inv = 1.0 / jnp.sum(total, axis=0, keepdims=True)
        w_len = 128 * n_win
        pw = (score[buf, :w_len, :] * inv).astype(BF)
        pg = (score[buf, w_len:, :] * inv).astype(BF)
        vt = vt_ref[lanes, pl.ds(pl.multiple_of(blk * QB, 128), w_len)]
        o_two = jnp.dot(vt, pw, preferred_element_type=F32) + jnp.dot(vgt_ref[lanes, :], pg, preferred_element_type=F32)
        o_ref[:, lanes] = jnp.transpose(unpair(o_two)).astype(BF)


def front_kernel(n_seq, scale, x_ref, gpos_ref, wq_ref, wk_ref, wv_ref, wqg_ref, qt_ref, k_ref, vt_ref, kg_ref, vgt_ref, qgt_ref,
                 x_send, x_half, x_in, x_in2, xg, send_sem, recv_sem):
    rank = lax.axis_index("sp")
    core = lax.rem(rank, 2)
    mate = rank + 1 - 2 * core
    across = lax.rem(rank + 2, n_seq)
    rows, dim = x_ref.shape
    half = gpos_ref.shape[0] // 2
    halo = (k_ref.shape[0] - rows) // 2

    barrier = pltpu.get_barrier_semaphore()
    for step in range(1, n_seq):
        pl.semaphore_signal(barrier, inc=1, device_id={"sp": lax.rem(rank + step, n_seq)}, device_id_type=MESH)
    pl.semaphore_wait(barrier, n_seq - 1)

    def copy(src, dst, idx, dev):
        return pltpu.make_async_remote_copy(
            src_ref=src, dst_ref=dst, send_sem=send_sem.at[idx], recv_sem=recv_sem.at[idx],
            device_id={"sp": dev}, device_id_type=MESH)

    def dot(a, b, dims):
        return lax.dot_general(a, b, (dims, ((), ())), preferred_element_type=F32)

    def picked(which):
        slots = gpos_ref[pl.ds(pl.multiple_of(which * half, half), half), :] - rank * rows
        acc = None
        for c in range(rows // 512):
            at = lax.broadcasted_iota(jnp.int32, (half, 512), 1) + 512 * c
            hot = jnp.where(slots == at, 1.0, 0.0).astype(BF)
            part = dot(hot, x_ref[512 * c:512 * c + 512, :], ((1,), (0,)))
            acc = part if acc is None else acc + part
        return acc.astype(BF)

    x_send[...] = picked(1 - core)
    first = copy(x_send, x_in, 0, mate)
    mine = picked(core)
    x_half[...] = mine
    first.start()

    def keys(c):
        at = pl.ds(pl.multiple_of(c * 256, 256), 256)
        k_ref[pl.ds(pl.multiple_of(halo + c * 256, 256), 256), :] = dot(x_ref[at, :], wk_ref[...], ((1,), (0,))).astype(BF)

    def values(c):
        at = pl.ds(pl.multiple_of(c * 256, 256), 256)
        vt_ref[:, pl.ds(pl.multiple_of(halo + c * 256, 256), 256)] = dot(wv_ref[...], x_ref[at, :], ((0,), (1,))).astype(BF)

    def queries(c):
        at = pl.ds(pl.multiple_of(c * 256, 256), 256)
        qt_ref[:, at] = dot(wq_ref[...], x_ref[at, :], ((0,), (1,))).astype(BF) * BF(scale)

    n_blk = rows // 256
    keys(0)
    keys(n_blk - 1)
    first.wait()
    x_half[...] = x_half[...] + x_in[...]
    values(0)
    second = copy(x_half, x_in2, 1, across)
    second.start()
    values(n_blk - 1)
    to_right = [
        copy(k_ref.at[pl.ds(rows, halo), :], k_ref.at[pl.ds(0, halo), :], 2, rank + 1),
        copy(vt_ref.at[:, pl.ds(rows, halo)], vt_ref.at[:, pl.ds(0, halo)], 3, rank + 1)]
    to_left = [
        copy(k_ref.at[pl.ds(halo, halo), :], k_ref.at[pl.ds(halo + rows, halo), :], 4, rank - 1),
        copy(vt_ref.at[:, pl.ds(halo, halo)], vt_ref.at[:, pl.ds(halo + rows, halo)], 5, rank - 1)]

    def later(c, carry):
        keys(c)
        values(c)
        return carry

    @pl.when(rank < n_seq - 1)
    def _():
        for c in to_right:
            c.start()

    @pl.when(rank > 0)
    def _():
        for c in to_left:
            c.start()

    lax.fori_loop(1, n_blk - 1, later, 0)
    lax.fori_loop(0, n_blk, lambda c, carry: (queries(c), carry)[1], 0)

    second.wait()
    own = pl.ds(pl.multiple_of(core * half, half), half)
    other = pl.ds(pl.multiple_of((1 - core) * half, half), half)
    xg[own, :] = x_half[...] + x_in2[...]

    def project(at):
        kg_ref[at, :] = dot(xg[at, :], wk_ref[...], ((1,), (0,))).astype(BF)
        vgt_ref[:, at] = dot(wv_ref[...], xg[at, :], ((0,), (1,))).astype(BF)

    def project_query(at):
        qgt_ref[:, at] = dot(wqg_ref[...], xg[at, :], ((0,), (1,))).astype(BF) * BF(scale)

    third = copy(xg.at[own, :], xg.at[own, :], 6, mate)
    project_query(own)
    third.start()
    project(own)
    third.wait()
    project_query(other)
    project(other)

    @pl.when(rank < n_seq - 1)
    def _():
        for c in to_right:
            c.wait_send()
        for c in to_left:
            c.wait_recv()

    @pl.when(rank > 0)
    def _():
        for c in to_left:
            c.wait_send()
        for c in to_right:
            c.wait_recv()

    @pl.when(rank == 0)
    def _():
        k_ref[0:halo, :] = jnp.zeros((halo, k_ref.shape[1]), BF)
        vt_ref[:, 0:halo] = jnp.zeros((vt_ref.shape[0], halo), BF)

    @pl.when(rank == n_seq - 1)
    def _():
        k_ref[halo + rows:, :] = jnp.zeros((halo, k_ref.shape[1]), BF)
        vt_ref[:, halo + rows:] = jnp.zeros((vt_ref.shape[0], halo), BF)


def glob_kernel(halo, q_ref, k_ref, vt_ref, o_ref, m_ref, l_ref, score):
    rows = k_ref.shape[0] - 2 * halo
    rhs = pair_rhs(q_ref[...])
    top = None
    for c in range(rows // 256):
        s = jnp.dot(k_ref[halo + 256 * c:halo + 256 * c + 256, :], rhs, preferred_element_type=F32)
        score[256 * c:256 * c + 256, :] = s
        part = jnp.max(s.reshape(32, 8, 2 * QB), axis=0)
        top = part if top is None else jnp.maximum(top, part)
    top = jnp.max(top, axis=0, keepdims=True)
    total = None
    acc = None
    for c in range(rows // 256):
        e = jnp.exp(score[256 * c:256 * c + 256, :] - top)
        part = jnp.sum(e.reshape(32, 8, 2 * QB), axis=0)
        total = part if total is None else total + part
        o = jnp.dot(vt_ref[:, halo + 256 * c:halo + 256 * c + 256], e.astype(BF), preferred_element_type=F32)
        acc = o if acc is None else acc + o
    o_ref[...] = unpair(acc)
    m_ref[0] = jnp.broadcast_to(top, (8, 2 * QB))
    l_ref[0] = jnp.broadcast_to(jnp.sum(total, axis=0, keepdims=True), (8, 2 * QB))


def mlp_kernel(info_ref, x_ref, oa_ref, ob_ref, wo_hbm, wu_hbm, wd_hbm, p0, p1, p2, p3, out_ref, wo, wu, wd, pk, sem):
    packs = (p0, p1, p2, p3)
    first = pl.program_id(0) == 0
    dim = wu.shape[0]
    piece = pk.shape[2]
    n_col = dim // piece
    depth = wo.shape[0] // 4
    head = dim + piece * n_col

    def part(src, dst, idx):
        return pltpu.make_async_copy(src, dst, sem.at[idx])

    loads = {"wo": part(wo_hbm, wo, 0)}
    for k in range(4):
        cols = pl.ds(k * piece, piece)
        loads["po", k] = part(packs[k].at[pl.ds(head, depth * n_col), :], pk.at[k, pl.ds(head, depth * n_col), :], 1 + k)
        loads["u", k] = part(wu_hbm.at[:, cols], wu.at[:, cols], 5 + k)
        loads["d", k] = part(wd_hbm.at[cols, :], wd.at[cols, :], 9 + k)
        loads["p", k] = part(packs[k].at[pl.ds(0, head), :], pk.at[k, pl.ds(0, head), :], 13 + k)

    @pl.when(first)
    def _():
        for c in loads.values():
            c.start()

    def ready(*key):
        @pl.when(first)
        def _():
            for k in key:
                loads[k].wait()

    ready("wo", ("po", 0), ("po", 1), ("po", 2), ("po", 3))
    acc = x_ref[...].astype(F32) + jnp.dot(oa_ref[...], wo[...], preferred_element_type=F32)
    extra = [None] * n_col
    for k in range(4):
        o = ob_ref[:, pl.ds(pl.multiple_of(info_ref[2 + k] * depth, depth), depth)]
        for c in range(n_col):
            t = jnp.dot(o, pk[k, head + c * depth:head + (c + 1) * depth, :], preferred_element_type=F32)
            extra[c] = t if extra[c] is None else extra[c] + t
    h = (acc + jnp.concatenate(extra, axis=1)).astype(BF)
    acc = h.astype(F32)
    for k in range(8):
        if k < 4:
            ready(("u", k), ("d", k))
            up = wu[:, k * piece:(k + 1) * piece]
        else:
            ready(("p", k - 4))
            up = pk[k - 4, :dim, :]
        act = jax.nn.gelu(jnp.dot(h, up, preferred_element_type=F32)).astype(BF)
        if k < 4:
            acc = acc + jnp.dot(act, wd[k * piece:(k + 1) * piece, :], preferred_element_type=F32)
        else:
            parts = [jnp.dot(act, pk[k - 4, dim + c * piece:dim + (c + 1) * piece, :], preferred_element_type=F32) for c in range(n_col)]
            acc = acc + jnp.concatenate(parts, axis=1)
    out_ref[...] = acc.astype(BF)


def solution(mesh):
    n_seq = mesh.shape["sp"]
    flip = {"tp": [(0, 1), (1, 0)], 1: [(s, s ^ 1) for s in range(n_seq)], 2: [(s, s ^ 2) for s in range(n_seq)]}

    def swap_tp(v):
        return lax.ppermute(v, "tp", flip["tp"])

    def swap_core(v):
        return lax.ppermute(v, "sp", flip[1])

    def swap_x(v):
        return lax.ppermute(v, "sp", flip[2])

    def local_layer(tokens, glob_pos, rel_bias, w_query, w_key, w_value, w_query_glob, w_out, w_up, w_down):
        rows, dim = tokens.shape
        heads, span = rel_bias.shape
        window = (span - 1) // 2
        loc = w_query.shape[1]
        head_dim = loc // heads
        n_glob = glob_pos.shape[0]
        n_pairs = loc // 128
        n_win = 2 * window // 128 + 1
        scale = head_dim ** -0.5
        rank = lax.axis_index("sp")
        row_start = rank * rows
        vmem = 60 * 1024 * 1024

        def dot(a, b, dims):
            return lax.dot_general(a, b, (dims, ((), ())), preferred_element_type=F32)

        def quarter(w, axis):
            size = w.shape[axis] // n_seq
            return lax.dynamic_slice_in_dim(w, rank * size, size, axis)

        piece = w_up.shape[1] // n_seq
        pack = [quarter(w_up, 1)]
        for w in (quarter(w_down, 0), quarter(w_out, 0)):
            pack += [w[:, c * piece:(c + 1) * piece] for c in range(dim // piece)]
        mine = swap_tp(jnp.concatenate(pack, axis=0))
        far = swap_x(mine)
        packs = [mine, far, swap_core(mine), swap_core(far)]

        slot = glob_pos - row_start
        pick = (slot[:, None] == jnp.arange(rows)[None, :]).astype(BF)
        n_ext = rows + 2 * window
        half = n_glob // 2
        vm = pl.BlockSpec(memory_space=pltpu.VMEM)
        q_t, k_ext, v_ext, kg, vg_t, qg_t = pl.pallas_call(
            functools.partial(front_kernel, n_seq, scale),
            name="front",
            in_specs=[vm] * 6,
            out_specs=[vm] * 6,
            out_shape=[jax.ShapeDtypeStruct(sh, BF) for sh in (
                (loc, rows), (n_ext, loc), (loc, n_ext), (n_glob, loc), (loc, n_glob), (loc, n_glob))],
            scratch_shapes=[
                pltpu.VMEM((half, dim), BF), pltpu.VMEM((half, dim), BF), pltpu.VMEM((half, dim), BF),
                pltpu.VMEM((half, dim), BF), pltpu.VMEM((n_glob, dim), BF),
                pltpu.SemaphoreType.DMA((7,)), pltpu.SemaphoreType.DMA((7,))],
            compiler_params=pltpu.CompilerParams(vmem_limit_bytes=vmem, collective_id=0, has_side_effects=True),
            cost_estimate=pl.CostEstimate(flops=16 * 10**9, bytes_accessed=16 * 2**20, transcendentals=0),
        )(tokens, glob_pos[:, None], w_query, w_key, w_value, w_query_glob)

        n_tiles = n_glob // QB
        part_o, part_m, part_l = pl.pallas_call(
            functools.partial(glob_kernel, window),
            name="glob_attn",
            grid=(n_pairs, n_tiles),
            in_specs=[
                pl.BlockSpec((128, QB), lambda p, t: (p, t)),
                pl.BlockSpec((n_ext, 128), lambda p, t: (0, p)),
                pl.BlockSpec((128, n_ext), lambda p, t: (p, 0)),
            ],
            out_specs=[
                pl.BlockSpec((128, QB), lambda p, t: (p, t)),
                pl.BlockSpec((1, 8, 2 * QB), lambda p, t: (p * n_tiles + t, 0, 0)),
                pl.BlockSpec((1, 8, 2 * QB), lambda p, t: (p * n_tiles + t, 0, 0)),
            ],
            out_shape=[
                jax.ShapeDtypeStruct((loc, n_glob), F32),
                jax.ShapeDtypeStruct((n_pairs * n_tiles, 8, 2 * QB), F32),
                jax.ShapeDtypeStruct((n_pairs * n_tiles, 8, 2 * QB), F32),
            ],
            scratch_shapes=[pltpu.VMEM((rows, 2 * QB), F32)],
            compiler_params=pltpu.CompilerParams(vmem_limit_bytes=vmem),
            cost_estimate=pl.CostEstimate(flops=16 * 10**9, bytes_accessed=8 * 2**20, transcendentals=heads * n_glob * rows),
        )(qg_t, k_ext, v_ext)

        def stat(s):
            s = s[:, 0, :].reshape(n_pairs, n_tiles, 2, QB)
            return s.transpose(0, 2, 1, 3).reshape(heads, n_glob)

        shape = (heads, head_dim, n_glob)
        m_all, l_all = stat(part_m), stat(part_l)
        for swap in (swap_core, swap_x):
            far = swap(jnp.concatenate([part_o, m_all, l_all], axis=0))
            m_far = far[loc:loc + heads]
            top = jnp.maximum(m_all, m_far)
            mine, theirs = jnp.exp(m_all - top), jnp.exp(m_far - top)
            m_all, l_all = top, l_all * mine + far[loc + heads:] * theirs
            part_o = (part_o.reshape(shape) * mine[:, None] + far[:loc].reshape(shape) * theirs[:, None]).reshape(loc, n_glob)
        glob_o = (part_o.reshape(shape) / l_all[:, None]).astype(BF).reshape(loc, n_glob)

        br = jnp.pad(rel_bias[:, ::-1], ((0, 0), (128, 127)), constant_values=NEG)
        info = jnp.stack([row_start, jnp.int32(rows * n_seq), rank, rank ^ 2, rank ^ 1, rank ^ 3]).astype(jnp.int32)
        n_calls = 2
        blocks = rows // QB // n_calls
        is_glob = (slot[:, None] == jnp.arange(rows)[None, :]).any(axis=0)
        o_mine, o_peer = [], []
        for call in range(n_calls):
            base = call * blocks
            o_win = pl.pallas_call(
                functools.partial(window_kernel, base, n_win),
                name="window_attn",
                grid=(blocks,),
                in_specs=[
                    pl.BlockSpec(memory_space=pltpu.SMEM),
                    pl.BlockSpec((loc, QB), functools.partial(lambda b, j: (0, j + b), base)),
                    const_spec((n_ext, loc)),
                    const_spec((loc, n_ext)),
                    const_spec((n_glob, loc)),
                    const_spec((loc, n_glob)),
                    const_spec((heads, span + 255)),
                    const_spec((n_glob, 1)),
                ],
                out_specs=pl.BlockSpec((QB, loc), lambda j: (j, 0)),
                out_shape=jax.ShapeDtypeStruct((blocks * QB, loc), BF),
                scratch_shapes=[
                    pltpu.VMEM((n_pairs, n_win + 1, 128, 2 * QB), F32),
                    pltpu.VMEM((n_glob, QB), F32),
                    pltpu.VMEM((2, n_win * 128 + n_glob, 2 * QB), F32),
                ],
                compiler_params=pltpu.CompilerParams(vmem_limit_bytes=vmem),
                cost_estimate=pl.CostEstimate(flops=16 * 10**9, bytes_accessed=8 * 2**20, transcendentals=heads * n_glob * rows),
            )(info, q_t, k_ext, v_ext, kg, vg_t, br, glob_pos[:, None])
            part = slice(base * QB, (base + blocks) * QB)
            glob_rows = dot(pick[:, part], glob_o, ((0,), (1,))).astype(BF)
            o_fix = jnp.where(is_glob[part, None], glob_rows, o_win)
            o_mine.append(o_fix)
            o_peer.append(swap_tp(o_fix))
        oa = jnp.concatenate(o_mine, axis=0)
        ob = jnp.concatenate(o_peer, axis=0)

        mb = 256
        hid = w_up.shape[1]
        return pl.pallas_call(
            mlp_kernel,
            name="mlp",
            grid=(rows // mb,),
            in_specs=[
                pl.BlockSpec(memory_space=pltpu.SMEM),
                pl.BlockSpec((mb, dim), lambda j: (j, 0)),
                pl.BlockSpec((mb, loc), lambda j: (j, 0)),
                pl.BlockSpec((mb, loc), lambda j: (j, 0)),
                *[pl.BlockSpec(memory_space=pl.ANY)] * 7,
            ],
            out_specs=pl.BlockSpec((mb, dim), lambda j: (j, 0)),
            out_shape=jax.ShapeDtypeStruct((rows, dim), BF),
            scratch_shapes=[
                pltpu.VMEM((loc, dim), BF), pltpu.VMEM((dim, hid), BF), pltpu.VMEM((hid, dim), BF),
                pltpu.VMEM((4,) + packs[0].shape, BF), pltpu.SemaphoreType.DMA((17,))],
            compiler_params=pltpu.CompilerParams(vmem_limit_bytes=vmem),
            cost_estimate=pl.CostEstimate(flops=38 * 10**9, bytes_accessed=30 * 2**20, transcendentals=rows * hid * 2),
        )(info, tokens, oa, ob, w_out, w_up, w_down, *packs)

    row_spec = P(("batch", "sp"), None)
    col_spec = P(None, "tp")
    head_spec = P("tp", None)
    in_specs = (row_spec, P("batch"), head_spec, col_spec, col_spec, col_spec, col_spec, head_spec, col_spec, head_spec)
    return jax.shard_map(local_layer, mesh=mesh, in_specs=in_specs, out_specs=row_spec, check_vma=False)
```

```python
import functools

import jax
import jax.numpy as jnp
from jax import lax
from jax.experimental import pallas as pl
from jax.experimental.pallas import tpu as pltpu
from jax.sharding import PartitionSpec as P

BF = jnp.bfloat16
F32 = jnp.float32
NEG = float("-inf")
QB = 128
MESH = pl.DeviceIdType.MESH


def dot(a, b, dims=((1,), (0,))):
    return lax.dot_general(a, b, (dims, ((), ())), preferred_element_type=F32)


def span(start, size):
    return pl.ds(pl.multiple_of(start, size), size)


def pair_rhs(q_pair):
    half = lax.broadcasted_iota(jnp.int32, q_pair.shape, 0) < q_pair.shape[0] // 2
    zero = jnp.zeros_like(q_pair)
    return jnp.concatenate([jnp.where(half, q_pair, zero), jnp.where(half, zero, q_pair)], axis=1)


def unpair(o_two):
    n = o_two.shape[1] // 2
    half = lax.broadcasted_iota(jnp.int32, (o_two.shape[0], n), 0) < o_two.shape[0] // 2
    return jnp.where(half, o_two[:, :n], o_two[:, n:])


def spread(stat):
    n = stat.shape[1] // 2
    return jnp.concatenate([jnp.broadcast_to(stat[0:1, :n], (64, n)), jnp.broadcast_to(stat[0:1, n:], (64, n))], axis=0)


def layer_kernel(n_seq, scale, halo, x_hbm, gcol, grow, br, wq_hbm, wk_hbm, wv_hbm, wqg_hbm, wo_hbm, wu_hbm, wd_hbm, out_hbm,
                 x, w4, wo, wu, wd, po, pu, pd, qt, kx, vx, kg, vgt, qgt, x_send, x_half, x_in, x_in2, xg,
                 go, gm, gl, in_o, in_m, in_l, gfin, bias, gmask, score, gscore, o_mine, o_peer, out_s,
                 send_sem, recv_sem, load_sem):
    rank = lax.axis_index("sp")
    peer = 1 - lax.axis_index("tp")
    core = lax.rem(rank, 2)
    mate = rank + 1 - 2 * core
    across = lax.rem(rank + 2, n_seq)
    rows, dim = x.shape
    n_glob = gcol.shape[0]
    n_pairs = qt.shape[0] // 128
    loc = qt.shape[0]
    half = n_glob // 2
    row_start = rank * rows
    n_win = 2 * halo // 128 + 1
    hid = wu.shape[1]
    piece = hid // n_seq
    depth = loc // n_seq

    loads = {}

    def load(key, src, dst):
        loads[key] = pltpu.make_async_copy(src, dst, load_sem.at[len(loads)])
        loads[key].start()

    for c in range(4):
        at = slice(512 * c, 512 * c + 512)
        load(("x", c), x_hbm.at[at, :], x.at[at, :])
    for c, w in enumerate((wk_hbm, wv_hbm, wq_hbm, wqg_hbm)):
        load(("w", c), w, w4.at[c])
    load("wo", wo_hbm, wo)
    load("wu", wu_hbm, wu)
    load("wd", wd_hbm, wd)
    wk, wv, wq, wqg = (w4.at[c] for c in range(4))

    barrier = pltpu.get_barrier_semaphore()
    for step in range(1, n_seq):
        pl.semaphore_signal(barrier, inc=1, device_id={"sp": lax.rem(rank + step, n_seq)}, device_id_type=MESH)
    pl.semaphore_signal(barrier, inc=1, device_id={"tp": peer}, device_id_type=MESH)
    pl.semaphore_wait(barrier, n_seq)

    used = [0]

    def copy(src, dst, sp=None):
        idx = used[0]
        used[0] += 1
        return pltpu.make_async_remote_copy(
            src_ref=src, dst_ref=dst, send_sem=send_sem.at[idx], recv_sem=recv_sem.at[idx],
            device_id={"tp": peer} if sp is None else {"sp": sp}, device_id_type=MESH)

    src_quarter = {
        "o": wo_hbm.at[span(rank * depth, depth), :],
        "u": wu_hbm.at[:, span(rank * piece, piece)],
        "d": wd_hbm.at[span(rank * piece, piece), :]}
    held = {"o": po, "u": pu, "d": pd}
    over_tp = {k: copy(src_quarter[k], held[k].at[0]) for k in held}
    over_x = {k: copy(held[k].at[0], held[k].at[1], across) for k in held}
    over_d = {k: copy(held[k].at[0], held[k].at[2], mate) for k in held}
    over_d2 = {k: copy(held[k].at[1], held[k].at[3], mate) for k in held}
    for k in ("o", "u", "d"):
        over_tp[k].start()

    def relay(k):
        over_tp[k].wait()
        over_x[k].start()
        over_d[k].start()

    def relay2(k):
        over_x[k].wait()
        over_d2[k].start()

    def picked(which):
        slots = gcol[span(which * half, half), :] - row_start
        acc = None
        for c in range(rows // 512):
            at = lax.broadcasted_iota(jnp.int32, (half, 512), 1) + 512 * c
            hot = jnp.where(slots == at, 1.0, 0.0).astype(BF)
            part = dot(hot, x[512 * c:512 * c + 512, :])
            acc = part if acc is None else acc + part
        return acc.astype(BF)

    for c in range(4):
        loads["x", c].wait()
    x_send[...] = picked(1 - core)
    first = copy(x_send, x_in, mate)
    x_half[...] = picked(core)
    first.start()

    def keys(c):
        kx[span(halo + c * 256, 256), :] = dot(x[span(c * 256, 256), :], wk[...]).astype(BF)

    def values(c):
        vx[:, span(halo + c * 256, 256)] = dot(wv[...], x[span(c * 256, 256), :], ((0,), (1,))).astype(BF)

    def queries(c):
        qt[:, span(c * 256, 256)] = dot(wq[...], x[span(c * 256, 256), :], ((0,), (1,))).astype(BF) * BF(scale)

    n_blk = rows // 256
    for c in range(4):
        loads["w", c].wait()
    keys(0)
    keys(n_blk - 1)
    first.wait()
    x_half[...] = x_half[...] + x_in[...]
    values(0)
    second = copy(x_half, x_in2, across)
    second.start()
    values(n_blk - 1)
    to_right = [
        copy(kx.at[pl.ds(rows, halo), :], kx.at[pl.ds(0, halo), :], rank + 1),
        copy(vx.at[:, pl.ds(rows, halo)], vx.at[:, pl.ds(0, halo)], rank + 1)]
    to_left = [
        copy(kx.at[pl.ds(halo, halo), :], kx.at[pl.ds(halo + rows, halo), :], rank - 1),
        copy(vx.at[:, pl.ds(halo, halo)], vx.at[:, pl.ds(halo + rows, halo)], rank - 1)]

    def later(c, carry):
        keys(c)
        values(c)
        return carry

    @pl.when(rank < n_seq - 1)
    def _():
        for c in to_right:
            c.start()

    @pl.when(rank > 0)
    def _():
        for c in to_left:
            c.start()

    lax.fori_loop(1, n_blk - 1, later, 0)
    lax.fori_loop(0, n_blk, lambda c, carry: (queries(c), carry)[1], 0)

    for head in range(2 * n_pairs):
        lanes = slice((head % 2) * QB, (head % 2 + 1) * QB)
        for c in range(n_win):
            hi = 128 * (n_win - c)
            g = jnp.concatenate([br[head:head + 1, hi:hi + 128], br[head:head + 1, hi - 128:hi]], axis=1)
            rolled = pltpu.roll(jnp.broadcast_to(g, (128, 256)), 0, 1, stride=1, stride_axis=0)
            bias[head // 2, c, :, lanes] = rolled[:, :QB]
        bias[head // 2, n_win, :, lanes] = jnp.full((128, QB), NEG, F32)

    relay("o")
    second.wait()
    own = span(core * half, half)
    other = span((1 - core) * half, half)
    xg[own, :] = x_half[...] + x_in2[...]

    def project(at):
        kg[at, :] = dot(xg[at, :], wk[...]).astype(BF)
        vgt[:, at] = dot(wv[...], xg[at, :], ((0,), (1,))).astype(BF)

    def project_query(at):
        qgt[:, at] = dot(wqg[...], xg[at, :], ((0,), (1,))).astype(BF) * BF(scale)

    third = copy(xg.at[own, :], xg.at[own, :], mate)
    project_query(own)
    third.start()
    project(own)
    third.wait()
    project_query(other)
    project(other)

    n_tiles = n_glob // QB

    def glob_unit(i, carry):
        @pl.when(i == 8)
        def _():
            relay("u")
            relay2("o")

        p, t = i // n_tiles, lax.rem(i, n_tiles)
        feat = span(p * 128, 128)
        rhs = pair_rhs(qgt[feat, span(t * QB, QB)])
        top = None
        for c in range(rows // 256):
            s = dot(kx[halo + 256 * c:halo + 256 * c + 256, feat], rhs)
            gscore[256 * c:256 * c + 256, :] = s
            part = jnp.max(s.reshape(32, 8, 2 * QB), axis=0)
            top = part if top is None else jnp.maximum(top, part)
        top = jnp.max(top, axis=0, keepdims=True)
        total = None
        acc = None
        for c in range(rows // 256):
            e = jnp.exp(gscore[256 * c:256 * c + 256, :] - top)
            part = jnp.sum(e.reshape(32, 8, 2 * QB), axis=0)
            total = part if total is None else total + part
            o = dot(vx[feat, halo + 256 * c:halo + 256 * c + 256], e.astype(BF))
            acc = o if acc is None else acc + o
        go[feat, span(t * QB, QB)] = unpair(acc)
        stat = (span(p * 8, 8), span(t * 2 * QB, 2 * QB))
        gm[stat] = jnp.broadcast_to(top, (8, 2 * QB))
        gl[stat] = jnp.broadcast_to(jnp.sum(total, axis=0, keepdims=True), (8, 2 * QB))
        return carry

    lax.fori_loop(0, n_pairs * n_tiles, glob_unit, 0)

    o_half, s_half = loc // 2, gm.shape[0] // 2
    far_o, far_s = span((1 - core) * o_half, o_half), span((1 - core) * s_half, s_half)
    near_o, near_s = span(core * o_half, o_half), span(core * s_half, s_half)
    round1 = [copy(go.at[far_o, :], in_o.at[0], mate), copy(gm.at[far_s, :], in_m.at[0], mate), copy(gl.at[far_s, :], in_l.at[0], mate)]
    round2 = [copy(go.at[near_o, :], in_o.at[1], across), copy(gm.at[near_s, :], in_m.at[1], across), copy(gl.at[near_s, :], in_l.at[1], across)]
    round3 = copy(gfin.at[:, near_o], gfin.at[:, near_o], mate)

    def merge(k, last):
        for pp in range(n_pairs // 2):
            for t in range(n_tiles):
                lanes, at8 = slice(2 * QB * t, 2 * QB * t + 2 * QB), slice(8 * pp, 8 * pp + 8)
                stat = (span(core * s_half + 8 * pp, 8), lanes)
                top = jnp.maximum(gm[stat], in_m[k, at8, lanes])
                a, b = jnp.exp(gm[stat] - top), jnp.exp(in_m[k, at8, lanes] - top)
                tot = gl[stat] * a + in_l[k, at8, lanes] * b
                feat = span(core * o_half + 128 * pp, 128)
                cols = slice(QB * t, QB * t + QB)
                o = go[feat, cols] * spread(a) + in_o[k, 128 * pp:128 * pp + 128, cols] * spread(b)
                if last:
                    gfin[cols, feat] = jnp.transpose(o / spread(tot)).astype(BF)
                else:
                    gm[stat] = top
                    gl[stat] = tot
                    go[feat, cols] = o

    o_base = used[0]

    def o_copy(j):
        at = span(j * QB, QB)
        return pltpu.make_async_remote_copy(
            src_ref=o_mine.at[at, :], dst_ref=o_peer.at[at, :], send_sem=send_sem.at[o_base + j], recv_sem=recv_sem.at[o_base + j],
            device_id={"tp": peer}, device_id_type=MESH)

    def fix(j, carry):
        at = span(j * QB, QB)
        ids = row_start + j * QB + lax.broadcasted_iota(jnp.int32, (QB, n_glob), 0)
        hot = jnp.where(grow[...] == ids, 1.0, 0.0)
        is_glob = jnp.max(hot, axis=1, keepdims=True) > 0.0
        val = dot(hot.astype(BF), gfin[...])
        o_mine[at, :] = jnp.where(is_glob, val, o_mine[at, :].astype(F32)).astype(BF)
        o_copy(j).start()
        return carry

    for c in round1:
        c.start()

    @pl.when(rank < n_seq - 1)
    def _():
        for c in to_right:
            c.wait_send()
        for c in to_left:
            c.wait_recv()

    @pl.when(rank > 0)
    def _():
        for c in to_left:
            c.wait_send()
        for c in to_right:
            c.wait_recv()

    @pl.when(rank == 0)
    def _():
        kx[0:halo, :] = jnp.zeros((halo, loc), BF)
        vx[:, 0:halo] = jnp.zeros((loc, halo), BF)

    @pl.when(rank == n_seq - 1)
    def _():
        kx[halo + rows:, :] = jnp.zeros((halo, loc), BF)
        vx[:, halo + rows:] = jnp.zeros((loc, halo), BF)

    n_chunk = n_win + n_glob // 128
    fix_at = 10

    def window_block(j, carry):
        @pl.when(j == 1)
        def _():
            for c in round1:
                c.wait()
            merge(0, False)
            for c in round2:
                c.start()

        @pl.when(j == 4)
        def _():
            relay("d")

        @pl.when(j == fix_at - 1)
        def _():
            for c in round2:
                c.wait()
            merge(1, True)
            round3.start()

        @pl.when(j == fix_at)
        def _():
            round3.wait()
            lax.fori_loop(0, fix_at - 1, fix, 0)

        @pl.when(j == 12)
        def _():
            relay2("u")

        @pl.when(j >= fix_at)
        def _():
            fix(j - 1, 0)

        q_start = row_start + j * QB
        q_pos = q_start + lax.broadcasted_iota(jnp.int32, (n_glob, QB), 1)
        gmask[...] = jnp.where(jnp.abs(q_pos - gcol[...]) > halo, 0.0, NEG)
        slots = []
        for c in range(n_win):
            key_start = q_start - halo + 128 * c
            slots.append(jnp.where((key_start >= 0) & (key_start < rows * n_seq), c, n_win))
        for p in range(n_pairs):
            lanes = slice(128 * p, 128 * p + 128)
            buf = p % 2
            rhs = pair_rhs(qt[lanes, span(j * QB, QB)])
            top = None
            for c in range(n_chunk):
                if c < n_win:
                    ks = kx[span((j + c) * 128, 128), lanes]
                    extra = bias[p, slots[c]]
                else:
                    at = slice(128 * (c - n_win), 128 * (c - n_win) + 128)
                    ks = kg[at, lanes]
                    extra = jnp.concatenate([gmask[at, :], gmask[at, :]], axis=1)
                s = dot(ks, rhs) + extra
                score[buf, 128 * c:128 * c + 128, :] = s
                part = jnp.max(s.reshape(16, 8, 2 * QB), axis=0)
                top = part if top is None else jnp.maximum(top, part)
            top = jnp.max(top, axis=0, keepdims=True)
            total = None
            for c in range(n_chunk):
                at = slice(128 * c, 128 * c + 128)
                e = jnp.exp(score[buf, at, :] - top)
                score[buf, at, :] = e
                part = jnp.sum(e.reshape(16, 8, 2 * QB), axis=0)
                total = part if total is None else total + part
            inv = 1.0 / jnp.sum(total, axis=0, keepdims=True)
            w_len = 128 * n_win
            pw = (score[buf, :w_len, :] * inv).astype(BF)
            pg = (score[buf, w_len:, :] * inv).astype(BF)
            vt = vx[lanes, pl.ds(pl.multiple_of(j * QB, QB), w_len)]
            o_two = dot(vt, pw) + dot(vgt[lanes, :], pg)
            o_mine[span(j * QB, QB), lanes] = jnp.transpose(unpair(o_two)).astype(BF)
        return carry

    n_win_blk = rows // QB
    lax.fori_loop(0, n_win_blk, window_block, 0)
    fix(n_win_blk - 1, 0)

    relay2("d")
    for k in ("wo", "wu", "wd"):
        loads[k].wait()
    for k in held:
        over_d[k].wait()
        over_d2[k].wait()
    quarter = (rank, across, mate, lax.rem(mate + 2, n_seq))
    mb = 256

    def out_copy(i):
        at = span(i * mb, mb)
        return pltpu.make_async_copy(out_s.at[at, :], out_hbm.at[at, :], load_sem.at[len(loads) + i])

    def mlp_block(i, carry):
        o_copy(2 * i).wait_recv()
        o_copy(2 * i + 1).wait_recv()
        at = span(i * mb, mb)
        acc = x[at, :].astype(F32) + dot(o_mine[at, :], wo[...])
        for k in range(4):
            acc = acc + dot(o_peer[at, span(quarter[k] * depth, depth)], po[k])
        h = acc.astype(BF)
        acc = h.astype(F32)
        for k in range(8):
            cols = slice(piece * (k % 4), piece * (k % 4) + piece)
            up = wu[:, cols] if k < 4 else pu[k - 4]
            down = wd[cols, :] if k < 4 else pd[k - 4]
            act = jax.nn.gelu(dot(h, up)).astype(BF)
            acc = acc + dot(act, down)
        out_s[at, :] = acc.astype(BF)
        out_copy(i).start()
        return carry

    lax.fori_loop(0, rows // mb, mlp_block, 0)

    def drain(j, carry):
        o_copy(j).wait_send()
        return carry

    lax.fori_loop(0, n_win_blk, drain, 0)

    def flush(i, carry):
        out_copy(i).wait()
        return carry

    lax.fori_loop(0, rows // mb, flush, 0)


def solution(mesh):
    n_seq = mesh.shape["sp"]

    def local_layer(tokens, glob_pos, rel_bias, w_query, w_key, w_value, w_query_glob, w_out, w_up, w_down):
        rows, dim = tokens.shape
        heads, n_bias = rel_bias.shape
        halo = (n_bias - 1) // 2
        loc = w_query.shape[1]
        n_glob = glob_pos.shape[0]
        n_pairs = loc // 128
        n_win = 2 * halo // 128 + 1
        scale = (loc // heads) ** -0.5
        hid = w_up.shape[1]
        n_ext = rows + 2 * halo
        half = n_glob // 2
        br = jnp.pad(rel_bias[:, ::-1], ((0, 0), (128, 127)), constant_values=NEG)
        vm = pl.BlockSpec(memory_space=pltpu.VMEM)
        hbm = pl.BlockSpec(memory_space=pl.ANY)

        def buf(*shape, dtype=BF):
            return pltpu.VMEM(shape, dtype)

        return pl.pallas_call(
            functools.partial(layer_kernel, n_seq, scale, halo),
            name="layer",
            in_specs=[hbm, vm, vm, vm] + [hbm] * 7,
            out_specs=hbm,
            out_shape=jax.ShapeDtypeStruct((rows, dim), BF),
            scratch_shapes=[
                buf(rows, dim), buf(4, dim, loc), buf(loc, dim), buf(dim, hid), buf(hid, dim),
                buf(4, loc // n_seq, dim), buf(4, dim, hid // n_seq), buf(4, hid // n_seq, dim),
                buf(loc, rows), buf(n_ext, loc), buf(loc, n_ext), buf(n_glob, loc), buf(loc, n_glob), buf(loc, n_glob),
                buf(half, dim), buf(half, dim), buf(half, dim), buf(half, dim), buf(n_glob, dim),
                buf(loc, n_glob, dtype=F32), buf(n_pairs * 8, 2 * n_glob, dtype=F32), buf(n_pairs * 8, 2 * n_glob, dtype=F32),
                buf(2, loc // 2, n_glob, dtype=F32), buf(2, n_pairs * 4, 2 * n_glob, dtype=F32), buf(2, n_pairs * 4, 2 * n_glob, dtype=F32),
                buf(n_glob, loc),
                buf(n_pairs, n_win + 1, 128, 2 * QB, dtype=F32), buf(n_glob, QB, dtype=F32),
                buf(2, n_win * 128 + n_glob, 2 * QB, dtype=F32), buf(rows, 2 * QB, dtype=F32),
                buf(rows, loc), buf(rows, loc), buf(rows, dim),
                pltpu.SemaphoreType.DMA((26 + rows // QB,)), pltpu.SemaphoreType.DMA((26 + rows // QB,)),
                pltpu.SemaphoreType.DMA((32,))],
            compiler_params=pltpu.CompilerParams(vmem_limit_bytes=67043328, collective_id=0, has_side_effects=True),
        )(tokens, glob_pos[:, None], glob_pos[None, :], br, w_query, w_key, w_value, w_query_glob, w_out, w_up, w_down)

    row_spec = P(("batch", "sp"), None)
    col_spec = P(None, "tp")
    head_spec = P("tp", None)
    in_specs = (row_spec, P("batch"), head_spec, col_spec, col_spec, col_spec, col_spec, head_spec, col_spec, head_spec)
    return jax.shard_map(local_layer, mesh=mesh, in_specs=in_specs, out_specs=row_spec, check_vma=False)
```

```python
import functools

import jax
import jax.numpy as jnp
from jax import lax
from jax.experimental import pallas as pl
from jax.experimental.pallas import tpu as pltpu
from jax.sharding import PartitionSpec as P

BF = jnp.bfloat16
F32 = jnp.float32
NEG = float("-inf")
QB = 128
GROUP = 2
MESH = pl.DeviceIdType.MESH


def dot(a, b, dims=((1,), (0,))):
    return lax.dot_general(a, b, (dims, ((), ())), preferred_element_type=F32)


def span(start, size):
    return pl.ds(pl.multiple_of(start, size), size)


def pair_rhs(q_pair):
    half = lax.broadcasted_iota(jnp.int32, q_pair.shape, 0) < q_pair.shape[0] // 2
    zero = jnp.zeros_like(q_pair)
    return jnp.concatenate([jnp.where(half, q_pair, zero), jnp.where(half, zero, q_pair)], axis=1)


def unpair(o_two):
    n = o_two.shape[1] // 2
    half = lax.broadcasted_iota(jnp.int32, (o_two.shape[0], n), 0) < o_two.shape[0] // 2
    return jnp.where(half, o_two[:, :n], o_two[:, n:])


def spread(stat):
    n = stat.shape[1] // 2
    return jnp.concatenate([jnp.broadcast_to(stat[0:1, :n], (64, n)), jnp.broadcast_to(stat[0:1, n:], (64, n))], axis=0)


def layer_kernel(n_seq, scale, halo, x_hbm, grow, rel, wq_hbm, wk_hbm, wv_hbm, wqg_hbm, wo_hbm, wu_hbm, wd_hbm, out_hbm,
                 x, w4, wo, wu, wd, po, pu, pd, qt, kx, vx, kg, vgt, qgt, x_send, x_half, x_in, x_in2, xg,
                 go, gm, gl, in_o, in_m, in_l, gfin, bias, gcol, score, prob, stat_w, gscore, stat_g, o_mine, o_peer, out_s,
                 send_sem, recv_sem, load_sem):
    rank = lax.axis_index("sp")
    peer = 1 - lax.axis_index("tp")
    core = lax.rem(rank, 2)
    mate = rank + 1 - 2 * core
    across = lax.rem(rank + 2, n_seq)
    rows, dim = x.shape
    n_glob = grow.shape[1]
    n_pairs = qt.shape[0] // 128
    loc = qt.shape[0]
    half = n_glob // 2
    row_start = rank * rows
    n_win = 2 * halo // 128 + 1
    hid = wu.shape[1]
    piece = hid // n_seq
    depth = loc // n_seq

    loads = {}

    def load(key, src, dst):
        loads[key] = pltpu.make_async_copy(src, dst, load_sem.at[len(loads)])
        loads[key].start()

    for c in range(4):
        at = slice(512 * c, 512 * c + 512)
        load(("x", c), x_hbm.at[at, :], x.at[at, :])
    for c, w in enumerate((wk_hbm, wv_hbm, wq_hbm, wqg_hbm)):
        load(("w", c), w, w4.at[c])
    load("wo", wo_hbm, wo)
    load("wu", wu_hbm, wu)
    load("wd", wd_hbm, wd)
    wk, wv, wq, wqg = (w4.at[c] for c in range(4))

    barrier = pltpu.get_barrier_semaphore()
    for step in range(1, n_seq):
        pl.semaphore_signal(barrier, inc=1, device_id={"sp": lax.rem(rank + step, n_seq)}, device_id_type=MESH)
    pl.semaphore_signal(barrier, inc=1, device_id={"tp": peer}, device_id_type=MESH)
    pl.semaphore_wait(barrier, n_seq)

    used = [0]

    def copy(src, dst, sp=None):
        idx = used[0]
        used[0] += 1
        return pltpu.make_async_remote_copy(
            src_ref=src, dst_ref=dst, send_sem=send_sem.at[idx], recv_sem=recv_sem.at[idx],
            device_id={"tp": peer} if sp is None else {"sp": sp}, device_id_type=MESH)

    hp = piece // 2
    src_quarter = {
        "o": wo_hbm.at[span(rank * depth, depth), :],
        "u0": wu_hbm.at[:, span(rank * piece, hp)], "u1": wu_hbm.at[:, pl.ds(pl.multiple_of(rank * piece + hp, hp), hp)],
        "d0": wd_hbm.at[span(rank * piece, hp), :], "d1": wd_hbm.at[pl.ds(pl.multiple_of(rank * piece + hp, hp), hp), :]}

    def held(k, slot):
        if k == "o":
            return po.at[slot]
        at = slice(hp * int(k[1]), hp * int(k[1]) + hp)
        return pu.at[slot, :, at] if k[0] == "u" else pd.at[slot, at, :]

    parts = tuple(src_quarter)
    over_tp = {k: copy(src_quarter[k], held(k, 0)) for k in parts}
    over_x = {k: copy(held(k, 0), held(k, 1), across) for k in parts}
    over_d = {k: copy(held(k, 0), held(k, 2), mate) for k in parts}
    over_d2 = {k: copy(held(k, 1), held(k, 3), mate) for k in parts}
    for k in parts:
        over_tp[k].start()

    def relay(k):
        over_tp[k].wait()
        over_x[k].start()
        over_d[k].start()

    def relay2(k):
        over_x[k].wait()
        over_d2[k].start()

    for c in range(n_glob // 128):
        at = slice(128 * c, 128 * c + 128)
        gcol[at, :] = jnp.transpose(jnp.broadcast_to(grow[:, at].astype(F32), (128, 128)))

    def picked(which):
        slots = gcol[span(which * half, half), 0:1].astype(jnp.int32) - row_start
        acc = None
        for c in range(rows // 512):
            at = lax.broadcasted_iota(jnp.int32, (half, 512), 1) + 512 * c
            hot = jnp.where(slots == at, 1.0, 0.0).astype(BF)
            part = dot(hot, x[512 * c:512 * c + 512, :])
            acc = part if acc is None else acc + part
        return acc.astype(BF)

    for c in range(4):
        loads["x", c].wait()
    x_send[...] = picked(1 - core)
    first = copy(x_send, x_in, mate)
    x_half[...] = picked(core)
    first.start()

    def keys(c):
        kx[span(halo + c * 256, 256), :] = dot(x[span(c * 256, 256), :], wk[...]).astype(BF)

    def values(c):
        vx[:, span(halo + c * 256, 256)] = dot(wv[...], x[span(c * 256, 256), :], ((0,), (1,))).astype(BF)

    def queries(c):
        qt[:, span(c * 256, 256)] = dot(wq[...], x[span(c * 256, 256), :], ((0,), (1,))).astype(BF) * BF(scale)

    n_blk = rows // 256
    for c in range(4):
        loads["w", c].wait()
    keys(0)
    keys(n_blk - 1)
    first.wait()
    x_half[...] = x_half[...] + x_in[...]
    values(0)
    second = copy(x_half, x_in2, across)
    second.start()
    values(n_blk - 1)
    to_right = [
        copy(kx.at[pl.ds(rows, halo), :], kx.at[pl.ds(0, halo), :], rank + 1),
        copy(vx.at[:, pl.ds(rows, halo)], vx.at[:, pl.ds(0, halo)], rank + 1)]
    to_left = [
        copy(kx.at[pl.ds(halo, halo), :], kx.at[pl.ds(halo + rows, halo), :], rank - 1),
        copy(vx.at[:, pl.ds(halo, halo)], vx.at[:, pl.ds(halo + rows, halo)], rank - 1)]

    def later(c, carry):
        keys(c)
        values(c)
        return carry

    @pl.when(rank < n_seq - 1)
    def _():
        for c in to_right:
            c.start()

    @pl.when(rank > 0)
    def _():
        for c in to_left:
            c.start()

    lax.fori_loop(1, n_blk - 1, later, 0)
    lax.fori_loop(0, n_blk, lambda c, carry: (queries(c), carry)[1], 0)

    for head in range(2 * n_pairs):
        lanes = slice((head % 2) * QB, (head % 2 + 1) * QB)
        known = []
        for c in range(n_win):
            row = rel[head:head + 1, 128 * c:min(128 * c + 128, 2 * halo + 1)]
            if row.shape[1] < 128:
                at = lax.broadcasted_iota(jnp.int32, (1, 128), 1) + 128 * c
                row = jnp.where(at <= 2 * halo, jnp.broadcast_to(row[:, 0:1], (1, 128)), NEG)
            known.append(row)
        for c in range(n_win):
            before = known[c - 1] if c else jnp.full((1, 128), NEG, F32)
            both = jnp.broadcast_to(jnp.concatenate([known[c], before], axis=1), (128, 256))
            bias[head // 2, c, :, lanes] = jnp.transpose(pltpu.roll(both, 0, 1, stride=1, stride_axis=0)[:, :QB])
        bias[head // 2, n_win, :, lanes] = jnp.full((128, QB), NEG, F32)

    second.wait()
    relay("o")
    relay("u0")
    own = span(core * half, half)
    other = span((1 - core) * half, half)
    xg[own, :] = x_half[...] + x_in2[...]

    def project(at):
        kg[at, :] = dot(xg[at, :], wk[...]).astype(BF)
        vgt[:, at] = dot(wv[...], xg[at, :], ((0,), (1,))).astype(BF)

    def project_query(at):
        qgt[:, at] = dot(wqg[...], xg[at, :], ((0,), (1,))).astype(BF) * BF(scale)

    third = copy(xg.at[own, :], xg.at[own, :], mate)
    project_query(own)
    third.start()
    project(own)
    third.wait()
    project_query(other)
    project(other)

    n_tiles = n_glob // QB

    gscore[...] = jnp.zeros(gscore.shape, F32)
    stat_g[...] = jnp.zeros(stat_g.shape, F32)
    n_units = n_pairs * n_tiles

    def glob_unit(i, carry):
        @pl.when(i == 5)
        def _():
            relay("u1")

        @pl.when(i == 12)
        def _():
            relay("d0")
            relay2("o")

        new, old = jnp.minimum(i, n_units - 1), jnp.maximum(i - 1, 0)
        p, t = new // n_tiles, lax.rem(new, n_tiles)
        feat = span(p * 128, 128)
        p_old, t_old = old // n_tiles, lax.rem(old, n_tiles)
        feat_old = span(p_old * 128, 128)
        rhs = pair_rhs(qgt[feat, span(t * QB, QB)])
        old_top = stat_g[...]
        top, total, acc = None, None, None
        for c in range(rows // 256):
            at = slice(256 * c, 256 * c + 256)
            e = jnp.exp(gscore[at, :].reshape(32, 8, 2 * QB) - old_top)
            part = jnp.sum(e, axis=0)
            total = part if total is None else total + part
            o = dot(vx[feat_old, halo + 256 * c:halo + 256 * c + 256], e.reshape(256, 2 * QB).astype(BF))
            acc = o if acc is None else acc + o
            s = dot(kx[halo + 256 * c:halo + 256 * c + 256, feat], rhs)
            gscore[at, :] = s
            part = jnp.max(s.reshape(32, 8, 2 * QB), axis=0)
            top = part if top is None else jnp.maximum(top, part)
        go[feat_old, span(t_old * QB, QB)] = unpair(acc)
        stat = (span(p_old * 8, 8), span(t_old * 2 * QB, 2 * QB))
        gm[stat] = old_top
        gl[stat] = jnp.broadcast_to(jnp.sum(total, axis=0, keepdims=True), (8, 2 * QB))
        stat_g[...] = jnp.broadcast_to(jnp.max(top, axis=0, keepdims=True), (8, 2 * QB))
        return carry

    lax.fori_loop(0, n_units + 1, glob_unit, 0)

    o_half, s_half = loc // 2, gm.shape[0] // 2
    far_o, far_s = span((1 - core) * o_half, o_half), span((1 - core) * s_half, s_half)
    near_o, near_s = span(core * o_half, o_half), span(core * s_half, s_half)
    round1 = [copy(go.at[far_o, :], in_o.at[0], mate), copy(gm.at[far_s, :], in_m.at[0], mate), copy(gl.at[far_s, :], in_l.at[0], mate)]
    round2 = [copy(go.at[near_o, :], in_o.at[1], across), copy(gm.at[near_s, :], in_m.at[1], across), copy(gl.at[near_s, :], in_l.at[1], across)]
    round3 = copy(gfin.at[:, near_o], gfin.at[:, near_o], mate)

    def merge(k, last):
        for pp in range(n_pairs // 2):
            for t in range(n_tiles):
                lanes, at8 = slice(2 * QB * t, 2 * QB * t + 2 * QB), slice(8 * pp, 8 * pp + 8)
                stat = (span(core * s_half + 8 * pp, 8), lanes)
                top = jnp.maximum(gm[stat], in_m[k, at8, lanes])
                a, b = jnp.exp(gm[stat] - top), jnp.exp(in_m[k, at8, lanes] - top)
                tot = gl[stat] * a + in_l[k, at8, lanes] * b
                feat = span(core * o_half + 128 * pp, 128)
                cols = slice(QB * t, QB * t + QB)
                o = go[feat, cols] * spread(a) + in_o[k, 128 * pp:128 * pp + 128, cols] * spread(b)
                if last:
                    gfin[cols, feat] = jnp.transpose(o / spread(tot)).astype(BF)
                else:
                    gm[stat] = top
                    gl[stat] = tot
                    go[feat, cols] = o

    o_base = used[0]

    def o_copy(j):
        at = span(j * QB, QB)
        return pltpu.make_async_remote_copy(
            src_ref=o_mine.at[at, :], dst_ref=o_peer.at[at, :], send_sem=send_sem.at[o_base + j], recv_sem=recv_sem.at[o_base + j],
            device_id={"tp": peer}, device_id_type=MESH)

    def fix(j, carry):
        at = span(j * QB, QB)
        ids = row_start + j * QB + lax.broadcasted_iota(jnp.int32, (QB, n_glob), 0)
        hot = jnp.where(grow[...] == ids, 1.0, 0.0)
        is_glob = jnp.max(hot, axis=1, keepdims=True) > 0.0
        val = dot(hot.astype(BF), gfin[...])
        o_mine[at, :] = jnp.where(is_glob, val, o_mine[at, :].astype(F32)).astype(BF)
        o_copy(j).start()
        return carry

    for c in round1:
        c.start()

    @pl.when(rank < n_seq - 1)
    def _():
        for c in to_right:
            c.wait_send()
        for c in to_left:
            c.wait_recv()

    @pl.when(rank > 0)
    def _():
        for c in to_left:
            c.wait_send()
        for c in to_right:
            c.wait_recv()

    @pl.when(rank == 0)
    def _():
        kx[0:halo, :] = jnp.zeros((halo, loc), BF)
        vx[:, 0:halo] = jnp.zeros((loc, halo), BF)

    @pl.when(rank == n_seq - 1)
    def _():
        kx[halo + rows:, :] = jnp.zeros((halo, loc), BF)
        vx[:, halo + rows:] = jnp.zeros((loc, halo), BF)

    n_chunk = n_win + n_glob // 128
    n_win_blk = rows // QB
    per = n_pairs // GROUP
    n_groups = n_win_blk * per
    fix_at = 22
    score[...] = jnp.zeros(score.shape, F32)
    prob[...] = jnp.zeros(prob.shape, F32)
    stat_w[...] = jnp.ones(stat_w.shape, F32)

    def window_group(n, carry):
        @pl.when(n == 2)
        def _():
            for c in round1:
                c.wait()
            merge(0, False)
            for c in round2:
                c.start()

        @pl.when(n == 18)
        def _():
            relay("d1")

        @pl.when(n == fix_at - 2)
        def _():
            for c in round2:
                c.wait()
            merge(1, True)
            round3.start()

        @pl.when(n == fix_at)
        def _():
            round3.wait()
            lax.fori_loop(0, fix_at // per - 1, fix, 0)

        @pl.when(n == 26)
        def _():
            relay2("u0")

        @pl.when(n == 30)
        def _():
            relay2("u1")

        @pl.when((n > fix_at) & (lax.rem(n, per) == 0))
        def _():
            fix(n // per - 2, 0)

        new, old = jnp.minimum(n, n_groups - 1), jnp.maximum(n - 2, 0)
        j, j_old = new // per, old // per
        q_start = row_start + j * QB
        q_pos = (q_start + lax.broadcasted_iota(jnp.int32, (128, QB), 1)).astype(F32)
        slots = []
        for c in range(n_win):
            key_start = q_start - halo + 128 * c
            slots.append(jnp.where((key_start >= 0) & (key_start < rows * n_seq), c, n_win))
        for u in range(GROUP):
            p = lax.rem(new, per) * GROUP + u
            feat = span(p * 128, 128)
            feat_old = span((lax.rem(old, per) * GROUP + u) * 128, 128)
            rhs = pair_rhs(qt[feat, span(j * QB, QB)])
            mid_top, old_inv = stat_w[0, u], stat_w[1, u]
            top, total, acc = None, None, None
            for b in range(0, n_chunk, 2):
                cs = list(range(b, min(b + 2, n_chunk)))
                at = slice(128 * b, 128 * (cs[-1] + 1))
                w = (prob[u, at, :].reshape(-1, 8, 2 * QB) * old_inv).reshape(-1, 2 * QB).astype(BF)
                vs = [vx[feat_old, span((j_old + c) * 128, 128)] if c < n_win else vgt[feat_old, 128 * (c - n_win):128 * (c - n_win) + 128]
                      for c in cs]
                o = dot(jnp.concatenate(vs, axis=1), w)
                acc = o if acc is None else acc + o
                e = jnp.exp(score[u, at, :].reshape(-1, 8, 2 * QB) - mid_top)
                prob[u, at, :] = e.reshape(-1, 2 * QB)
                part = jnp.sum(e, axis=0)
                total = part if total is None else total + part
                for c in cs:
                    if c < n_win:
                        ks = kx[span((j + c) * 128, 128), feat]
                        extra = bias[p, slots[c]]
                    else:
                        rows_g = slice(128 * (c - n_win), 128 * (c - n_win) + 128)
                        ks = kg[rows_g, feat]
                        mask = jnp.where(jnp.abs(q_pos - gcol[rows_g, :]) > halo, 0.0, NEG)
                        extra = jnp.concatenate([mask, mask], axis=1)
                    s = dot(ks, rhs) + extra
                    score[u, 128 * c:128 * c + 128, :] = s
                    part = jnp.max(s.reshape(16, 8, 2 * QB), axis=0)
                    top = part if top is None else jnp.maximum(top, part)
            o_mine[span(j_old * QB, QB), feat_old] = jnp.transpose(unpair(acc)).astype(BF)
            stat_w[0, u] = jnp.broadcast_to(jnp.max(top, axis=0, keepdims=True), (8, 2 * QB))
            stat_w[1, u] = jnp.broadcast_to(1.0 / jnp.sum(total, axis=0, keepdims=True), (8, 2 * QB))
        return carry

    lax.fori_loop(0, n_groups + 2, window_group, 0)
    fix(n_win_blk - 1, 0)

    relay2("d0")
    for k in ("wo", "wu", "wd"):
        loads[k].wait()
    for k in parts:
        over_d[k].wait()
        if k[0] != "d":
            over_d2[k].wait()
    quarter = (rank, across, mate, lax.rem(mate + 2, n_seq))
    mb = 256

    def out_copy(i):
        at = span(i * mb, mb)
        return pltpu.make_async_copy(out_s.at[at, :], out_hbm.at[at, :], load_sem.at[len(loads) + i])

    def mlp_block(i, carry):
        o_copy(2 * i).wait_recv()
        o_copy(2 * i + 1).wait_recv()
        at = span(i * mb, mb)
        acc = x[at, :].astype(F32) + dot(o_mine[at, :], wo[...])
        for k in range(4):
            acc = acc + dot(o_peer[at, span(quarter[k] * depth, depth)], po[k])
        h = acc.astype(BF)
        acc = h.astype(F32)
        for k in (0, 1, 2, 3, 4, 6, 5, 7):
            if k == 5:
                @pl.when(i == 0)
                def _():
                    relay2("d1")
                    over_d2["d0"].wait()
                    over_d2["d1"].wait()
            cols = slice(piece * (k % 4), piece * (k % 4) + piece)
            up = wu[:, cols] if k < 4 else pu[k - 4]
            down = wd[cols, :] if k < 4 else pd[k - 4]
            act = jax.nn.gelu(dot(h, up)).astype(BF)
            acc = acc + dot(act, down)
        out_s[at, :] = acc.astype(BF)
        out_copy(i).start()
        return carry

    lax.fori_loop(0, rows // mb, mlp_block, 0)

    def drain(j, carry):
        o_copy(j).wait_send()
        return carry

    lax.fori_loop(0, n_win_blk, drain, 0)

    def flush(i, carry):
        out_copy(i).wait()
        return carry

    lax.fori_loop(0, rows // mb, flush, 0)


def solution(mesh):
    n_seq = mesh.shape["sp"]

    def local_layer(tokens, glob_pos, rel_bias, w_query, w_key, w_value, w_query_glob, w_out, w_up, w_down):
        rows, dim = tokens.shape
        heads, n_bias = rel_bias.shape
        halo = (n_bias - 1) // 2
        loc = w_query.shape[1]
        n_glob = glob_pos.shape[0]
        n_pairs = loc // 128
        n_win = 2 * halo // 128 + 1
        scale = (loc // heads) ** -0.5
        hid = w_up.shape[1]
        n_ext = rows + 2 * halo
        half = n_glob // 2
        vm = pl.BlockSpec(memory_space=pltpu.VMEM)
        hbm = pl.BlockSpec(memory_space=pl.ANY)

        def buf(*shape, dtype=BF):
            return pltpu.VMEM(shape, dtype)

        return pl.pallas_call(
            functools.partial(layer_kernel, n_seq, scale, halo),
            name="layer",
            in_specs=[hbm, vm, vm] + [hbm] * 7,
            out_specs=hbm,
            out_shape=jax.ShapeDtypeStruct((rows, dim), BF),
            scratch_shapes=[
                buf(rows, dim), buf(4, dim, loc), buf(loc, dim), buf(dim, hid), buf(hid, dim),
                buf(4, loc // n_seq, dim), buf(4, dim, hid // n_seq), buf(4, hid // n_seq, dim),
                buf(loc, rows), buf(n_ext, loc), buf(loc, n_ext), buf(n_glob, loc), buf(loc, n_glob), buf(loc, n_glob),
                buf(half, dim), buf(half, dim), buf(half, dim), buf(half, dim), buf(n_glob, dim),
                buf(loc, n_glob, dtype=F32), buf(n_pairs * 8, 2 * n_glob, dtype=F32), buf(n_pairs * 8, 2 * n_glob, dtype=F32),
                buf(2, loc // 2, n_glob, dtype=F32), buf(2, n_pairs * 4, 2 * n_glob, dtype=F32), buf(2, n_pairs * 4, 2 * n_glob, dtype=F32),
                buf(n_glob, loc),
                buf(n_pairs, n_win + 1, 128, 2 * QB, dtype=F32), buf(n_glob, QB, dtype=F32),
                buf(GROUP, n_win * 128 + n_glob, 2 * QB, dtype=F32), buf(GROUP, n_win * 128 + n_glob, 2 * QB, dtype=F32),
                buf(2, GROUP, 8, 2 * QB, dtype=F32), buf(rows, 2 * QB, dtype=F32), buf(8, 2 * QB, dtype=F32),
                buf(rows, loc), buf(rows, loc), buf(rows, dim),
                pltpu.SemaphoreType.DMA((34 + rows // QB,)), pltpu.SemaphoreType.DMA((34 + rows // QB,)),
                pltpu.SemaphoreType.DMA((32,))],
            compiler_params=pltpu.CompilerParams(vmem_limit_bytes=67043328, collective_id=0, has_side_effects=True),
        )(tokens, glob_pos[None, :], rel_bias, w_query, w_key, w_value, w_query_glob, w_out, w_up, w_down)

    row_spec = P(("batch", "sp"), None)
    col_spec = P(None, "tp")
    head_spec = P("tp", None)
    in_specs = (row_spec, P("batch"), head_spec, col_spec, col_spec, col_spec, col_spec, head_spec, col_spec, head_spec)
    return jax.shard_map(local_layer, mesh=mesh, in_specs=in_specs, out_specs=row_spec, check_vma=False)
```

```python
import functools

import jax
import jax.numpy as jnp
from jax import lax
from jax.experimental import pallas as pl
from jax.experimental.pallas import tpu as pltpu
from jax.sharding import PartitionSpec as P

BF = jnp.bfloat16
F32 = jnp.float32
NEG = float("-inf")
QB = 128
GROUP = 2
MESH = pl.DeviceIdType.MESH


def dot(a, b, dims=((1,), (0,))):
    return lax.dot_general(a, b, (dims, ((), ())), preferred_element_type=F32)


def span(start, size):
    return pl.ds(pl.multiple_of(start, size), size)


def pair_rhs(q_pair):
    half = lax.broadcasted_iota(jnp.int32, q_pair.shape, 0) < q_pair.shape[0] // 2
    zero = jnp.zeros_like(q_pair)
    return jnp.concatenate([jnp.where(half, q_pair, zero), jnp.where(half, zero, q_pair)], axis=1)


def unpair(o_two):
    n = o_two.shape[1] // 2
    half = lax.broadcasted_iota(jnp.int32, (o_two.shape[0], n), 0) < o_two.shape[0] // 2
    return jnp.where(half, o_two[:, :n], o_two[:, n:])


def spread(stat):
    n = stat.shape[1] // 2
    return jnp.concatenate([jnp.broadcast_to(stat[0:1, :n], (64, n)), jnp.broadcast_to(stat[0:1, n:], (64, n))], axis=0)


def layer_kernel(n_seq, scale, halo, x_hbm, grow, rel, wq_hbm, wk_hbm, wv_hbm, wqg_hbm, wo_hbm, wu_hbm, wd_hbm, out_hbm,
                 x, w4, wo, wu, wd, po, pu, pd, qt, kx, vx, kg, vgt, qgt, x_send, x_half, x_in, x_in2, xg,
                 go, gm, gl, in_o, in_m, in_l, gfin, bias, gcol, score, prob, stat_w, gscore, stat_g, o_mine, o_peer, out_s,
                 send_sem, recv_sem, load_sem):
    rank = lax.axis_index("sp")
    peer = 1 - lax.axis_index("tp")
    core = lax.rem(rank, 2)
    mate = rank + 1 - 2 * core
    across = lax.rem(rank + 2, n_seq)
    rows, dim = x.shape
    n_glob = grow.shape[1]
    n_pairs = qt.shape[0] // 128
    loc = qt.shape[0]
    half = n_glob // 2
    row_start = rank * rows
    n_win = 2 * halo // 128 + 1
    hid = wu.shape[1]
    piece = hid // n_seq
    depth = loc // n_seq

    loads = {}

    def load(key, src, dst):
        loads[key] = pltpu.make_async_copy(src, dst, load_sem.at[len(loads)])
        loads[key].start()

    for c in range(4):
        at = slice(512 * c, 512 * c + 512)
        load(("x", c), x_hbm.at[at, :], x.at[at, :])
    for c, w in enumerate((wk_hbm, wv_hbm, wq_hbm, wqg_hbm)):
        load(("w", c), w, w4.at[c])
    load("wo", wo_hbm, wo)
    load("wu", wu_hbm, wu)
    load("wd", wd_hbm, wd)
    wk, wv, wq, wqg = (w4.at[c] for c in range(4))

    barrier = pltpu.get_barrier_semaphore()
    for step in range(1, n_seq):
        pl.semaphore_signal(barrier, inc=1, device_id={"sp": lax.rem(rank + step, n_seq)}, device_id_type=MESH)
    pl.semaphore_signal(barrier, inc=1, device_id={"tp": peer}, device_id_type=MESH)
    pl.semaphore_wait(barrier, n_seq)

    used = [0]

    def copy(src, dst, sp=None):
        idx = used[0]
        used[0] += 1
        return pltpu.make_async_remote_copy(
            src_ref=src, dst_ref=dst, send_sem=send_sem.at[idx], recv_sem=recv_sem.at[idx],
            device_id={"tp": peer} if sp is None else {"sp": sp}, device_id_type=MESH)

    hp = piece // 2
    src_quarter = {
        "o": wo_hbm.at[span(rank * depth, depth), :],
        "u0": wu_hbm.at[:, span(rank * piece, hp)], "u1": wu_hbm.at[:, pl.ds(pl.multiple_of(rank * piece + hp, hp), hp)],
        "d0": wd_hbm.at[span(rank * piece, hp), :], "d1": wd_hbm.at[pl.ds(pl.multiple_of(rank * piece + hp, hp), hp), :]}

    def held(k, slot):
        if k == "o":
            return po.at[slot]
        at = slice(hp * int(k[1]), hp * int(k[1]) + hp)
        return pu.at[slot, :, at] if k[0] == "u" else pd.at[slot, at, :]

    parts = tuple(src_quarter)
    over_tp = {k: copy(src_quarter[k], held(k, 0)) for k in parts}
    over_x = {k: copy(held(k, 0), held(k, 1), across) for k in parts if k != "d1"}
    over_d = {k: copy(held(k, 0), held(k, 2), mate) for k in parts}
    over_d2 = {k: copy(held(k, 1), held(k, 3), mate) for k in parts}
    over_x["d1"] = copy(wd_hbm.at[pl.ds(pl.multiple_of(across * piece + hp, hp), hp), :], held("d1", 1))
    for k in ("o", "u0", "u1"):
        over_tp[k].start()
    then = {"o": over_tp["d0"], "u0": over_tp["d1"], "u1": over_x["d1"]}

    def relay(k):
        over_tp[k].wait()
        if k in then:
            then[k].start()
        if k != "d1":
            over_x[k].start()
        over_d[k].start()

    def relay2(k):
        over_x[k].wait()
        over_d2[k].start()

    for c in range(n_glob // 128):
        at = slice(128 * c, 128 * c + 128)
        gcol[at, :] = jnp.transpose(jnp.broadcast_to(grow[:, at].astype(F32), (128, 128)))

    def picked(which):
        slots = gcol[span(which * half, half), 0:1].astype(jnp.int32) - row_start
        acc = None
        for c in range(rows // 512):
            at = lax.broadcasted_iota(jnp.int32, (half, 512), 1) + 512 * c
            hot = jnp.where(slots == at, 1.0, 0.0).astype(BF)
            part = dot(hot, x[512 * c:512 * c + 512, :])
            acc = part if acc is None else acc + part
        return acc.astype(BF)

    for c in range(4):
        loads["x", c].wait()
    x_send[...] = picked(1 - core)
    first = copy(x_send, x_in, mate)
    x_half[...] = picked(core)
    first.start()

    def keys(c):
        kx[span(halo + c * 256, 256), :] = dot(x[span(c * 256, 256), :], wk[...]).astype(BF)

    def values(c):
        vx[:, span(halo + c * 256, 256)] = dot(wv[...], x[span(c * 256, 256), :], ((0,), (1,))).astype(BF)

    def queries(c):
        qt[:, span(c * 256, 256)] = dot(wq[...], x[span(c * 256, 256), :], ((0,), (1,))).astype(BF) * BF(scale)

    n_blk = rows // 256
    for c in range(4):
        loads["w", c].wait()
    keys(0)
    keys(n_blk - 1)
    first.wait()
    x_half[...] = x_half[...] + x_in[...]
    values(0)
    second = copy(x_half, x_in2, across)
    second.start()
    values(n_blk - 1)
    to_right = [
        copy(kx.at[pl.ds(rows, halo), :], kx.at[pl.ds(0, halo), :], rank + 1),
        copy(vx.at[:, pl.ds(rows, halo)], vx.at[:, pl.ds(0, halo)], rank + 1)]
    to_left = [
        copy(kx.at[pl.ds(halo, halo), :], kx.at[pl.ds(halo + rows, halo), :], rank - 1),
        copy(vx.at[:, pl.ds(halo, halo)], vx.at[:, pl.ds(halo + rows, halo)], rank - 1)]

    def later(c, carry):
        keys(c)
        values(c)
        return carry

    @pl.when(rank < n_seq - 1)
    def _():
        for c in to_right:
            c.start()

    @pl.when(rank > 0)
    def _():
        for c in to_left:
            c.start()

    lax.fori_loop(1, n_blk - 1, later, 0)
    lax.fori_loop(0, n_blk, lambda c, carry: (queries(c), carry)[1], 0)

    for head in range(2 * n_pairs):
        lanes = slice((head % 2) * QB, (head % 2 + 1) * QB)
        known = []
        for c in range(n_win):
            row = rel[head:head + 1, 128 * c:min(128 * c + 128, 2 * halo + 1)]
            if row.shape[1] < 128:
                at = lax.broadcasted_iota(jnp.int32, (1, 128), 1) + 128 * c
                row = jnp.where(at <= 2 * halo, jnp.broadcast_to(row[:, 0:1], (1, 128)), NEG)
            known.append(row)
        for c in range(n_win):
            before = known[c - 1] if c else jnp.full((1, 128), NEG, F32)
            both = jnp.broadcast_to(jnp.concatenate([known[c], before], axis=1), (128, 256))
            bias[head // 2, c, :, lanes] = jnp.transpose(pltpu.roll(both, 0, 1, stride=1, stride_axis=0)[:, :QB])
        bias[head // 2, n_win, :, lanes] = jnp.full((128, QB), NEG, F32)

    second.wait()
    relay("o")
    relay("u0")
    own = span(core * half, half)
    other = span((1 - core) * half, half)
    xg[own, :] = x_half[...] + x_in2[...]

    def project(at):
        kg[at, :] = dot(xg[at, :], wk[...]).astype(BF)
        vgt[:, at] = dot(wv[...], xg[at, :], ((0,), (1,))).astype(BF)

    def project_query(at):
        qgt[:, at] = dot(wqg[...], xg[at, :], ((0,), (1,))).astype(BF) * BF(scale)

    third = copy(xg.at[own, :], xg.at[own, :], mate)
    project_query(own)
    third.start()
    project(own)
    third.wait()
    project_query(other)
    project(other)

    n_tiles = n_glob // QB

    gscore[...] = jnp.zeros(gscore.shape, F32)
    stat_g[...] = jnp.zeros(stat_g.shape, F32)
    n_units = n_pairs * n_tiles

    def glob_unit(i, carry):
        @pl.when(i == 8)
        def _():
            relay2("o")

        new, old = jnp.minimum(i, n_units - 1), jnp.maximum(i - 1, 0)
        p, t = new // n_tiles, lax.rem(new, n_tiles)
        feat = span(p * 128, 128)
        p_old, t_old = old // n_tiles, lax.rem(old, n_tiles)
        feat_old = span(p_old * 128, 128)
        rhs = pair_rhs(qgt[feat, span(t * QB, QB)])
        old_top = stat_g[...]
        top, total, acc = None, None, None
        for c in range(rows // 256):
            at = slice(256 * c, 256 * c + 256)
            e = jnp.exp(gscore[at, :].reshape(32, 8, 2 * QB) - old_top)
            part = jnp.sum(e, axis=0)
            total = part if total is None else total + part
            o = dot(vx[feat_old, halo + 256 * c:halo + 256 * c + 256], e.reshape(256, 2 * QB).astype(BF))
            acc = o if acc is None else acc + o
            s = dot(kx[halo + 256 * c:halo + 256 * c + 256, feat], rhs)
            gscore[at, :] = s
            part = jnp.max(s.reshape(32, 8, 2 * QB), axis=0)
            top = part if top is None else jnp.maximum(top, part)
        go[feat_old, span(t_old * QB, QB)] = unpair(acc)
        stat = (span(p_old * 8, 8), span(t_old * 2 * QB, 2 * QB))
        gm[stat] = old_top
        gl[stat] = jnp.broadcast_to(jnp.sum(total, axis=0, keepdims=True), (8, 2 * QB))
        stat_g[...] = jnp.broadcast_to(jnp.max(top, axis=0, keepdims=True), (8, 2 * QB))
        return carry

    lax.fori_loop(0, n_units + 1, glob_unit, 0)

    o_half, s_half = loc // 2, gm.shape[0] // 2
    far_o, far_s = span((1 - core) * o_half, o_half), span((1 - core) * s_half, s_half)
    near_o, near_s = span(core * o_half, o_half), span(core * s_half, s_half)
    round1 = [copy(go.at[far_o, :], in_o.at[0], mate), copy(gm.at[far_s, :], in_m.at[0], mate), copy(gl.at[far_s, :], in_l.at[0], mate)]
    round2 = [copy(go.at[near_o, :], in_o.at[1], across), copy(gm.at[near_s, :], in_m.at[1], across), copy(gl.at[near_s, :], in_l.at[1], across)]
    round3 = copy(gfin.at[:, near_o], gfin.at[:, near_o], mate)

    def merge(k, last):
        for pp in range(n_pairs // 2):
            for t in range(n_tiles):
                lanes, at8 = slice(2 * QB * t, 2 * QB * t + 2 * QB), slice(8 * pp, 8 * pp + 8)
                stat = (span(core * s_half + 8 * pp, 8), lanes)
                top = jnp.maximum(gm[stat], in_m[k, at8, lanes])
                a, b = jnp.exp(gm[stat] - top), jnp.exp(in_m[k, at8, lanes] - top)
                tot = gl[stat] * a + in_l[k, at8, lanes] * b
                feat = span(core * o_half + 128 * pp, 128)
                cols = slice(QB * t, QB * t + QB)
                o = go[feat, cols] * spread(a) + in_o[k, 128 * pp:128 * pp + 128, cols] * spread(b)
                if last:
                    gfin[cols, feat] = jnp.transpose(o / spread(tot)).astype(BF)
                else:
                    gm[stat] = top
                    gl[stat] = tot
                    go[feat, cols] = o

    o_base = used[0]

    def o_copy(j):
        at = span(j * QB, QB)
        return pltpu.make_async_remote_copy(
            src_ref=o_mine.at[at, :], dst_ref=o_peer.at[at, :], send_sem=send_sem.at[o_base + j], recv_sem=recv_sem.at[o_base + j],
            device_id={"tp": peer}, device_id_type=MESH)

    def fix(j, carry):
        at = span(j * QB, QB)
        ids = row_start + j * QB + lax.broadcasted_iota(jnp.int32, (QB, n_glob), 0)
        hot = jnp.where(grow[...] == ids, 1.0, 0.0)
        is_glob = jnp.max(hot, axis=1, keepdims=True) > 0.0
        val = dot(hot.astype(BF), gfin[...])
        o_mine[at, :] = jnp.where(is_glob, val, o_mine[at, :].astype(F32)).astype(BF)
        o_copy(j).start()
        return carry

    for c in round1:
        c.start()

    @pl.when(rank < n_seq - 1)
    def _():
        for c in to_right:
            c.wait_send()
        for c in to_left:
            c.wait_recv()

    @pl.when(rank > 0)
    def _():
        for c in to_left:
            c.wait_send()
        for c in to_right:
            c.wait_recv()

    @pl.when(rank == 0)
    def _():
        kx[0:halo, :] = jnp.zeros((halo, loc), BF)
        vx[:, 0:halo] = jnp.zeros((loc, halo), BF)

    @pl.when(rank == n_seq - 1)
    def _():
        kx[halo + rows:, :] = jnp.zeros((halo, loc), BF)
        vx[:, halo + rows:] = jnp.zeros((loc, halo), BF)

    n_chunk = n_win + n_glob // 128
    n_win_blk = rows // QB
    per = n_pairs // GROUP
    n_groups = n_win_blk * per
    fix_at = 20
    score[...] = jnp.zeros(score.shape, F32)
    prob[...] = jnp.zeros(prob.shape, F32)
    stat_w[...] = jnp.ones(stat_w.shape, F32)

    def window_group(n, carry):
        @pl.when(n == 2)
        def _():
            for c in round1:
                c.wait()
            merge(0, False)
            for c in round2:
                c.start()
            relay("u1")

        @pl.when(n == 6)
        def _():
            relay2("u0")

        @pl.when(n == 9)
        def _():
            relay("d0")

        @pl.when(n == fix_at - 2)
        def _():
            for c in round2:
                c.wait()
            merge(1, True)
            round3.start()

        @pl.when(n == fix_at)
        def _():
            round3.wait()
            relay("d1")
            lax.fori_loop(0, fix_at // per - 1, fix, 0)

        @pl.when(n == 28)
        def _():
            relay2("u1")

        @pl.when(n == 30)
        def _():
            relay2("d1")

        @pl.when((n > fix_at) & (lax.rem(n, per) == 0))
        def _():
            fix(n // per - 2, 0)

        new, old = jnp.minimum(n, n_groups - 1), jnp.maximum(n - 2, 0)
        j, j_old = new // per, old // per
        q_start = row_start + j * QB
        q_pos = (q_start + lax.broadcasted_iota(jnp.int32, (128, QB), 1)).astype(F32)
        slots = []
        for c in range(n_win):
            key_start = q_start - halo + 128 * c
            slots.append(jnp.where((key_start >= 0) & (key_start < rows * n_seq), c, n_win))
        units = range(GROUP)
        p = [lax.rem(new, per) * GROUP + u for u in units]
        feat = [span(p[u] * 128, 128) for u in units]
        feat_old = [span((lax.rem(old, per) * GROUP + u) * 128, 128) for u in units]
        rhs = [pair_rhs(qt[feat[u], span(j * QB, QB)]) for u in units]
        mid_top, old_inv = [stat_w[0, u] for u in units], [stat_w[1, u] for u in units]
        top, total, acc = [None] * GROUP, [None] * GROUP, [None] * GROUP

        def plus(a, b):
            return b if a is None else a + b

        for b in range(0, n_chunk, 2):
            cs = list(range(b, min(b + 2, n_chunk)))
            at = slice(128 * b, 128 * (cs[-1] + 1))
            for u in units:
                w = (prob[u, at, :].reshape(-1, 8, 2 * QB) * old_inv[u]).reshape(-1, 2 * QB).astype(BF)
                vs = [vx[feat_old[u], span((j_old + c) * 128, 128)] if c < n_win else vgt[feat_old[u], 128 * (c - n_win):128 * (c - n_win) + 128]
                      for c in cs]
                acc[u] = plus(acc[u], dot(jnp.concatenate(vs, axis=1), w))
            for u in units:
                e = jnp.exp(score[u, at, :].reshape(-1, 8, 2 * QB) - mid_top[u])
                prob[u, at, :] = e.reshape(-1, 2 * QB)
                total[u] = plus(total[u], jnp.sum(e, axis=0))
            for c in cs:
                if c >= n_win:
                    rows_g = slice(128 * (c - n_win), 128 * (c - n_win) + 128)
                    mask = jnp.where(jnp.abs(q_pos - gcol[rows_g, :]) > halo, 0.0, NEG)
                    mask = jnp.concatenate([mask, mask], axis=1)
                for u in units:
                    if c < n_win:
                        s = dot(kx[span((j + c) * 128, 128), feat[u]], rhs[u]) + bias[p[u], slots[c]]
                    else:
                        s = dot(kg[rows_g, feat[u]], rhs[u]) + mask
                    score[u, 128 * c:128 * c + 128, :] = s
                    part = jnp.max(s.reshape(16, 8, 2 * QB), axis=0)
                    top[u] = part if top[u] is None else jnp.maximum(top[u], part)
        for u in units:
            o_mine[span(j_old * QB, QB), feat_old[u]] = jnp.transpose(unpair(acc[u])).astype(BF)
            stat_w[0, u] = jnp.broadcast_to(jnp.max(top[u], axis=0, keepdims=True), (8, 2 * QB))
            stat_w[1, u] = jnp.broadcast_to(1.0 / jnp.sum(total[u], axis=0, keepdims=True), (8, 2 * QB))
        return carry

    lax.fori_loop(0, n_groups + 2, window_group, 0)
    fix(n_win_blk - 1, 0)

    for k in ("wo", "wu", "wd"):
        loads[k].wait()
    for k in parts:
        over_d[k].wait()
        if k[0] != "d":
            over_d2[k].wait()
    quarter = (rank, across, mate, lax.rem(mate + 2, n_seq))
    mb = 256

    def out_copy(i):
        at = span(i * mb, mb)
        return pltpu.make_async_copy(out_s.at[at, :], out_hbm.at[at, :], load_sem.at[len(loads) + i])

    def mlp_block(i, carry):
        o_copy(2 * i).wait_recv()
        o_copy(2 * i + 1).wait_recv()
        at = span(i * mb, mb)
        acc = x[at, :].astype(F32) + dot(o_mine[at, :], wo[...])
        for k in range(4):
            acc = acc + dot(o_peer[at, span(quarter[k] * depth, depth)], po[k])
        h = acc.astype(BF)
        acc = h.astype(F32)
        for k in (0, 1, 2, 3, 4, 6, 5, 7):
            if k == 5:
                @pl.when(i == 0)
                def _():
                    relay2("d0")
                    over_d2["d0"].wait()
                    over_d2["d1"].wait()
            cols = slice(piece * (k % 4), piece * (k % 4) + piece)
            up = wu[:, cols] if k < 4 else pu[k - 4]
            down = wd[cols, :] if k < 4 else pd[k - 4]
            act = jax.nn.gelu(dot(h, up)).astype(BF)
            acc = acc + dot(act, down)
        out_s[at, :] = acc.astype(BF)
        out_copy(i).start()
        return carry

    lax.fori_loop(0, rows // mb, mlp_block, 0)

    def drain(j, carry):
        o_copy(j).wait_send()
        return carry

    lax.fori_loop(0, n_win_blk, drain, 0)

    def flush(i, carry):
        out_copy(i).wait()
        return carry

    lax.fori_loop(0, rows // mb, flush, 0)


def solution(mesh):
    n_seq = mesh.shape["sp"]

    def local_layer(tokens, glob_pos, rel_bias, w_query, w_key, w_value, w_query_glob, w_out, w_up, w_down):
        rows, dim = tokens.shape
        heads, n_bias = rel_bias.shape
        halo = (n_bias - 1) // 2
        loc = w_query.shape[1]
        n_glob = glob_pos.shape[0]
        n_pairs = loc // 128
        n_win = 2 * halo // 128 + 1
        scale = (loc // heads) ** -0.5
        hid = w_up.shape[1]
        n_ext = rows + 2 * halo
        half = n_glob // 2
        vm = pl.BlockSpec(memory_space=pltpu.VMEM)
        hbm = pl.BlockSpec(memory_space=pl.ANY)

        def buf(*shape, dtype=BF):
            return pltpu.VMEM(shape, dtype)

        return pl.pallas_call(
            functools.partial(layer_kernel, n_seq, scale, halo),
            name="layer",
            in_specs=[hbm, vm, vm] + [hbm] * 7,
            out_specs=hbm,
            out_shape=jax.ShapeDtypeStruct((rows, dim), BF),
            scratch_shapes=[
                buf(rows, dim), buf(4, dim, loc), buf(loc, dim), buf(dim, hid), buf(hid, dim),
                buf(4, loc // n_seq, dim), buf(4, dim, hid // n_seq), buf(4, hid // n_seq, dim),
                buf(loc, rows), buf(n_ext, loc), buf(loc, n_ext), buf(n_glob, loc), buf(loc, n_glob), buf(loc, n_glob),
                buf(half, dim), buf(half, dim), buf(half, dim), buf(half, dim), buf(n_glob, dim),
                buf(loc, n_glob, dtype=F32), buf(n_pairs * 8, 2 * n_glob, dtype=F32), buf(n_pairs * 8, 2 * n_glob, dtype=F32),
                buf(2, loc // 2, n_glob, dtype=F32), buf(2, n_pairs * 4, 2 * n_glob, dtype=F32), buf(2, n_pairs * 4, 2 * n_glob, dtype=F32),
                buf(n_glob, loc),
                buf(n_pairs, n_win + 1, 128, 2 * QB, dtype=F32), buf(n_glob, QB, dtype=F32),
                buf(GROUP, n_win * 128 + n_glob, 2 * QB, dtype=F32), buf(GROUP, n_win * 128 + n_glob, 2 * QB, dtype=F32),
                buf(2, GROUP, 8, 2 * QB, dtype=F32), buf(rows, 2 * QB, dtype=F32), buf(8, 2 * QB, dtype=F32),
                buf(rows, loc), buf(rows, loc), buf(rows, dim),
                pltpu.SemaphoreType.DMA((34 + rows // QB,)), pltpu.SemaphoreType.DMA((34 + rows // QB,)),
                pltpu.SemaphoreType.DMA((32,))],
            compiler_params=pltpu.CompilerParams(vmem_limit_bytes=67043328, collective_id=0, has_side_effects=True),
        )(tokens, glob_pos[None, :], rel_bias, w_query, w_key, w_value, w_query_glob, w_out, w_up, w_down)

    row_spec = P(("batch", "sp"), None)
    col_spec = P(None, "tp")
    head_spec = P("tp", None)
    in_specs = (row_spec, P("batch"), head_spec, col_spec, col_spec, col_spec, col_spec, head_spec, col_spec, head_spec)
    return jax.shard_map(local_layer, mesh=mesh, in_specs=in_specs, out_specs=row_spec, check_vma=False)
```

```python
import functools

import jax
import jax.numpy as jnp
from jax import lax
from jax.experimental import pallas as pl
from jax.experimental.pallas import tpu as pltpu
from jax.sharding import PartitionSpec as P

BF = jnp.bfloat16
F32 = jnp.float32
NEG = float("-inf")
QB = 128
GROUP = 2
MESH = pl.DeviceIdType.MESH


def dot(a, b, dims=((1,), (0,))):
    return lax.dot_general(a, b, (dims, ((), ())), preferred_element_type=F32)


def span(start, size):
    return pl.ds(pl.multiple_of(start, size), size)


def pair_rhs(q_pair):
    half = lax.broadcasted_iota(jnp.int32, q_pair.shape, 0) < q_pair.shape[0] // 2
    zero = jnp.zeros_like(q_pair)
    return jnp.concatenate([jnp.where(half, q_pair, zero), jnp.where(half, zero, q_pair)], axis=1)


def unpair(o_two):
    n = o_two.shape[1] // 2
    half = lax.broadcasted_iota(jnp.int32, (o_two.shape[0], n), 0) < o_two.shape[0] // 2
    return jnp.where(half, o_two[:, :n], o_two[:, n:])


def spread(stat):
    n = stat.shape[1] // 2
    return jnp.concatenate([jnp.broadcast_to(stat[0:1, :n], (64, n)), jnp.broadcast_to(stat[0:1, n:], (64, n))], axis=0)


def layer_kernel(n_seq, scale, halo, x_hbm, grow, rel, wq_hbm, wk_hbm, wv_hbm, wqg_hbm, wo_hbm, wu_hbm, wd_hbm, out_ref,
                 x, w4, wo, wu, wd, po, pu, pd, qt, kx, vx, kg, vgt, qgt, x_send, x_half, x_in, x_in2, xg,
                 go, gm, gl, in_o, in_m, in_l, gfin, bias, gcol, score, prob, stat_w, gscore, stat_g, o_mine, o_peer,
                 send_sem, recv_sem, load_sem):
    rank = lax.axis_index("sp")
    peer = 1 - lax.axis_index("tp")
    core = lax.rem(rank, 2)
    mate = rank + 1 - 2 * core
    across = lax.rem(rank + 2, n_seq)
    rows, dim = x.shape
    n_glob = grow.shape[1]
    n_pairs = qt.shape[0] // 128
    loc = qt.shape[0]
    half = n_glob // 2
    row_start = rank * rows
    n_win = 2 * halo // 128 + 1
    hid = wu.shape[1]
    piece = hid // n_seq
    depth = loc // n_seq

    loads = {}

    def load(key, src, dst):
        loads[key] = pltpu.make_async_copy(src, dst, load_sem.at[len(loads)])

    for c in range(4):
        at = slice(512 * c, 512 * c + 512)
        load(("x", c), x_hbm.at[at, :], x.at[at, :])
    for c, w in enumerate((wk_hbm, wv_hbm, wq_hbm, wqg_hbm)):
        load(("w", c), w, w4.at[c])
    load("wo", wo_hbm, wo)
    load("wu", wu_hbm, wu)
    load("wd", wd_hbm, wd)
    for c in range(4):
        loads["x", c].start()
    for c in range(2):
        loads["w", c].start()
    wk, wv, wq, wqg = (w4.at[c] for c in range(4))

    barrier = pltpu.get_barrier_semaphore()
    for step in range(1, n_seq):
        pl.semaphore_signal(barrier, inc=1, device_id={"sp": lax.rem(rank + step, n_seq)}, device_id_type=MESH)
    pl.semaphore_signal(barrier, inc=1, device_id={"tp": peer}, device_id_type=MESH)
    pl.semaphore_wait(barrier, n_seq)

    used = [0]

    def copy(src, dst, sp=None):
        idx = used[0]
        used[0] += 1
        return pltpu.make_async_remote_copy(
            src_ref=src, dst_ref=dst, send_sem=send_sem.at[idx], recv_sem=recv_sem.at[idx],
            device_id={"tp": peer} if sp is None else {"sp": sp}, device_id_type=MESH)

    hp = piece // 2
    src_quarter = {
        "o": wo_hbm.at[span(rank * depth, depth), :],
        "u0": wu_hbm.at[:, span(rank * piece, hp)], "u1": wu_hbm.at[:, pl.ds(pl.multiple_of(rank * piece + hp, hp), hp)],
        "d0": wd_hbm.at[span(rank * piece, hp), :], "d1": wd_hbm.at[pl.ds(pl.multiple_of(rank * piece + hp, hp), hp), :]}

    def held(k, slot):
        if k == "o":
            return po.at[span((across if slot in (1, 3) else rank) * depth, depth), :]
        at = slice(hp * int(k[1]), hp * int(k[1]) + hp)
        return pu.at[slot, :, at] if k[0] == "u" else pd.at[slot, at, :]

    parts = tuple(src_quarter)
    over_tp = {k: copy(src_quarter[k], held(k, 0)) for k in parts}
    over_x = {k: copy(held(k, 0), held(k, 0 if k == "o" else 1), across) for k in parts if k != "d1"}
    over_d = {k: copy(held(k, 0), held(k, 0 if k == "o" else 2), mate) for k in parts}
    over_d2 = {k: copy(held(k, 1), held(k, 3), mate) for k in parts}
    over_x["d1"] = copy(wd_hbm.at[pl.ds(pl.multiple_of(across * piece + hp, hp), hp), :], held("d1", 1))
    for k in ("o", "u0", "u1"):
        over_tp[k].start()
    then = {"o": over_tp["d0"], "u0": over_tp["d1"], "u1": over_x["d1"]}

    def relay(k):
        over_tp[k].wait()
        if k in then:
            then[k].start()
        if k != "d1":
            over_x[k].start()
        over_d[k].start()

    def relay2(k):
        over_x[k].wait()
        over_d2[k].start()

    for c in range(n_glob // 128):
        at = slice(128 * c, 128 * c + 128)
        gcol[at, :] = jnp.transpose(jnp.broadcast_to(grow[:, at].astype(F32), (128, 128)))

    def picked(which, fresh):
        slots = gcol[span(which * half, half), 0:1].astype(jnp.int32) - row_start
        acc = None
        for c in range(rows // 512):
            at = lax.broadcasted_iota(jnp.int32, (half, 512), 1) + 512 * c
            hot = jnp.where(slots == at, 1.0, 0.0).astype(BF)
            if fresh:
                loads["x", c].wait()
            part = dot(hot, x[512 * c:512 * c + 512, :])
            acc = part if acc is None else acc + part
        return acc.astype(BF)

    x_send[...] = picked(1 - core, True)
    for c in range(2, 4):
        loads["w", c].start()
    first = copy(x_send, x_in, mate)
    x_half[...] = picked(core, False)
    first.start()

    def keys(c):
        kx[span(halo + c * 256, 256), :] = dot(x[span(c * 256, 256), :], wk[...]).astype(BF)

    def values(c):
        vx[:, span(halo + c * 256, 256)] = dot(wv[...], x[span(c * 256, 256), :], ((0,), (1,))).astype(BF)

    def queries(c):
        qt[:, span(c * 256, 256)] = dot(wq[...], x[span(c * 256, 256), :], ((0,), (1,))).astype(BF) * BF(scale)

    n_blk = rows // 256
    for c in range(2):
        loads["w", c].wait()
    keys(0)
    keys(n_blk - 1)
    first.wait()
    x_half[...] = x_half[...] + x_in[...]
    values(0)
    second = copy(x_half, x_in2, across)
    second.start()
    values(n_blk - 1)
    to_right = [
        copy(kx.at[pl.ds(rows, halo), :], kx.at[pl.ds(0, halo), :], rank + 1),
        copy(vx.at[:, pl.ds(rows, halo)], vx.at[:, pl.ds(0, halo)], rank + 1)]
    to_left = [
        copy(kx.at[pl.ds(halo, halo), :], kx.at[pl.ds(halo + rows, halo), :], rank - 1),
        copy(vx.at[:, pl.ds(halo, halo)], vx.at[:, pl.ds(halo + rows, halo)], rank - 1)]

    def later(c, carry):
        keys(c)
        values(c)
        return carry

    @pl.when(rank < n_seq - 1)
    def _():
        for c in to_right:
            c.start()

    @pl.when(rank > 0)
    def _():
        for c in to_left:
            c.start()

    lax.fori_loop(1, n_blk - 1, later, 0)
    for c in range(2, 4):
        loads["w", c].wait()
    for k in ("wo", "wu", "wd"):
        loads[k].start()
    lax.fori_loop(0, n_blk, lambda c, carry: (queries(c), carry)[1], 0)

    for head in range(2 * n_pairs):
        lanes = slice((head % 2) * QB, (head % 2 + 1) * QB)
        known = []
        for c in range(n_win):
            row = rel[head:head + 1, 128 * c:min(128 * c + 128, 2 * halo + 1)]
            if row.shape[1] < 128:
                at = lax.broadcasted_iota(jnp.int32, (1, 128), 1) + 128 * c
                row = jnp.where(at <= 2 * halo, jnp.broadcast_to(row[:, 0:1], (1, 128)), NEG)
            known.append(row)
        for c in range(n_win):
            before = known[c - 1] if c else jnp.full((1, 128), NEG, F32)
            both = jnp.broadcast_to(jnp.concatenate([known[c], before], axis=1), (128, 256))
            bias[head // 2, c, :, lanes] = jnp.transpose(pltpu.roll(both, 0, 1, stride=1, stride_axis=0)[:, :QB])
        bias[head // 2, n_win, :, lanes] = jnp.full((128, QB), NEG, F32)

    second.wait()
    relay("o")
    relay("u0")
    own = span(core * half, half)
    other = span((1 - core) * half, half)
    xg[own, :] = x_half[...] + x_in2[...]

    def project(at):
        kg[at, :] = dot(xg[at, :], wk[...]).astype(BF)
        vgt[:, at] = dot(wv[...], xg[at, :], ((0,), (1,))).astype(BF)

    def project_query(at):
        qgt[:, at] = dot(wqg[...], xg[at, :], ((0,), (1,))).astype(BF) * BF(scale)

    third = copy(xg.at[own, :], xg.at[own, :], mate)
    project_query(own)
    third.start()
    project(own)
    third.wait()
    project_query(other)
    project(other)

    n_tiles = n_glob // QB

    gscore[...] = jnp.zeros(gscore.shape, F32)
    stat_g[...] = jnp.zeros(stat_g.shape, F32)
    n_units = n_pairs * n_tiles

    def glob_unit(i, carry):
        @pl.when(i == 8)
        def _():
            relay2("o")

        new, old = jnp.minimum(i, n_units - 1), jnp.maximum(i - 1, 0)
        p, t = new // n_tiles, lax.rem(new, n_tiles)
        feat = span(p * 128, 128)
        p_old, t_old = old // n_tiles, lax.rem(old, n_tiles)
        feat_old = span(p_old * 128, 128)
        rhs = pair_rhs(qgt[feat, span(t * QB, QB)])
        old_top = stat_g[...]
        top, total, acc = None, None, None
        for c in range(rows // 256):
            at = slice(256 * c, 256 * c + 256)
            e = jnp.exp(gscore[at, :].reshape(32, 8, 2 * QB) - old_top)
            part = jnp.sum(e, axis=0)
            total = part if total is None else total + part
            o = dot(vx[feat_old, halo + 256 * c:halo + 256 * c + 256], e.reshape(256, 2 * QB).astype(BF))
            acc = o if acc is None else acc + o
            s = dot(kx[halo + 256 * c:halo + 256 * c + 256, feat], rhs)
            gscore[at, :] = s
            part = jnp.max(s.reshape(32, 8, 2 * QB), axis=0)
            top = part if top is None else jnp.maximum(top, part)
        go[feat_old, span(t_old * QB, QB)] = unpair(acc)
        stat = (span(p_old * 8, 8), span(t_old * 2 * QB, 2 * QB))
        gm[stat] = old_top
        gl[stat] = jnp.broadcast_to(jnp.sum(total, axis=0, keepdims=True), (8, 2 * QB))
        stat_g[...] = jnp.broadcast_to(jnp.max(top, axis=0, keepdims=True), (8, 2 * QB))
        return carry

    lax.fori_loop(0, n_units + 1, glob_unit, 0)

    o_half, s_half = loc // 2, gm.shape[0] // 2
    far_o, far_s = span((1 - core) * o_half, o_half), span((1 - core) * s_half, s_half)
    near_o, near_s = span(core * o_half, o_half), span(core * s_half, s_half)
    round1 = [copy(go.at[far_o, :], in_o.at[0], mate), copy(gm.at[far_s, :], in_m.at[0], mate), copy(gl.at[far_s, :], in_l.at[0], mate)]
    round2 = [copy(go.at[near_o, :], in_o.at[1], across), copy(gm.at[near_s, :], in_m.at[1], across), copy(gl.at[near_s, :], in_l.at[1], across)]
    round3 = copy(gfin.at[:, near_o], gfin.at[:, near_o], mate)

    def merge(k, last):
        for pp in range(n_pairs // 2):
            for t in range(n_tiles):
                lanes, at8 = slice(2 * QB * t, 2 * QB * t + 2 * QB), slice(8 * pp, 8 * pp + 8)
                stat = (span(core * s_half + 8 * pp, 8), lanes)
                top = jnp.maximum(gm[stat], in_m[k, at8, lanes])
                a, b = jnp.exp(gm[stat] - top), jnp.exp(in_m[k, at8, lanes] - top)
                tot = gl[stat] * a + in_l[k, at8, lanes] * b
                feat = span(core * o_half + 128 * pp, 128)
                cols = slice(QB * t, QB * t + QB)
                o = go[feat, cols] * spread(a) + in_o[k, 128 * pp:128 * pp + 128, cols] * spread(b)
                if last:
                    gfin[cols, feat] = jnp.transpose(o / spread(tot)).astype(BF)
                else:
                    gm[stat] = top
                    gl[stat] = tot
                    go[feat, cols] = o

    o_base = used[0]

    def o_copy(j):
        at = span(j * QB, QB)
        return pltpu.make_async_remote_copy(
            src_ref=o_mine.at[at, :], dst_ref=o_peer.at[at, :], send_sem=send_sem.at[o_base + j], recv_sem=recv_sem.at[o_base + j],
            device_id={"tp": peer}, device_id_type=MESH)

    def fix(j, carry):
        at = span(j * QB, QB)
        ids = row_start + j * QB + lax.broadcasted_iota(jnp.int32, (QB, n_glob), 0)
        hot = jnp.where(grow[...] == ids, 1.0, 0.0)
        is_glob = jnp.max(hot, axis=1, keepdims=True) > 0.0
        val = dot(hot.astype(BF), gfin[...])
        o_mine[at, :] = jnp.where(is_glob, val, o_mine[at, :].astype(F32)).astype(BF)
        o_copy(j).start()
        return carry

    for c in round1:
        c.start()

    @pl.when(rank < n_seq - 1)
    def _():
        for c in to_right:
            c.wait_send()
        for c in to_left:
            c.wait_recv()

    @pl.when(rank > 0)
    def _():
        for c in to_left:
            c.wait_send()
        for c in to_right:
            c.wait_recv()

    @pl.when(rank == 0)
    def _():
        kx[0:halo, :] = jnp.zeros((halo, loc), BF)
        vx[:, 0:halo] = jnp.zeros((loc, halo), BF)

    @pl.when(rank == n_seq - 1)
    def _():
        kx[halo + rows:, :] = jnp.zeros((halo, loc), BF)
        vx[:, halo + rows:] = jnp.zeros((loc, halo), BF)

    n_chunk = n_win + n_glob // 128
    n_win_blk = rows // QB
    per = n_pairs // GROUP
    n_groups = n_win_blk * per
    fix_at = 20
    score[...] = jnp.zeros(score.shape, F32)
    prob[...] = jnp.zeros(prob.shape, F32)
    stat_w[...] = jnp.ones(stat_w.shape, F32)

    def window_group(n, carry):
        @pl.when(n == 2)
        def _():
            for c in round1:
                c.wait()
            merge(0, False)
            for c in round2:
                c.start()
            relay("u1")

        @pl.when(n == 6)
        def _():
            relay2("u0")

        @pl.when(n == 9)
        def _():
            relay("d0")

        @pl.when(n == fix_at - 2)
        def _():
            for c in round2:
                c.wait()
            merge(1, True)
            round3.start()

        @pl.when(n == fix_at)
        def _():
            round3.wait()
            relay("d1")
            lax.fori_loop(0, fix_at // per - 1, fix, 0)

        @pl.when(n == 28)
        def _():
            relay2("u1")

        @pl.when(n == 30)
        def _():
            relay2("d1")

        @pl.when((n > fix_at) & (lax.rem(n, per) == 0))
        def _():
            fix(n // per - 2, 0)

        new, old = jnp.minimum(n, n_groups - 1), jnp.maximum(n - 2, 0)
        j, j_old = new // per, old // per
        q_start = row_start + j * QB
        q_pos = (q_start + lax.broadcasted_iota(jnp.int32, (128, QB), 1)).astype(F32)
        slots = []
        for c in range(n_win):
            key_start = q_start - halo + 128 * c
            slots.append(jnp.where((key_start >= 0) & (key_start < rows * n_seq), c, n_win))
        units = range(GROUP)
        p = [lax.rem(new, per) * GROUP + u for u in units]
        feat = [span(p[u] * 128, 128) for u in units]
        feat_old = [span((lax.rem(old, per) * GROUP + u) * 128, 128) for u in units]
        rhs = [pair_rhs(qt[feat[u], span(j * QB, QB)]) for u in units]
        mid_top, old_inv = [stat_w[0, u] for u in units], [stat_w[1, u] for u in units]
        top, total, acc = [None] * GROUP, [None] * GROUP, [None] * GROUP

        def plus(a, b):
            return b if a is None else a + b

        for b in range(0, n_chunk, 2):
            cs = list(range(b, min(b + 2, n_chunk)))
            at = slice(128 * b, 128 * (cs[-1] + 1))
            for u in units:
                w = (prob[u, at, :].reshape(-1, 8, 2 * QB) * old_inv[u]).reshape(-1, 2 * QB).astype(BF)
                vs = [vx[feat_old[u], span((j_old + c) * 128, 128)] if c < n_win else vgt[feat_old[u], 128 * (c - n_win):128 * (c - n_win) + 128]
                      for c in cs]
                acc[u] = plus(acc[u], dot(jnp.concatenate(vs, axis=1), w))
            for u in units:
                e = jnp.exp(score[u, at, :].reshape(-1, 8, 2 * QB) - mid_top[u])
                prob[u, at, :] = e.reshape(-1, 2 * QB)
                total[u] = plus(total[u], jnp.sum(e, axis=0))
            for c in cs:
                if c >= n_win:
                    rows_g = slice(128 * (c - n_win), 128 * (c - n_win) + 128)
                    mask = jnp.where(jnp.abs(q_pos - gcol[rows_g, :]) > halo, 0.0, NEG)
                    mask = jnp.concatenate([mask, mask], axis=1)
                for u in units:
                    if c < n_win:
                        s = dot(kx[span((j + c) * 128, 128), feat[u]], rhs[u]) + bias[p[u], slots[c]]
                    else:
                        s = dot(kg[rows_g, feat[u]], rhs[u]) + mask
                    score[u, 128 * c:128 * c + 128, :] = s
                    part = jnp.max(s.reshape(16, 8, 2 * QB), axis=0)
                    top[u] = part if top[u] is None else jnp.maximum(top[u], part)
        for u in units:
            o_mine[span(j_old * QB, QB), feat_old[u]] = jnp.transpose(unpair(acc[u])).astype(BF)
            stat_w[0, u] = jnp.broadcast_to(jnp.max(top[u], axis=0, keepdims=True), (8, 2 * QB))
            stat_w[1, u] = jnp.broadcast_to(1.0 / jnp.sum(total[u], axis=0, keepdims=True), (8, 2 * QB))
        return carry

    lax.fori_loop(0, n_groups + 2, window_group, 0)
    fix(n_win_blk - 1, 0)

    for k in ("wo", "wu", "wd"):
        loads[k].wait()
    for k in parts:
        over_d[k].wait()
        if k[0] != "d":
            over_d2[k].wait()
    mb = 256

    def mlp_block(i, carry):
        o_copy(2 * i).wait_recv()
        o_copy(2 * i + 1).wait_recv()
        at = span(i * mb, mb)
        acc = x[at, :].astype(F32) + dot(o_mine[at, :], wo[...])
        acc = acc + dot(o_peer[at, :], po[...])
        h = acc.astype(BF)
        acc = h.astype(F32)
        for k in (0, 1, 2, 3, 4, 6, 5, 7):
            if k == 5:
                @pl.when(i == 0)
                def _():
                    relay2("d0")
                    over_d2["d0"].wait()
                    over_d2["d1"].wait()
            cols = slice(piece * (k % 4), piece * (k % 4) + piece)
            up = wu[:, cols] if k < 4 else pu[k - 4]
            down = wd[cols, :] if k < 4 else pd[k - 4]
            act = jax.nn.gelu(dot(h, up)).astype(BF)
            acc = acc + dot(act, down)
        out_ref[at, :] = acc.astype(BF)
        return carry

    lax.fori_loop(0, rows // mb, mlp_block, 0)

    def drain(j, carry):
        o_copy(j).wait_send()
        return carry

    lax.fori_loop(0, n_win_blk, drain, 0)


def solution(mesh):
    n_seq = mesh.shape["sp"]

    def local_layer(tokens, glob_pos, rel_bias, w_query, w_key, w_value, w_query_glob, w_out, w_up, w_down):
        rows, dim = tokens.shape
        heads, n_bias = rel_bias.shape
        halo = (n_bias - 1) // 2
        loc = w_query.shape[1]
        n_glob = glob_pos.shape[0]
        n_pairs = loc // 128
        n_win = 2 * halo // 128 + 1
        scale = (loc // heads) ** -0.5
        hid = w_up.shape[1]
        n_ext = rows + 2 * halo
        half = n_glob // 2
        vm = pl.BlockSpec(memory_space=pltpu.VMEM)
        hbm = pl.BlockSpec(memory_space=pl.ANY)

        def buf(*shape, dtype=BF):
            return pltpu.VMEM(shape, dtype)

        return pl.pallas_call(
            functools.partial(layer_kernel, n_seq, scale, halo),
            name="layer",
            in_specs=[hbm, vm, vm] + [hbm] * 7,
            out_specs=vm,
            out_shape=pltpu.VMEM((rows, dim), BF),
            scratch_shapes=[
                buf(rows, dim), buf(4, dim, loc), buf(loc, dim), buf(dim, hid), buf(hid, dim),
                buf(loc, dim), buf(4, dim, hid // n_seq), buf(4, hid // n_seq, dim),
                buf(loc, rows), buf(n_ext, loc), buf(loc, n_ext), buf(n_glob, loc), buf(loc, n_glob), buf(loc, n_glob),
                buf(half, dim), buf(half, dim), buf(half, dim), buf(half, dim), buf(n_glob, dim),
                buf(loc, n_glob, dtype=F32), buf(n_pairs * 8, 2 * n_glob, dtype=F32), buf(n_pairs * 8, 2 * n_glob, dtype=F32),
                buf(2, loc // 2, n_glob, dtype=F32), buf(2, n_pairs * 4, 2 * n_glob, dtype=F32), buf(2, n_pairs * 4, 2 * n_glob, dtype=F32),
                buf(n_glob, loc),
                buf(n_pairs, n_win + 1, 128, 2 * QB, dtype=F32), buf(n_glob, QB, dtype=F32),
                buf(GROUP, n_win * 128 + n_glob, 2 * QB, dtype=F32), buf(GROUP, n_win * 128 + n_glob, 2 * QB, dtype=F32),
                buf(2, GROUP, 8, 2 * QB, dtype=F32), buf(rows, 2 * QB, dtype=F32), buf(8, 2 * QB, dtype=F32),
                buf(rows, loc), buf(rows, loc),
                pltpu.SemaphoreType.DMA((34 + rows // QB,)), pltpu.SemaphoreType.DMA((34 + rows // QB,)),
                pltpu.SemaphoreType.DMA((32,))],
            compiler_params=pltpu.CompilerParams(vmem_limit_bytes=62 * 10**6, collective_id=0, has_side_effects=True),
        )(tokens, glob_pos[None, :], rel_bias, w_query, w_key, w_value, w_query_glob, w_out, w_up, w_down)

    row_spec = P(("batch", "sp"), None)
    col_spec = P(None, "tp")
    head_spec = P("tp", None)
    in_specs = (row_spec, P("batch"), head_spec, col_spec, col_spec, col_spec, col_spec, head_spec, col_spec, head_spec)
    return jax.shard_map(local_layer, mesh=mesh, in_specs=in_specs, out_specs=row_spec, check_vma=False)
```

```python
import functools

import jax
import jax.numpy as jnp
from jax import lax
from jax.experimental import pallas as pl
from jax.experimental.pallas import tpu as pltpu
from jax.sharding import PartitionSpec as P

BF = jnp.bfloat16
F32 = jnp.float32
NEG = float("-inf")
QB = 128
GROUP = 2
LEAD = 1
MESH = pl.DeviceIdType.MESH


def dot(a, b, dims=((1,), (0,))):
    return lax.dot_general(a, b, (dims, ((), ())), preferred_element_type=F32)


def span(start, size):
    return pl.ds(pl.multiple_of(start, size), size)


def pair_rhs(q_pair):
    half = lax.broadcasted_iota(jnp.int32, q_pair.shape, 0) < q_pair.shape[0] // 2
    zero = jnp.zeros_like(q_pair)
    return jnp.concatenate([jnp.where(half, q_pair, zero), jnp.where(half, zero, q_pair)], axis=1)


def unpair(o_two):
    n = o_two.shape[1] // 2
    half = lax.broadcasted_iota(jnp.int32, (o_two.shape[0], n), 0) < o_two.shape[0] // 2
    return jnp.where(half, o_two[:, :n], o_two[:, n:])


def spread(stat):
    n = stat.shape[1] // 2
    return jnp.concatenate([jnp.broadcast_to(stat[0:1, :n], (64, n)), jnp.broadcast_to(stat[0:1, n:], (64, n))], axis=0)


def layer_kernel(n_seq, scale, halo, x_hbm, grow, rel, wq_hbm, wk_hbm, wv_hbm, wqg_hbm, wo_hbm, wu_hbm, wd_hbm, out_ref,
                 x, w4, wo, wu, wd, po, pu, pd, qt, kx, vx, kg, vgt, qgt, x_send, x_half, x_in, x_in2, xg,
                 go, gm, gl, in_o, in_m, in_l, gfin, bias, gcol, score, prob, stat_w, gscore, stat_g, o_mine, o_peer,
                 send_sem, recv_sem, load_sem):
    rank = lax.axis_index("sp")
    peer = 1 - lax.axis_index("tp")
    core = lax.rem(rank, 2)
    mate = rank + 1 - 2 * core
    across = lax.rem(rank + 2, n_seq)
    rows, dim = x.shape
    n_glob = grow.shape[1]
    n_pairs = qt.shape[0] // 128
    loc = qt.shape[0]
    half = n_glob // 2
    row_start = rank * rows
    n_win = 2 * halo // 128 + 1
    hid = wu.shape[1]
    piece = hid // n_seq
    depth = loc // n_seq

    loads = {}

    def load(key, src, dst):
        loads[key] = pltpu.make_async_copy(src, dst, load_sem.at[len(loads)])

    for c in range(4):
        at = slice(512 * c, 512 * c + 512)
        load(("x", c), x_hbm.at[at, :], x.at[at, :])
    for c, w in enumerate((wk_hbm, wv_hbm, wq_hbm, wqg_hbm)):
        load(("w", c), w, w4.at[c])
    load("wo", wo_hbm, wo)
    load("wu", wu_hbm, wu)
    load("wd", wd_hbm, wd)
    for c in range(4):
        loads["x", c].start()
    for c in range(2):
        loads["w", c].start()
    wk, wv, wq, wqg = (w4.at[c] for c in range(4))

    barrier = pltpu.get_barrier_semaphore()
    for step in range(1, n_seq):
        pl.semaphore_signal(barrier, inc=1, device_id={"sp": lax.rem(rank + step, n_seq)}, device_id_type=MESH)
    pl.semaphore_signal(barrier, inc=1, device_id={"tp": peer}, device_id_type=MESH)
    pl.semaphore_wait(barrier, n_seq)

    used = [0]

    def copy(src, dst, sp=None):
        idx = used[0]
        used[0] += 1
        return pltpu.make_async_remote_copy(
            src_ref=src, dst_ref=dst, send_sem=send_sem.at[idx], recv_sem=recv_sem.at[idx],
            device_id={"tp": peer} if sp is None else {"sp": sp}, device_id_type=MESH)

    hp = piece // 2
    src_quarter = {
        "o": wo_hbm.at[span(rank * depth, depth), :],
        "u0": wu_hbm.at[:, span(rank * piece, hp)], "u1": wu_hbm.at[:, pl.ds(pl.multiple_of(rank * piece + hp, hp), hp)],
        "d0": wd_hbm.at[span(rank * piece, hp), :], "d1": wd_hbm.at[pl.ds(pl.multiple_of(rank * piece + hp, hp), hp), :]}

    def held(k, slot):
        if k == "o":
            return po.at[span((across if slot in (1, 3) else rank) * depth, depth), :]
        at = slice(hp * int(k[1]), hp * int(k[1]) + hp)
        return pu.at[slot, :, at] if k[0] == "u" else pd.at[slot, at, :]

    parts = tuple(src_quarter)
    over_tp = {k: copy(src_quarter[k], held(k, 0)) for k in parts}
    over_x = {k: copy(held(k, 0), held(k, 0 if k == "o" else 1), across) for k in parts if k != "d1"}
    over_d = {k: copy(held(k, 0), held(k, 0 if k == "o" else 2), mate) for k in parts}
    over_d2 = {k: copy(held(k, 1), held(k, 3), mate) for k in parts}
    over_x["d1"] = copy(wd_hbm.at[pl.ds(pl.multiple_of(across * piece + hp, hp), hp), :], held("d1", 1))
    for k in ("o", "u0", "u1"):
        over_tp[k].start()
    then = {"o": over_tp["d0"], "u0": over_tp["d1"], "u1": over_x["d1"]}

    def relay(k):
        over_tp[k].wait()
        if k in then:
            then[k].start()
        if k != "d1":
            over_x[k].start()
        over_d[k].start()

    def relay2(k):
        over_x[k].wait()
        over_d2[k].start()

    for c in range(n_glob // 128):
        at = slice(128 * c, 128 * c + 128)
        gcol[at, :] = jnp.transpose(jnp.broadcast_to(grow[:, at].astype(F32), (128, 128)))

    def picked(which, fresh):
        slots = gcol[span(which * half, half), 0:1].astype(jnp.int32) - row_start
        acc = None
        for c in range(rows // 512):
            at = lax.broadcasted_iota(jnp.int32, (half, 512), 1) + 512 * c
            hot = jnp.where(slots == at, 1.0, 0.0).astype(BF)
            if fresh:
                loads["x", c].wait()
            part = dot(hot, x[512 * c:512 * c + 512, :])
            acc = part if acc is None else acc + part
        return acc.astype(BF)

    x_send[...] = picked(1 - core, True)
    for c in range(2, 4):
        loads["w", c].start()
    first = copy(x_send, x_in, mate)
    x_half[...] = picked(core, False)
    first.start()

    def keys(c):
        kx[span(halo + c * 256, 256), :] = dot(x[span(c * 256, 256), :], wk[...]).astype(BF)

    def values(c):
        vx[:, span(halo + c * 256, 256)] = dot(wv[...], x[span(c * 256, 256), :], ((0,), (1,))).astype(BF)

    def queries(c):
        qt[:, span(c * 256, 256)] = dot(wq[...], x[span(c * 256, 256), :], ((0,), (1,))).astype(BF) * BF(scale)

    n_blk = rows // 256
    for c in range(2):
        loads["w", c].wait()
    keys(0)
    keys(n_blk - 1)
    first.wait()
    x_half[...] = x_half[...] + x_in[...]
    values(0)
    second = copy(x_half, x_in2, across)
    second.start()
    values(n_blk - 1)
    to_right = [
        copy(kx.at[pl.ds(rows, halo), :], kx.at[pl.ds(0, halo), :], rank + 1),
        copy(vx.at[:, pl.ds(rows, halo)], vx.at[:, pl.ds(0, halo)], rank + 1)]
    to_left = [
        copy(kx.at[pl.ds(halo, halo), :], kx.at[pl.ds(halo + rows, halo), :], rank - 1),
        copy(vx.at[:, pl.ds(halo, halo)], vx.at[:, pl.ds(halo + rows, halo)], rank - 1)]

    def later(c, carry):
        keys(c)
        values(c)
        return carry

    @pl.when(rank < n_seq - 1)
    def _():
        for c in to_right:
            c.start()

    @pl.when(rank > 0)
    def _():
        for c in to_left:
            c.start()

    lax.fori_loop(1, n_blk - 1, later, 0)
    for c in range(2, 4):
        loads["w", c].wait()
    for k in ("wo", "wu", "wd"):
        loads[k].start()
    lax.fori_loop(0, n_blk, lambda c, carry: (queries(c), carry)[1], 0)

    for head in range(2 * n_pairs):
        lanes = slice((head % 2) * QB, (head % 2 + 1) * QB)
        known = []
        for c in range(n_win):
            row = rel[head:head + 1, 128 * c:min(128 * c + 128, 2 * halo + 1)]
            if row.shape[1] < 128:
                at = lax.broadcasted_iota(jnp.int32, (1, 128), 1) + 128 * c
                row = jnp.where(at <= 2 * halo, jnp.broadcast_to(row[:, 0:1], (1, 128)), NEG)
            known.append(row)
        for c in range(n_win):
            before = known[c - 1] if c else jnp.full((1, 128), NEG, F32)
            both = jnp.broadcast_to(jnp.concatenate([known[c], before], axis=1), (128, 256))
            bias[head // 2, c, :, lanes] = jnp.transpose(pltpu.roll(both, 0, 1, stride=1, stride_axis=0)[:, :QB])
        bias[head // 2, n_win, :, lanes] = jnp.full((128, QB), NEG, F32)

    second.wait()
    relay("o")
    relay("u0")
    own = span(core * half, half)
    other = span((1 - core) * half, half)
    xg[own, :] = x_half[...] + x_in2[...]

    def project(at):
        kg[at, :] = dot(xg[at, :], wk[...]).astype(BF)
        vgt[:, at] = dot(wv[...], xg[at, :], ((0,), (1,))).astype(BF)

    def project_query(at):
        qgt[:, at] = dot(wqg[...], xg[at, :], ((0,), (1,))).astype(BF) * BF(scale)

    third = copy(xg.at[own, :], xg.at[own, :], mate)
    project_query(own)
    third.start()
    project(own)
    third.wait()
    project_query(other)
    project(other)

    n_tiles = n_glob // QB

    gscore[...] = jnp.zeros(gscore.shape, F32)
    stat_g[...] = jnp.zeros(stat_g.shape, F32)
    n_units = n_pairs * n_tiles

    def glob_unit(i, carry):
        @pl.when(i == 8)
        def _():
            relay2("o")

        new, old = jnp.minimum(i, n_units - 1), jnp.maximum(i - 1, 0)
        p, t = new // n_tiles, lax.rem(new, n_tiles)
        feat = span(p * 128, 128)
        p_old, t_old = old // n_tiles, lax.rem(old, n_tiles)
        feat_old = span(p_old * 128, 128)
        rhs = pair_rhs(qgt[feat, span(t * QB, QB)])
        old_top = stat_g[...]
        top, total, acc = None, None, None
        for c in range(rows // 256):
            at = slice(256 * c, 256 * c + 256)
            e = jnp.exp(gscore[at, :].reshape(32, 8, 2 * QB) - old_top)
            part = jnp.sum(e, axis=0)
            total = part if total is None else total + part
            s = dot(kx[halo + 256 * c:halo + 256 * c + 256, feat], rhs)
            gscore[at, :] = s
            o = dot(vx[feat_old, halo + 256 * c:halo + 256 * c + 256], e.reshape(256, 2 * QB).astype(BF))
            acc = o if acc is None else acc + o
            part = jnp.max(s.reshape(32, 8, 2 * QB), axis=0)
            top = part if top is None else jnp.maximum(top, part)
        go[feat_old, span(t_old * QB, QB)] = unpair(acc)
        stat = (span(p_old * 8, 8), span(t_old * 2 * QB, 2 * QB))
        gm[stat] = old_top
        gl[stat] = jnp.broadcast_to(jnp.sum(total, axis=0, keepdims=True), (8, 2 * QB))
        stat_g[...] = jnp.broadcast_to(jnp.max(top, axis=0, keepdims=True), (8, 2 * QB))
        return carry

    lax.fori_loop(0, n_units + 1, glob_unit, 0)

    o_half, s_half = loc // 2, gm.shape[0] // 2
    far_o, far_s = span((1 - core) * o_half, o_half), span((1 - core) * s_half, s_half)
    near_o, near_s = span(core * o_half, o_half), span(core * s_half, s_half)
    round1 = [copy(go.at[far_o, :], in_o.at[0], mate), copy(gm.at[far_s, :], in_m.at[0], mate), copy(gl.at[far_s, :], in_l.at[0], mate)]
    round2 = [copy(go.at[near_o, :], in_o.at[1], across), copy(gm.at[near_s, :], in_m.at[1], across), copy(gl.at[near_s, :], in_l.at[1], across)]
    round3 = copy(gfin.at[:, near_o], gfin.at[:, near_o], mate)

    def merge(k, last):
        for pp in range(n_pairs // 2):
            for t in range(n_tiles):
                lanes, at8 = slice(2 * QB * t, 2 * QB * t + 2 * QB), slice(8 * pp, 8 * pp + 8)
                stat = (span(core * s_half + 8 * pp, 8), lanes)
                top = jnp.maximum(gm[stat], in_m[k, at8, lanes])
                a, b = jnp.exp(gm[stat] - top), jnp.exp(in_m[k, at8, lanes] - top)
                tot = gl[stat] * a + in_l[k, at8, lanes] * b
                feat = span(core * o_half + 128 * pp, 128)
                cols = slice(QB * t, QB * t + QB)
                o = go[feat, cols] * spread(a) + in_o[k, 128 * pp:128 * pp + 128, cols] * spread(b)
                if last:
                    gfin[cols, feat] = jnp.transpose(o / spread(tot)).astype(BF)
                else:
                    gm[stat] = top
                    gl[stat] = tot
                    go[feat, cols] = o

    o_base = used[0]

    def o_copy(j):
        at = span(j * QB, QB)
        return pltpu.make_async_remote_copy(
            src_ref=o_mine.at[at, :], dst_ref=o_peer.at[at, :], send_sem=send_sem.at[o_base + j], recv_sem=recv_sem.at[o_base + j],
            device_id={"tp": peer}, device_id_type=MESH)

    def fix(j, carry):
        at = span(j * QB, QB)
        ids = row_start + j * QB + lax.broadcasted_iota(jnp.int32, (QB, n_glob), 0)
        hot = jnp.where(grow[...] == ids, 1.0, 0.0)
        is_glob = jnp.max(hot, axis=1, keepdims=True) > 0.0
        val = dot(hot.astype(BF), gfin[...])
        o_mine[at, :] = jnp.where(is_glob, val, o_mine[at, :].astype(F32)).astype(BF)
        o_copy(j).start()
        return carry

    for c in round1:
        c.start()

    @pl.when(rank < n_seq - 1)
    def _():
        for c in to_right:
            c.wait_send()
        for c in to_left:
            c.wait_recv()

    @pl.when(rank > 0)
    def _():
        for c in to_left:
            c.wait_send()
        for c in to_right:
            c.wait_recv()

    @pl.when(rank == 0)
    def _():
        kx[0:halo, :] = jnp.zeros((halo, loc), BF)
        vx[:, 0:halo] = jnp.zeros((loc, halo), BF)

    @pl.when(rank == n_seq - 1)
    def _():
        kx[halo + rows:, :] = jnp.zeros((halo, loc), BF)
        vx[:, halo + rows:] = jnp.zeros((loc, halo), BF)

    n_chunk = n_win + n_glob // 128
    n_win_blk = rows // QB
    per = n_pairs // GROUP
    n_groups = n_win_blk * per
    fix_at = 20
    score[...] = jnp.zeros(score.shape, F32)
    prob[...] = jnp.zeros(prob.shape, F32)
    stat_w[...] = jnp.ones(stat_w.shape, F32)

    def window_group(n, carry):
        @pl.when(n == 2)
        def _():
            for c in round1:
                c.wait()
            merge(0, False)
            for c in round2:
                c.start()
            relay("u1")

        @pl.when(n == 6)
        def _():
            relay2("u0")

        @pl.when(n == 9)
        def _():
            relay("d0")

        @pl.when(n == fix_at - 2)
        def _():
            for c in round2:
                c.wait()
            merge(1, True)
            round3.start()

        @pl.when(n == fix_at)
        def _():
            round3.wait()
            relay("d1")
            lax.fori_loop(0, fix_at // per - 1, fix, 0)

        @pl.when(n == 28)
        def _():
            relay2("u1")

        @pl.when(n == 30)
        def _():
            relay2("d1")

        @pl.when((n > fix_at) & (lax.rem(n, per) == 0))
        def _():
            fix(n // per - 2, 0)

        new, old = jnp.minimum(n, n_groups - 1), jnp.maximum(n - 2, 0)
        j, j_old = new // per, old // per
        q_start = row_start + j * QB
        q_pos = (q_start + lax.broadcasted_iota(jnp.int32, (128, QB), 1)).astype(F32)
        slots = []
        for c in range(n_win):
            key_start = q_start - halo + 128 * c
            slots.append(jnp.where((key_start >= 0) & (key_start < rows * n_seq), c, n_win))
        units = range(GROUP)
        p = [lax.rem(new, per) * GROUP + u for u in units]
        feat = [span(p[u] * 128, 128) for u in units]
        feat_old = [span((lax.rem(old, per) * GROUP + u) * 128, 128) for u in units]
        rhs = [pair_rhs(qt[feat[u], span(j * QB, QB)]) for u in units]
        mid_top = [jnp.broadcast_to(jnp.max(stat_w[0, u], axis=0, keepdims=True), (8, 2 * QB)) for u in units]
        old_inv = [jnp.broadcast_to(1.0 / jnp.sum(stat_w[1, u], axis=0, keepdims=True), (8, 2 * QB)) for u in units]
        top, total, acc = [None] * GROUP, [None] * GROUP, [None] * GROUP

        def plus(a, b):
            return b if a is None else a + b

        def chunks(b):
            cs = list(range(2 * b, min(2 * b + 2, n_chunk)))
            return cs, slice(128 * cs[0], 128 * (cs[-1] + 1))

        def weigh(b):
            cs, at = chunks(b)
            for u in units:
                w = (prob[u, at, :].reshape(-1, 8, 2 * QB) * old_inv[u]).reshape(-1, 2 * QB).astype(BF)
                vs = [vx[feat_old[u], span((j_old + c) * 128, 128)] if c < n_win else vgt[feat_old[u], 128 * (c - n_win):128 * (c - n_win) + 128]
                      for c in cs]
                acc[u] = plus(acc[u], dot(jnp.concatenate(vs, axis=1), w))

        def power(b):
            cs, at = chunks(b)
            for u in units:
                e = jnp.exp(score[u, at, :].reshape(-1, 8, 2 * QB) - mid_top[u])
                prob[u, at, :] = e.reshape(-1, 2 * QB)
                total[u] = plus(total[u], jnp.sum(e, axis=0))

        def match(b):
            for c in chunks(b)[0]:
                if c >= n_win:
                    rows_g = slice(128 * (c - n_win), 128 * (c - n_win) + 128)
                    mask = jnp.where(jnp.abs(q_pos - gcol[rows_g, :]) > halo, 0.0, NEG)
                    mask = jnp.concatenate([mask, mask], axis=1)
                for u in units:
                    if c < n_win:
                        s = dot(kx[span((j + c) * 128, 128), feat[u]], rhs[u]) + bias[p[u], slots[c]]
                    else:
                        s = dot(kg[rows_g, feat[u]], rhs[u]) + mask
                    score[u, 128 * c:128 * c + 128, :] = s
                    part = jnp.max(s.reshape(16, 8, 2 * QB), axis=0)
                    top[u] = part if top[u] is None else jnp.maximum(top[u], part)

        n_b = (n_chunk + 1) // 2
        led = 0
        for b in range(n_b):
            for _ in range(LEAD):
                if led < n_b:
                    weigh(led)
                    led += 1
            power(b)
            match(b)
        for u in units:
            o_mine[span(j_old * QB, QB), feat_old[u]] = jnp.transpose(unpair(acc[u])).astype(BF)
            stat_w[0, u] = top[u]
            stat_w[1, u] = total[u]
        return carry

    lax.fori_loop(0, n_groups + 2, window_group, 0)
    fix(n_win_blk - 1, 0)

    for k in ("wo", "wu", "wd"):
        loads[k].wait()
    for k in parts:
        over_d[k].wait()
        if k[0] != "d":
            over_d2[k].wait()
    mb = 256

    def mlp_block(i, carry):
        o_copy(2 * i).wait_recv()
        o_copy(2 * i + 1).wait_recv()
        at = span(i * mb, mb)
        acc = x[at, :].astype(F32) + dot(o_mine[at, :], wo[...])
        acc = acc + dot(o_peer[at, :], po[...])
        h = acc.astype(BF)
        acc = h.astype(F32)
        order = (0, 1, 2, 3, 4, 6, 5, 7)

        def up(k):
            return dot(h, wu[:, piece * k:piece * k + piece] if k < 4 else pu[k - 4])

        def down(k, act):
            return dot(act, wd[piece * k:piece * k + piece, :] if k < 4 else pd[k - 4])

        ahead = up(order[0])
        for n, k in enumerate(order):
            now = ahead
            if n + 1 < len(order):
                ahead = up(order[n + 1])
            if k == 5:
                @pl.when(i == 0)
                def _():
                    relay2("d0")
                    over_d2["d0"].wait()
                    over_d2["d1"].wait()
            acc = acc + down(k, jax.nn.gelu(now).astype(BF))
        out_ref[at, :] = acc.astype(BF)
        return carry

    lax.fori_loop(0, rows // mb, mlp_block, 0)

    def drain(j, carry):
        o_copy(j).wait_send()
        return carry

    lax.fori_loop(0, n_win_blk, drain, 0)


def solution(mesh):
    n_seq = mesh.shape["sp"]

    def local_layer(tokens, glob_pos, rel_bias, w_query, w_key, w_value, w_query_glob, w_out, w_up, w_down):
        rows, dim = tokens.shape
        heads, n_bias = rel_bias.shape
        halo = (n_bias - 1) // 2
        loc = w_query.shape[1]
        n_glob = glob_pos.shape[0]
        n_pairs = loc // 128
        n_win = 2 * halo // 128 + 1
        scale = (loc // heads) ** -0.5
        hid = w_up.shape[1]
        n_ext = rows + 2 * halo
        half = n_glob // 2
        vm = pl.BlockSpec(memory_space=pltpu.VMEM)
        hbm = pl.BlockSpec(memory_space=pl.ANY)

        def buf(*shape, dtype=BF):
            return pltpu.VMEM(shape, dtype)

        return pl.pallas_call(
            functools.partial(layer_kernel, n_seq, scale, halo),
            name="layer",
            in_specs=[hbm, vm, vm] + [hbm] * 7,
            out_specs=vm,
            out_shape=pltpu.VMEM((rows, dim), BF),
            scratch_shapes=[
                buf(rows, dim), buf(4, dim, loc), buf(loc, dim), buf(dim, hid), buf(hid, dim),
                buf(loc, dim), buf(4, dim, hid // n_seq), buf(4, hid // n_seq, dim),
                buf(loc, rows), buf(n_ext, loc), buf(loc, n_ext), buf(n_glob, loc), buf(loc, n_glob), buf(loc, n_glob),
                buf(half, dim), buf(half, dim), buf(half, dim), buf(half, dim), buf(n_glob, dim),
                buf(loc, n_glob, dtype=F32), buf(n_pairs * 8, 2 * n_glob, dtype=F32), buf(n_pairs * 8, 2 * n_glob, dtype=F32),
                buf(2, loc // 2, n_glob, dtype=F32), buf(2, n_pairs * 4, 2 * n_glob, dtype=F32), buf(2, n_pairs * 4, 2 * n_glob, dtype=F32),
                buf(n_glob, loc),
                buf(n_pairs, n_win + 1, 128, 2 * QB, dtype=F32), buf(n_glob, QB, dtype=F32),
                buf(GROUP, n_win * 128 + n_glob, 2 * QB, dtype=F32), buf(GROUP, n_win * 128 + n_glob, 2 * QB, dtype=F32),
                buf(2, GROUP, 8, 2 * QB, dtype=F32), buf(rows, 2 * QB, dtype=F32), buf(8, 2 * QB, dtype=F32),
                buf(rows, loc), buf(rows, loc),
                pltpu.SemaphoreType.DMA((34 + rows // QB,)), pltpu.SemaphoreType.DMA((34 + rows // QB,)),
                pltpu.SemaphoreType.DMA((32,))],
            compiler_params=pltpu.CompilerParams(vmem_limit_bytes=62 * 10**6, collective_id=0, has_side_effects=True),
        )(tokens, glob_pos[None, :], rel_bias, w_query, w_key, w_value, w_query_glob, w_out, w_up, w_down)

    row_spec = P(("batch", "sp"), None)
    col_spec = P(None, "tp")
    head_spec = P("tp", None)
    in_specs = (row_spec, P("batch"), head_spec, col_spec, col_spec, col_spec, col_spec, head_spec, col_spec, head_spec)
    return jax.shard_map(local_layer, mesh=mesh, in_specs=in_specs, out_specs=row_spec, check_vma=False)
```

```python
import functools

import jax
import jax.numpy as jnp
from jax import lax
from jax.experimental import pallas as pl
from jax.experimental.pallas import tpu as pltpu
from jax.sharding import PartitionSpec as P

BF = jnp.bfloat16
F32 = jnp.float32
NEG = float("-inf")
QB = 128
GROUP = 2
LEAD = 1
MESH = pl.DeviceIdType.MESH


def dot(a, b, dims=((1,), (0,))):
    return lax.dot_general(a, b, (dims, ((), ())), preferred_element_type=F32)


def span(start, size):
    return pl.ds(pl.multiple_of(start, size), size)


def pair_rhs(q_pair):
    half = lax.broadcasted_iota(jnp.int32, q_pair.shape, 0) < q_pair.shape[0] // 2
    zero = jnp.zeros_like(q_pair)
    return jnp.concatenate([jnp.where(half, q_pair, zero), jnp.where(half, zero, q_pair)], axis=1)


def unpair(o_two):
    n = o_two.shape[1] // 2
    half = lax.broadcasted_iota(jnp.int32, (o_two.shape[0], n), 0) < o_two.shape[0] // 2
    return jnp.where(half, o_two[:, :n], o_two[:, n:])


def spread(stat):
    n = stat.shape[1] // 2
    return jnp.concatenate([jnp.broadcast_to(stat[0:1, :n], (64, n)), jnp.broadcast_to(stat[0:1, n:], (64, n))], axis=0)


def layer_kernel(n_seq, scale, halo, x_hbm, grow, rel, wq_hbm, wk_hbm, wv_hbm, wqg_hbm, wo_hbm, wu_hbm, wd_hbm, out_ref,
                 x, w4, wo, wu, wd, po, pu, pd, qt, kx, vx, kg, vgt, qgt, x_send, x_half, x_in, x_in2, xg,
                 go, gm, gl, in_o, in_m, in_l, gfin, bias, gcol, score, prob, stat_w, gscore, stat_g, o_mine, o_peer,
                 send_sem, recv_sem, load_sem):
    rank = lax.axis_index("sp")
    peer = 1 - lax.axis_index("tp")
    core = lax.rem(rank, 2)
    mate = rank + 1 - 2 * core
    across = lax.rem(rank + 2, n_seq)
    rows, dim = x.shape
    n_glob = grow.shape[1]
    n_pairs = qt.shape[0] // 128
    loc = qt.shape[0]
    half = n_glob // 2
    row_start = rank * rows
    n_win = 2 * halo // 128 + 1
    hid = wu.shape[1]
    piece = hid // n_seq
    depth = loc // n_seq

    loads = {}

    def load(key, src, dst):
        loads[key] = pltpu.make_async_copy(src, dst, load_sem.at[len(loads)])

    for c in range(4):
        at = slice(512 * c, 512 * c + 512)
        load(("x", c), x_hbm.at[at, :], x.at[at, :])
    for c, w in enumerate((wk_hbm, wv_hbm, wq_hbm, wqg_hbm)):
        load(("w", c), w, w4.at[c])
    load("wo", wo_hbm, wo)
    load("wu", wu_hbm, wu)
    load("wd", wd_hbm, wd)
    for c in range(4):
        loads["x", c].start()
    for c in range(2):
        loads["w", c].start()
    wk, wv, wq, wqg = (w4.at[c] for c in range(4))

    barrier = pltpu.get_barrier_semaphore()
    for step in range(1, n_seq):
        pl.semaphore_signal(barrier, inc=1, device_id={"sp": lax.rem(rank + step, n_seq)}, device_id_type=MESH)
    pl.semaphore_signal(barrier, inc=1, device_id={"tp": peer}, device_id_type=MESH)
    pl.semaphore_wait(barrier, n_seq)

    used = [0]

    def copy(src, dst, sp=None):
        idx = used[0]
        used[0] += 1
        return pltpu.make_async_remote_copy(
            src_ref=src, dst_ref=dst, send_sem=send_sem.at[idx], recv_sem=recv_sem.at[idx],
            device_id={"tp": peer} if sp is None else {"sp": sp}, device_id_type=MESH)

    hp = piece // 2
    src_quarter = {
        "o": wo_hbm.at[span(rank * depth, depth), :],
        "u0": wu_hbm.at[:dim // 2, span(rank * piece, piece)], "u1": wu_hbm.at[dim // 2:, span(rank * piece, piece)],
        "d0": wd_hbm.at[span(rank * piece, hp), :], "d1": wd_hbm.at[pl.ds(pl.multiple_of(rank * piece + hp, hp), hp), :]}

    def held(k, slot):
        if k == "o":
            return po.at[span((across if slot in (1, 3) else rank) * depth, depth), :]
        size = dim // 2 if k[0] == "u" else hp
        return (pu if k[0] == "u" else pd).at[slot, size * int(k[1]):size * int(k[1]) + size, :]

    parts = tuple(src_quarter)
    over_tp = {k: copy(src_quarter[k], held(k, 0)) for k in parts}
    over_x = {k: copy(held(k, 0), held(k, 0 if k == "o" else 1), across) for k in parts if k != "d1"}
    over_d = {k: copy(held(k, 0), held(k, 0 if k == "o" else 2), mate) for k in parts}
    over_d2 = {k: copy(held(k, 1), held(k, 3), mate) for k in parts}
    over_x["d1"] = copy(wd_hbm.at[pl.ds(pl.multiple_of(across * piece + hp, hp), hp), :], held("d1", 1))
    for k in ("o", "u0", "u1"):
        over_tp[k].start()
    then = {"o": over_tp["d0"], "u0": over_tp["d1"], "u1": over_x["d1"]}

    def relay(k):
        over_tp[k].wait()
        if k in then:
            then[k].start()
        if k != "d1":
            over_x[k].start()
        over_d[k].start()

    def relay2(k):
        over_x[k].wait()
        over_d2[k].start()

    for c in range(n_glob // 128):
        at = slice(128 * c, 128 * c + 128)
        gcol[at, :] = jnp.transpose(jnp.broadcast_to(grow[:, at].astype(F32), (128, 128)))

    part = half // 2

    def picked(which, piece_no, fresh=False):
        slots = gcol[span(which * half + piece_no * part, part), 0:1].astype(jnp.int32) - row_start
        acc = None
        for c in range(rows // 512):
            at = lax.broadcasted_iota(jnp.int32, (part, 512), 1) + 512 * c
            hot = jnp.where(slots == at, 1.0, 0.0).astype(BF)
            if fresh:
                loads["x", c].wait()
            got = dot(hot, x[512 * c:512 * c + 512, :])
            acc = got if acc is None else acc + got
        return acc.astype(BF)

    two = [slice(0, part), slice(part, half)]
    first = [copy(x_send.at[at, :], x_in.at[at, :], mate) for at in two]
    second = [copy(x_half.at[at, :], x_in2.at[at, :], across) for at in two]
    x_send[two[0], :] = picked(1 - core, 0, True)
    for c in range(2, 4):
        loads["w", c].start()
    x_send[two[1], :] = picked(1 - core, 1)
    first[0].start()
    x_half[two[0], :] = picked(core, 0)
    first[1].start()
    x_half[two[1], :] = picked(core, 1)

    def keys(c):
        kx[span(halo + c * 256, 256), :] = dot(x[span(c * 256, 256), :], wk[...]).astype(BF)

    def values(c):
        vx[:, span(halo + c * 256, 256)] = dot(wv[...], x[span(c * 256, 256), :], ((0,), (1,))).astype(BF)

    def queries(c):
        qt[:, span(c * 256, 256)] = dot(wq[...], x[span(c * 256, 256), :], ((0,), (1,))).astype(BF) * BF(scale)

    n_blk = rows // 256
    for c in range(2):
        loads["w", c].wait()
    first[0].wait()
    x_half[two[0], :] = x_half[two[0], :] + x_in[two[0], :]
    keys(0)
    second[0].start()
    first[1].wait()
    x_half[two[1], :] = x_half[two[1], :] + x_in[two[1], :]
    keys(n_blk - 1)
    second[1].start()
    values(0)
    values(n_blk - 1)
    to_right = [
        copy(kx.at[pl.ds(rows, halo), :], kx.at[pl.ds(0, halo), :], rank + 1),
        copy(vx.at[:, pl.ds(rows, halo)], vx.at[:, pl.ds(0, halo)], rank + 1)]
    to_left = [
        copy(kx.at[pl.ds(halo, halo), :], kx.at[pl.ds(halo + rows, halo), :], rank - 1),
        copy(vx.at[:, pl.ds(halo, halo)], vx.at[:, pl.ds(halo + rows, halo)], rank - 1)]

    def later(c, carry):
        keys(c)
        values(c)
        return carry

    @pl.when(rank < n_seq - 1)
    def _():
        for c in to_right:
            c.start()

    @pl.when(rank > 0)
    def _():
        for c in to_left:
            c.start()

    lax.fori_loop(1, n_blk - 1, later, 0)
    for c in range(2, 4):
        loads["w", c].wait()
    for k in ("wo", "wu", "wd"):
        loads[k].start()
    lax.fori_loop(0, n_blk, lambda c, carry: (queries(c), carry)[1], 0)

    for head in range(2 * n_pairs):
        lanes = slice((head % 2) * QB, (head % 2 + 1) * QB)
        known = []
        for c in range(n_win):
            row = rel[head:head + 1, 128 * c:min(128 * c + 128, 2 * halo + 1)]
            if row.shape[1] < 128:
                at = lax.broadcasted_iota(jnp.int32, (1, 128), 1) + 128 * c
                row = jnp.where(at <= 2 * halo, jnp.broadcast_to(row[:, 0:1], (1, 128)), NEG)
            known.append(row)
        for c in range(n_win):
            before = known[c - 1] if c else jnp.full((1, 128), NEG, F32)
            both = jnp.broadcast_to(jnp.concatenate([known[c], before], axis=1), (128, 256))
            bias[head // 2, c, :, lanes] = jnp.transpose(pltpu.roll(both, 0, 1, stride=1, stride_axis=0)[:, :QB])
        bias[head // 2, n_win, :, lanes] = jnp.full((128, QB), NEG, F32)

    relay("o")
    second[0].wait()
    own = span(core * half, half)
    other = span((1 - core) * half, half)
    own_two = [span(core * half + part * c, part) for c in range(2)]
    third = [copy(xg.at[at, :], xg.at[at, :], mate) for at in own_two]
    xg[own_two[0], :] = x_half[two[0], :] + x_in2[two[0], :]
    second[1].wait()
    third[0].start()
    xg[own_two[1], :] = x_half[two[1], :] + x_in2[two[1], :]
    relay("u0")

    def project(at):
        kg[at, :] = dot(xg[at, :], wk[...]).astype(BF)
        vgt[:, at] = dot(wv[...], xg[at, :], ((0,), (1,))).astype(BF)

    def project_query(at):
        qgt[:, at] = dot(wqg[...], xg[at, :], ((0,), (1,))).astype(BF) * BF(scale)

    project_query(own)
    third[1].start()
    project(own)
    third[0].wait()
    third[1].wait()
    project_query(other)
    project(other)

    n_tiles = n_glob // QB

    gscore[...] = jnp.zeros(gscore.shape, F32)
    stat_g[...] = jnp.zeros(stat_g.shape, F32)
    n_units = n_pairs * n_tiles

    def glob_unit(i, carry):
        @pl.when(i == 8)
        def _():
            relay2("o")

        new, old = jnp.minimum(i, n_units - 1), jnp.maximum(i - 1, 0)
        p, t = new // n_tiles, lax.rem(new, n_tiles)
        feat = span(p * 128, 128)
        p_old, t_old = old // n_tiles, lax.rem(old, n_tiles)
        feat_old = span(p_old * 128, 128)
        rhs = pair_rhs(qgt[feat, span(t * QB, QB)])
        old_top = stat_g[...]
        top, total, acc = None, None, None
        for c in range(rows // 256):
            at = slice(256 * c, 256 * c + 256)
            e = jnp.exp(gscore[at, :].reshape(32, 8, 2 * QB) - old_top)
            part = jnp.sum(e, axis=0)
            total = part if total is None else total + part
            s = dot(kx[halo + 256 * c:halo + 256 * c + 256, feat], rhs)
            gscore[at, :] = s
            o = dot(vx[feat_old, halo + 256 * c:halo + 256 * c + 256], e.reshape(256, 2 * QB).astype(BF))
            acc = o if acc is None else acc + o
            part = jnp.max(s.reshape(32, 8, 2 * QB), axis=0)
            top = part if top is None else jnp.maximum(top, part)
        go[feat_old, span(t_old * QB, QB)] = unpair(acc)
        stat = (span(p_old * 8, 8), span(t_old * 2 * QB, 2 * QB))
        gm[stat] = old_top
        gl[stat] = jnp.broadcast_to(jnp.sum(total, axis=0, keepdims=True), (8, 2 * QB))
        stat_g[...] = jnp.broadcast_to(jnp.max(top, axis=0, keepdims=True), (8, 2 * QB))
        return carry

    lax.fori_loop(0, n_units + 1, glob_unit, 0)

    o_half, s_half = loc // 2, gm.shape[0] // 2
    far_o, far_s = span((1 - core) * o_half, o_half), span((1 - core) * s_half, s_half)
    near_o, near_s = span(core * o_half, o_half), span(core * s_half, s_half)
    round1 = [copy(go.at[far_o, :], in_o.at[0], mate), copy(gm.at[far_s, :], in_m.at[0], mate), copy(gl.at[far_s, :], in_l.at[0], mate)]
    round2 = [copy(go.at[near_o, :], in_o.at[1], across), copy(gm.at[near_s, :], in_m.at[1], across), copy(gl.at[near_s, :], in_l.at[1], across)]
    round3 = copy(gfin.at[:, near_o], gfin.at[:, near_o], mate)

    def merge(k, last):
        for pp in range(n_pairs // 2):
            for t in range(n_tiles):
                lanes, at8 = slice(2 * QB * t, 2 * QB * t + 2 * QB), slice(8 * pp, 8 * pp + 8)
                stat = (span(core * s_half + 8 * pp, 8), lanes)
                top = jnp.maximum(gm[stat], in_m[k, at8, lanes])
                a, b = jnp.exp(gm[stat] - top), jnp.exp(in_m[k, at8, lanes] - top)
                tot = gl[stat] * a + in_l[k, at8, lanes] * b
                feat = span(core * o_half + 128 * pp, 128)
                cols = slice(QB * t, QB * t + QB)
                o = go[feat, cols] * spread(a) + in_o[k, 128 * pp:128 * pp + 128, cols] * spread(b)
                if last:
                    gfin[cols, feat] = jnp.transpose(o / spread(tot)).astype(BF)
                else:
                    gm[stat] = top
                    gl[stat] = tot
                    go[feat, cols] = o

    o_base = used[0]

    def o_copy(j):
        at = span(j * QB, QB)
        return pltpu.make_async_remote_copy(
            src_ref=o_mine.at[at, :], dst_ref=o_peer.at[at, :], send_sem=send_sem.at[o_base + j], recv_sem=recv_sem.at[o_base + j],
            device_id={"tp": peer}, device_id_type=MESH)

    def fix(j, carry):
        at = span(j * QB, QB)
        ids = row_start + j * QB + lax.broadcasted_iota(jnp.int32, (QB, n_glob), 0)
        hot = jnp.where(grow[...] == ids, 1.0, 0.0)
        is_glob = jnp.max(hot, axis=1, keepdims=True) > 0.0
        val = dot(hot.astype(BF), gfin[...])
        o_mine[at, :] = jnp.where(is_glob, val, o_mine[at, :].astype(F32)).astype(BF)
        o_copy(j).start()
        return carry

    for c in round1:
        c.start()

    @pl.when(rank < n_seq - 1)
    def _():
        for c in to_right:
            c.wait_send()
        for c in to_left:
            c.wait_recv()

    @pl.when(rank > 0)
    def _():
        for c in to_left:
            c.wait_send()
        for c in to_right:
            c.wait_recv()

    @pl.when(rank == 0)
    def _():
        kx[0:halo, :] = jnp.zeros((halo, loc), BF)
        vx[:, 0:halo] = jnp.zeros((loc, halo), BF)

    @pl.when(rank == n_seq - 1)
    def _():
        kx[halo + rows:, :] = jnp.zeros((halo, loc), BF)
        vx[:, halo + rows:] = jnp.zeros((loc, halo), BF)

    n_chunk = n_win + n_glob // 128
    n_win_blk = rows // QB
    per = n_pairs // GROUP
    n_groups = n_win_blk * per
    fix_at = 26
    score[...] = jnp.zeros(score.shape, F32)
    prob[...] = jnp.zeros(prob.shape, F32)
    stat_w[...] = jnp.ones(stat_w.shape, F32)

    def window_group(n, carry):
        @pl.when(n == 2)
        def _():
            for c in round1:
                c.wait()
            merge(0, False)
            for c in round2:
                c.start()
            relay("u1")

        @pl.when(n == 6)
        def _():
            relay2("u0")

        @pl.when(n == 9)
        def _():
            relay("d0")

        @pl.when(n == fix_at - 2)
        def _():
            for c in round2:
                c.wait()
            merge(1, True)
            round3.start()

        @pl.when(n == fix_at)
        def _():
            round3.wait()
            lax.fori_loop(0, fix_at // per - 1, fix, 0)

        @pl.when(n == 28)
        def _():
            relay2("u1")

        @pl.when(n == 18)
        def _():
            relay("d1")

        @pl.when((n > fix_at) & (lax.rem(n, per) == 0))
        def _():
            fix(n // per - 2, 0)

        new, old = jnp.minimum(n, n_groups - 1), jnp.maximum(n - 2, 0)
        j, j_old = new // per, old // per
        q_start = row_start + j * QB
        q_pos = (q_start + lax.broadcasted_iota(jnp.int32, (128, QB), 1)).astype(F32)
        slots = []
        for c in range(n_win):
            key_start = q_start - halo + 128 * c
            slots.append(jnp.where((key_start >= 0) & (key_start < rows * n_seq), c, n_win))
        units = range(GROUP)
        p = [lax.rem(new, per) * GROUP + u for u in units]
        feat = [span(p[u] * 128, 128) for u in units]
        feat_old = [span((lax.rem(old, per) * GROUP + u) * 128, 128) for u in units]
        rhs = [pair_rhs(qt[feat[u], span(j * QB, QB)]) for u in units]
        mid_top = [jnp.broadcast_to(jnp.max(stat_w[0, u], axis=0, keepdims=True), (8, 2 * QB)) for u in units]
        old_inv = [jnp.broadcast_to(1.0 / jnp.sum(stat_w[1, u], axis=0, keepdims=True), (8, 2 * QB)) for u in units]
        top, total, acc = [None] * GROUP, [None] * GROUP, [None] * GROUP

        def plus(a, b):
            return b if a is None else a + b

        def chunks(b):
            cs = list(range(2 * b, min(2 * b + 2, n_chunk)))
            return cs, slice(128 * cs[0], 128 * (cs[-1] + 1))

        def weigh(b):
            cs, at = chunks(b)
            for u in units:
                w = (prob[u, at, :].reshape(-1, 8, 2 * QB) * old_inv[u]).reshape(-1, 2 * QB).astype(BF)
                vs = [vx[feat_old[u], span((j_old + c) * 128, 128)] if c < n_win else vgt[feat_old[u], 128 * (c - n_win):128 * (c - n_win) + 128]
                      for c in cs]
                acc[u] = plus(acc[u], dot(jnp.concatenate(vs, axis=1), w))

        def power(b):
            cs, at = chunks(b)
            for u in units:
                e = jnp.exp(score[u, at, :].reshape(-1, 8, 2 * QB) - mid_top[u])
                prob[u, at, :] = e.reshape(-1, 2 * QB)
                total[u] = plus(total[u], jnp.sum(e, axis=0))

        def match(b):
            for c in chunks(b)[0]:
                if c >= n_win:
                    rows_g = slice(128 * (c - n_win), 128 * (c - n_win) + 128)
                    mask = jnp.where(jnp.abs(q_pos - gcol[rows_g, :]) > halo, 0.0, NEG)
                    mask = jnp.concatenate([mask, mask], axis=1)
                for u in units:
                    if c < n_win:
                        s = dot(kx[span((j + c) * 128, 128), feat[u]], rhs[u]) + bias[p[u], slots[c]]
                    else:
                        s = dot(kg[rows_g, feat[u]], rhs[u]) + mask
                    score[u, 128 * c:128 * c + 128, :] = s
                    part = jnp.max(s.reshape(16, 8, 2 * QB), axis=0)
                    top[u] = part if top[u] is None else jnp.maximum(top[u], part)

        n_b = (n_chunk + 1) // 2
        led = 0
        for b in range(n_b):
            for _ in range(LEAD):
                if led < n_b:
                    weigh(led)
                    led += 1
            power(b)
            match(b)
        for u in units:
            o_mine[span(j_old * QB, QB), feat_old[u]] = jnp.transpose(unpair(acc[u])).astype(BF)
            stat_w[0, u] = top[u]
            stat_w[1, u] = total[u]
        return carry

    lax.fori_loop(0, n_groups + 2, window_group, 0)
    fix(n_win_blk - 1, 0)
    relay2("d1")

    for k in ("wo", "wu", "wd"):
        loads[k].wait()
    for k in parts:
        over_d[k].wait()
        if k[0] != "d":
            over_d2[k].wait()
    mb = 256

    def mlp_block(i, carry):
        o_copy(2 * i).wait_recv()
        o_copy(2 * i + 1).wait_recv()
        at = span(i * mb, mb)
        acc = x[at, :].astype(F32) + dot(o_mine[at, :], wo[...])
        acc = acc + dot(o_peer[at, :], po[...])
        h = acc.astype(BF)
        acc = h.astype(F32)
        order = (0, 1, 2, 3, 4, 6, 5, 7)

        def up(k):
            return dot(h, wu[:, piece * k:piece * k + piece] if k < 4 else pu[k - 4])

        def down(k, act):
            return dot(act, wd[piece * k:piece * k + piece, :] if k < 4 else pd[k - 4])

        ahead = up(order[0])
        for n, k in enumerate(order):
            now = ahead
            if n + 1 < len(order):
                ahead = up(order[n + 1])
            if k == 5:
                @pl.when(i == 0)
                def _():
                    relay2("d0")
                    over_d2["d0"].wait()
                    over_d2["d1"].wait()
            acc = acc + down(k, jax.nn.gelu(now).astype(BF))
        out_ref[at, :] = acc.astype(BF)
        return carry

    lax.fori_loop(0, rows // mb, mlp_block, 0)

    def drain(j, carry):
        o_copy(j).wait_send()
        return carry

    lax.fori_loop(0, n_win_blk, drain, 0)


def solution(mesh):
    n_seq = mesh.shape["sp"]

    def local_layer(tokens, glob_pos, rel_bias, w_query, w_key, w_value, w_query_glob, w_out, w_up, w_down):
        rows, dim = tokens.shape
        heads, n_bias = rel_bias.shape
        halo = (n_bias - 1) // 2
        loc = w_query.shape[1]
        n_glob = glob_pos.shape[0]
        n_pairs = loc // 128
        n_win = 2 * halo // 128 + 1
        scale = (loc // heads) ** -0.5
        hid = w_up.shape[1]
        n_ext = rows + 2 * halo
        half = n_glob // 2
        vm = pl.BlockSpec(memory_space=pltpu.VMEM)
        hbm = pl.BlockSpec(memory_space=pl.ANY)

        def buf(*shape, dtype=BF):
            return pltpu.VMEM(shape, dtype)

        return pl.pallas_call(
            functools.partial(layer_kernel, n_seq, scale, halo),
            name="layer",
            in_specs=[hbm, vm, vm] + [hbm] * 7,
            out_specs=vm,
            out_shape=pltpu.VMEM((rows, dim), BF),
            scratch_shapes=[
                buf(rows, dim), buf(4, dim, loc), buf(loc, dim), buf(dim, hid), buf(hid, dim),
                buf(loc, dim), buf(4, dim, hid // n_seq), buf(4, hid // n_seq, dim),
                buf(loc, rows), buf(n_ext, loc), buf(loc, n_ext), buf(n_glob, loc), buf(loc, n_glob), buf(loc, n_glob),
                buf(half, dim), buf(half, dim), buf(half, dim), buf(half, dim), buf(n_glob, dim),
                buf(loc, n_glob, dtype=F32), buf(n_pairs * 8, 2 * n_glob, dtype=F32), buf(n_pairs * 8, 2 * n_glob, dtype=F32),
                buf(2, loc // 2, n_glob, dtype=F32), buf(2, n_pairs * 4, 2 * n_glob, dtype=F32), buf(2, n_pairs * 4, 2 * n_glob, dtype=F32),
                buf(n_glob, loc),
                buf(n_pairs, n_win + 1, 128, 2 * QB, dtype=F32), buf(n_glob, QB, dtype=F32),
                buf(GROUP, n_win * 128 + n_glob, 2 * QB, dtype=F32), buf(GROUP, n_win * 128 + n_glob, 2 * QB, dtype=F32),
                buf(2, GROUP, 8, 2 * QB, dtype=F32), buf(rows, 2 * QB, dtype=F32), buf(8, 2 * QB, dtype=F32),
                buf(rows, loc), buf(rows, loc),
                pltpu.SemaphoreType.DMA((37 + rows // QB,)), pltpu.SemaphoreType.DMA((37 + rows // QB,)),
                pltpu.SemaphoreType.DMA((32,))],
            compiler_params=pltpu.CompilerParams(vmem_limit_bytes=62 * 10**6, collective_id=0, has_side_effects=True),
        )(tokens, glob_pos[None, :], rel_bias, w_query, w_key, w_value, w_query_glob, w_out, w_up, w_down)

    row_spec = P(("batch", "sp"), None)
    col_spec = P(None, "tp")
    head_spec = P("tp", None)
    in_specs = (row_spec, P("batch"), head_spec, col_spec, col_spec, col_spec, col_spec, head_spec, col_spec, head_spec)
    return jax.shard_map(local_layer, mesh=mesh, in_specs=in_specs, out_specs=row_spec, check_vma=False)
```

```python
import functools

import jax
import jax.numpy as jnp
from jax import lax
from jax.experimental import pallas as pl
from jax.experimental.pallas import tpu as pltpu
from jax.sharding import PartitionSpec as P

BF = jnp.bfloat16
F32 = jnp.float32
NEG = float("-inf")
QB = 128
GROUP = 2
LEAD = 1
MESH = pl.DeviceIdType.MESH


def dot(a, b, dims=((1,), (0,))):
    return lax.dot_general(a, b, (dims, ((), ())), preferred_element_type=F32)


def span(start, size):
    return pl.ds(pl.multiple_of(start, size), size)


def pair_rhs(q_pair):
    half = lax.broadcasted_iota(jnp.int32, q_pair.shape, 0) < q_pair.shape[0] // 2
    zero = jnp.zeros_like(q_pair)
    return jnp.concatenate([jnp.where(half, q_pair, zero), jnp.where(half, zero, q_pair)], axis=1)


def unpair(o_two):
    n = o_two.shape[1] // 2
    half = lax.broadcasted_iota(jnp.int32, (o_two.shape[0], n), 0) < o_two.shape[0] // 2
    return jnp.where(half, o_two[:, :n], o_two[:, n:])


def spread(stat):
    n = stat.shape[1] // 2
    return jnp.concatenate([jnp.broadcast_to(stat[0:1, :n], (64, n)), jnp.broadcast_to(stat[0:1, n:], (64, n))], axis=0)


def layer_kernel(n_seq, scale, halo, x_hbm, grow, rel, wq_hbm, wk_hbm, wv_hbm, wqg_hbm, wo_hbm, wu_hbm, wd_hbm, out_ref,
                 x, w4, wo, wu, wd, po, pu, pd, qt, kx, vx, kg, vgt, qgt, x_send, x_half, x_in, x_in2, xg,
                 go, gm, gl, in_o, in_m, in_l, gfin, bias, gcol, pool, stat_w, stat_g, o_mine, o_peer,
                 send_sem, recv_sem, load_sem):
    rank = lax.axis_index("sp")
    peer = 1 - lax.axis_index("tp")
    core = lax.rem(rank, 2)
    mate = rank + 1 - 2 * core
    across = lax.rem(rank + 2, n_seq)
    rows, dim = x.shape
    n_glob = grow.shape[1]
    n_pairs = qt.shape[0] // 128
    loc = qt.shape[0]
    half = n_glob // 2
    row_start = rank * rows
    n_win = 2 * halo // 128 + 1
    hid = wu.shape[1]
    piece = hid // n_seq
    depth = loc // n_seq

    loads = {}

    def load(key, src, dst):
        loads[key] = pltpu.make_async_copy(src, dst, load_sem.at[len(loads)])

    for c in range(4):
        at = slice(512 * c, 512 * c + 512)
        load(("x", c), x_hbm.at[at, :], x.at[at, :])
    for c, w in enumerate((wk_hbm, wv_hbm, wq_hbm, wqg_hbm)):
        load(("w", c), w, w4.at[c])
    load("wo", wo_hbm, wo)
    load("wu", wu_hbm, wu)
    load("wd", wd_hbm, wd)
    for c in range(4):
        loads["x", c].start()
    for c in range(2):
        loads["w", c].start()
    wk, wv, wq, wqg = (w4.at[c] for c in range(4))

    barrier = pltpu.get_barrier_semaphore()
    for step in range(1, n_seq):
        pl.semaphore_signal(barrier, inc=1, device_id={"sp": lax.rem(rank + step, n_seq)}, device_id_type=MESH)
    pl.semaphore_signal(barrier, inc=1, device_id={"tp": peer}, device_id_type=MESH)
    pl.semaphore_wait(barrier, n_seq)

    used = [0]

    def copy(src, dst, sp=None):
        idx = used[0]
        used[0] += 1
        return pltpu.make_async_remote_copy(
            src_ref=src, dst_ref=dst, send_sem=send_sem.at[idx], recv_sem=recv_sem.at[idx],
            device_id={"tp": peer} if sp is None else {"sp": sp}, device_id_type=MESH)

    hp = piece // 2
    src_quarter = {
        "o": wo_hbm.at[span(rank * depth, depth), :],
        "u0": wu_hbm.at[:dim // 2, span(rank * piece, piece)], "u1": wu_hbm.at[dim // 2:, span(rank * piece, piece)],
        "d0": wd_hbm.at[span(rank * piece, hp), :], "d1": wd_hbm.at[pl.ds(pl.multiple_of(rank * piece + hp, hp), hp), :]}

    def held(k, slot):
        if k == "o":
            return po.at[span((across if slot in (1, 3) else rank) * depth, depth), :]
        size = dim // 2 if k[0] == "u" else hp
        return (pu if k[0] == "u" else pd).at[slot, size * int(k[1]):size * int(k[1]) + size, :]

    parts = tuple(src_quarter)
    over_tp = {k: copy(src_quarter[k], held(k, 0)) for k in parts}
    over_x = {k: copy(held(k, 0), held(k, 0 if k == "o" else 1), across) for k in parts}
    over_d = {k: copy(held(k, 0), held(k, 0 if k == "o" else 2), mate) for k in parts}
    over_d2 = {k: copy(held(k, 1), held(k, 3), mate) for k in parts}
    over_tp["o"].start()
    over_tp["u0"].start()

    def arrive(k):
        over_tp[k].wait()
        over_d[k].start()

    def relay2(k):
        over_x[k].wait()
        over_d2[k].start()

    for c in range(n_glob // 128):
        at = slice(128 * c, 128 * c + 128)
        gcol[at, :] = jnp.transpose(jnp.broadcast_to(grow[:, at].astype(F32), (128, 128)))

    part = half // 2

    def picked(which, piece_no, fresh=False):
        slots = gcol[span(which * half + piece_no * part, part), 0:1].astype(jnp.int32) - row_start
        acc = None
        for c in range(rows // 512):
            at = lax.broadcasted_iota(jnp.int32, (part, 512), 1) + 512 * c
            hot = jnp.where(slots == at, 1.0, 0.0).astype(BF)
            if fresh:
                loads["x", c].wait()
            got = dot(hot, x[512 * c:512 * c + 512, :])
            acc = got if acc is None else acc + got
        return acc.astype(BF)

    two = [slice(0, part), slice(part, half)]
    first = [copy(x_send.at[at, :], x_in.at[at, :], mate) for at in two]
    second = [copy(x_half.at[at, :], x_in2.at[at, :], across) for at in two]
    x_send[two[0], :] = picked(1 - core, 0, True)
    for c in range(2, 4):
        loads["w", c].start()
    x_send[two[1], :] = picked(1 - core, 1)
    first[0].start()
    x_half[two[0], :] = picked(core, 0)
    first[1].start()
    x_half[two[1], :] = picked(core, 1)

    def keys(c):
        kx[span(halo + c * 256, 256), :] = dot(x[span(c * 256, 256), :], wk[...]).astype(BF)

    def values(c):
        vx[:, span(halo + c * 256, 256)] = dot(wv[...], x[span(c * 256, 256), :], ((0,), (1,))).astype(BF)

    def queries(c):
        qt[:, span(c * 256, 256)] = dot(wq[...], x[span(c * 256, 256), :], ((0,), (1,))).astype(BF) * BF(scale)

    n_blk = rows // 256
    for c in range(2):
        loads["w", c].wait()
    first[0].wait()
    x_half[two[0], :] = x_half[two[0], :] + x_in[two[0], :]
    keys(0)
    second[0].start()
    first[1].wait()
    x_half[two[1], :] = x_half[two[1], :] + x_in[two[1], :]
    keys(n_blk - 1)
    second[1].start()
    values(0)
    values(n_blk - 1)
    to_right = [
        copy(kx.at[pl.ds(rows, halo), :], kx.at[pl.ds(0, halo), :], rank + 1),
        copy(vx.at[:, pl.ds(rows, halo)], vx.at[:, pl.ds(0, halo)], rank + 1)]
    to_left = [
        copy(kx.at[pl.ds(halo, halo), :], kx.at[pl.ds(halo + rows, halo), :], rank - 1),
        copy(vx.at[:, pl.ds(halo, halo)], vx.at[:, pl.ds(halo + rows, halo)], rank - 1)]

    def later(c, carry):
        keys(c)
        values(c)
        return carry

    lax.fori_loop(1, n_blk - 1, later, 0)
    for c in range(2, 4):
        loads["w", c].wait()
    for k in ("wo", "wu", "wd"):
        loads[k].start()
    lax.fori_loop(0, n_blk, lambda c, carry: (queries(c), carry)[1], 0)

    over_tp["u1"].start()

    for head in range(2 * n_pairs):
        lanes = slice((head % 2) * QB, (head % 2 + 1) * QB)
        known = []
        for c in range(n_win):
            row = rel[head:head + 1, 128 * c:min(128 * c + 128, 2 * halo + 1)]
            if row.shape[1] < 128:
                at = lax.broadcasted_iota(jnp.int32, (1, 128), 1) + 128 * c
                row = jnp.where(at <= 2 * halo, jnp.broadcast_to(row[:, 0:1], (1, 128)), NEG)
            known.append(row)
        for c in range(n_win):
            before = known[c - 1] if c else jnp.full((1, 128), NEG, F32)
            both = jnp.broadcast_to(jnp.concatenate([known[c], before], axis=1), (128, 256))
            bias[head // 2, c, :, lanes] = jnp.transpose(pltpu.roll(both, 0, 1, stride=1, stride_axis=0)[:, :QB])
        bias[head // 2, n_win, :, lanes] = jnp.full((128, QB), NEG, F32)

    second[0].wait()
    own = span(core * half, half)
    other = span((1 - core) * half, half)
    own_two = [span(core * half + part * c, part) for c in range(2)]
    third = [copy(xg.at[at, :], xg.at[at, :], mate) for at in own_two]
    xg[own_two[0], :] = x_half[two[0], :] + x_in2[two[0], :]
    second[1].wait()
    third[0].start()
    xg[own_two[1], :] = x_half[two[1], :] + x_in2[two[1], :]

    def project(at):
        kg[at, :] = dot(xg[at, :], wk[...]).astype(BF)
        vgt[:, at] = dot(wv[...], xg[at, :], ((0,), (1,))).astype(BF)

    def project_query(at):
        qgt[:, at] = dot(wqg[...], xg[at, :], ((0,), (1,))).astype(BF) * BF(scale)

    project_query(own)
    third[1].start()
    arrive("o")
    over_x["o"].start()

    @pl.when(rank < n_seq - 1)
    def _():
        for c in to_right:
            c.start()

    @pl.when(rank > 0)
    def _():
        for c in to_left:
            c.start()

    project(own)
    third[0].wait()
    third[1].wait()
    project_query(other)
    project(other)

    n_tiles = n_glob // QB

    wide = n_win * 128 + n_glob
    score = [pool.at[wide * u:wide * u + wide, :] for u in range(GROUP)]
    prob = [pool.at[wide * (GROUP + u):wide * (GROUP + u + 1), :] for u in range(GROUP)]
    gscore = pool.at[2 * GROUP * wide:2 * GROUP * wide + rows, :]
    gscore[...] = jnp.zeros(gscore.shape, F32)
    stat_g[...] = jnp.zeros(stat_g.shape, F32)
    n_units = n_pairs * n_tiles

    def glob_unit(i, carry):
        @pl.when(i == 3)
        def _():
            arrive("u0")
            over_tp["d0"].start()

        new, old = jnp.minimum(i, n_units - 1), jnp.maximum(i - 1, 0)
        p, t = new // n_tiles, lax.rem(new, n_tiles)
        feat = span(p * 128, 128)
        p_old, t_old = old // n_tiles, lax.rem(old, n_tiles)
        feat_old = span(p_old * 128, 128)
        rhs = pair_rhs(qgt[feat, span(t * QB, QB)])
        old_top = stat_g[...]
        top, total, acc = None, None, None
        for c in range(rows // 256):
            at = slice(256 * c, 256 * c + 256)
            e = jnp.exp(gscore[at, :].reshape(32, 8, 2 * QB) - old_top)
            part = jnp.sum(e, axis=0)
            total = part if total is None else total + part
            s = dot(kx[halo + 256 * c:halo + 256 * c + 256, feat], rhs)
            gscore[at, :] = s
            o = dot(vx[feat_old, halo + 256 * c:halo + 256 * c + 256], e.reshape(256, 2 * QB).astype(BF))
            acc = o if acc is None else acc + o
            part = jnp.max(s.reshape(32, 8, 2 * QB), axis=0)
            top = part if top is None else jnp.maximum(top, part)
        go[feat_old, span(t_old * QB, QB)] = unpair(acc)
        stat = (span(p_old * 8, 8), span(t_old * 2 * QB, 2 * QB))
        gm[stat] = old_top
        gl[stat] = jnp.broadcast_to(jnp.sum(total, axis=0, keepdims=True), (8, 2 * QB))
        stat_g[...] = jnp.broadcast_to(jnp.max(top, axis=0, keepdims=True), (8, 2 * QB))
        return carry

    lax.fori_loop(0, n_units + 1, glob_unit, 0)

    o_half, s_half = loc // 2, gm.shape[0] // 2
    far_o, far_s = span((1 - core) * o_half, o_half), span((1 - core) * s_half, s_half)
    near_o, near_s = span(core * o_half, o_half), span(core * s_half, s_half)
    round1 = [copy(go.at[far_o, :], in_o.at[0], mate), copy(gm.at[far_s, :], in_m.at[0], mate), copy(gl.at[far_s, :], in_l.at[0], mate)]
    round2 = [copy(go.at[near_o, :], in_o.at[1], across), copy(gm.at[near_s, :], in_m.at[1], across), copy(gl.at[near_s, :], in_l.at[1], across)]
    round3 = copy(gfin.at[:, near_o], gfin.at[:, near_o], mate)

    def merge(k, last):
        for pp in range(n_pairs // 2):
            for t in range(n_tiles):
                lanes, at8 = slice(2 * QB * t, 2 * QB * t + 2 * QB), slice(8 * pp, 8 * pp + 8)
                stat = (span(core * s_half + 8 * pp, 8), lanes)
                top = jnp.maximum(gm[stat], in_m[k, at8, lanes])
                a, b = jnp.exp(gm[stat] - top), jnp.exp(in_m[k, at8, lanes] - top)
                tot = gl[stat] * a + in_l[k, at8, lanes] * b
                feat = span(core * o_half + 128 * pp, 128)
                cols = slice(QB * t, QB * t + QB)
                o = go[feat, cols] * spread(a) + in_o[k, 128 * pp:128 * pp + 128, cols] * spread(b)
                if last:
                    gfin[cols, feat] = jnp.transpose(o / spread(tot)).astype(BF)
                else:
                    gm[stat] = top
                    gl[stat] = tot
                    go[feat, cols] = o

    o_base = used[0]

    def o_copy(j):
        at = span(j * QB, QB)
        return pltpu.make_async_remote_copy(
            src_ref=o_mine.at[at, :], dst_ref=o_peer.at[at, :], send_sem=send_sem.at[o_base + j], recv_sem=recv_sem.at[o_base + j],
            device_id={"tp": peer}, device_id_type=MESH)

    def fix(j, carry):
        at = span(j * QB, QB)
        ids = row_start + j * QB + lax.broadcasted_iota(jnp.int32, (QB, n_glob), 0)
        hot = jnp.where(grow[...] == ids, 1.0, 0.0)
        is_glob = jnp.max(hot, axis=1, keepdims=True) > 0.0
        val = dot(hot.astype(BF), gfin[...])
        o_mine[at, :] = jnp.where(is_glob, val, o_mine[at, :].astype(F32)).astype(BF)
        o_copy(j).start()
        return carry

    for c in round1:
        c.start()

    @pl.when(rank < n_seq - 1)
    def _():
        for c in to_right:
            c.wait_send()
        for c in to_left:
            c.wait_recv()

    @pl.when(rank > 0)
    def _():
        for c in to_left:
            c.wait_send()
        for c in to_right:
            c.wait_recv()

    @pl.when(rank == 0)
    def _():
        kx[0:halo, :] = jnp.zeros((halo, loc), BF)
        vx[:, 0:halo] = jnp.zeros((loc, halo), BF)

    @pl.when(rank == n_seq - 1)
    def _():
        kx[halo + rows:, :] = jnp.zeros((halo, loc), BF)
        vx[:, halo + rows:] = jnp.zeros((loc, halo), BF)

    n_chunk = n_win + n_glob // 128
    n_win_blk = rows // QB
    per = n_pairs // GROUP
    n_groups = n_win_blk * per
    fix_at = 18
    for r in score + prob:
        r[...] = jnp.zeros(r.shape, F32)
    stat_w[...] = jnp.ones(stat_w.shape, F32)

    def window_group(n, carry):
        @pl.when(n == 2)
        def _():
            for c in round1:
                c.wait()
            merge(0, False)
            for c in round2:
                c.start()

        @pl.when(n == 4)
        def _():
            arrive("u1")
            over_tp["d1"].start()
            relay2("o")

        @pl.when(n == 30)
        def _():
            over_x["u1"].start()

        @pl.when(n == fix_at - 2)
        def _():
            for c in round2:
                c.wait()
            merge(1, True)
            round3.start()
            over_x["u0"].start()
            arrive("d0")

        @pl.when(n == fix_at)
        def _():
            round3.wait()
            lax.fori_loop(0, fix_at // per - 1, fix, 0)

        @pl.when((n > fix_at) & (lax.rem(n, per) == 0))
        def _():
            fix(n // per - 2, 0)

        new, old = jnp.minimum(n, n_groups - 1), jnp.maximum(n - 2, 0)
        j, j_old = new // per, old // per
        q_start = row_start + j * QB
        q_pos = (q_start + lax.broadcasted_iota(jnp.int32, (128, QB), 1)).astype(F32)
        slots = []
        for c in range(n_win):
            key_start = q_start - halo + 128 * c
            slots.append(jnp.where((key_start >= 0) & (key_start < rows * n_seq), c, n_win))
        units = range(GROUP)
        p = [lax.rem(new, per) * GROUP + u for u in units]
        feat = [span(p[u] * 128, 128) for u in units]
        feat_old = [span((lax.rem(old, per) * GROUP + u) * 128, 128) for u in units]
        rhs = [pair_rhs(qt[feat[u], span(j * QB, QB)]) for u in units]
        mid_top = [jnp.broadcast_to(jnp.max(stat_w[0, u], axis=0, keepdims=True), (8, 2 * QB)) for u in units]
        old_inv = [jnp.broadcast_to(1.0 / jnp.sum(stat_w[1, u], axis=0, keepdims=True), (8, 2 * QB)) for u in units]
        top, total, acc = [None] * GROUP, [None] * GROUP, [None] * GROUP

        def plus(a, b):
            return b if a is None else a + b

        def chunks(b):
            cs = list(range(2 * b, min(2 * b + 2, n_chunk)))
            return cs, slice(128 * cs[0], 128 * (cs[-1] + 1))

        def weigh(b):
            cs, at = chunks(b)
            for u in units:
                w = (prob[u][at, :].reshape(-1, 8, 2 * QB) * old_inv[u]).reshape(-1, 2 * QB).astype(BF)
                vs = [vx[feat_old[u], span((j_old + c) * 128, 128)] if c < n_win else vgt[feat_old[u], 128 * (c - n_win):128 * (c - n_win) + 128]
                      for c in cs]
                acc[u] = plus(acc[u], dot(jnp.concatenate(vs, axis=1), w))

        def power(b):
            cs, at = chunks(b)
            for u in units:
                e = jnp.exp(score[u][at, :].reshape(-1, 8, 2 * QB) - mid_top[u])
                prob[u][at, :] = e.reshape(-1, 2 * QB)
                total[u] = plus(total[u], jnp.sum(e, axis=0))

        def match(b):
            for c in chunks(b)[0]:
                if c >= n_win:
                    rows_g = slice(128 * (c - n_win), 128 * (c - n_win) + 128)
                    mask = jnp.where(jnp.abs(q_pos - gcol[rows_g, :]) > halo, 0.0, NEG)
                    mask = jnp.concatenate([mask, mask], axis=1)
                for u in units:
                    if c < n_win:
                        s = dot(kx[span((j + c) * 128, 128), feat[u]], rhs[u]) + bias[p[u], slots[c]]
                    else:
                        s = dot(kg[rows_g, feat[u]], rhs[u]) + mask
                    score[u][128 * c:128 * c + 128, :] = s
                    part = jnp.max(s.reshape(16, 8, 2 * QB), axis=0)
                    top[u] = part if top[u] is None else jnp.maximum(top[u], part)

        n_b = (n_chunk + 1) // 2
        led = 0
        for b in range(n_b):
            for _ in range(LEAD):
                if led < n_b:
                    weigh(led)
                    led += 1
            power(b)
            match(b)
        for u in units:
            o_mine[span(j_old * QB, QB), feat_old[u]] = jnp.transpose(unpair(acc[u])).astype(BF)
            stat_w[0, u] = top[u]
            stat_w[1, u] = total[u]
        return carry

    lax.fori_loop(0, n_groups + 2, window_group, 0)
    fix(n_win_blk - 1, 0)
    relay2("u0")
    arrive("d1")

    for k in ("wo", "wu", "wd"):
        loads[k].wait()
    for k in parts:
        over_d[k].wait()
    over_d2["o"].wait()
    mb = 256
    n_mb = rows // mb

    def products(h, acc, order):
        def up(k):
            return dot(h, wu[:, piece * k:piece * k + piece] if k < 4 else pu[k - 4])

        def down(k, act):
            return dot(act, wd[piece * k:piece * k + piece, :] if k < 4 else pd[k - 4])

        ahead = up(order[0])
        for n, k in enumerate(order):
            now = ahead
            if n + 1 < len(order):
                ahead = up(order[n + 1])
            acc = acc + down(k, jax.nn.gelu(now).astype(BF))
        return acc

    def mlp_near(i, carry):
        @pl.when(i == 1)
        def _():
            over_x["d0"].start()

        @pl.when(i == 2)
        def _():
            relay2("u1")

        @pl.when(i == 3)
        def _():
            over_x["d1"].start()

        @pl.when(i == 4)
        def _():
            relay2("d0")

        o_copy(2 * i).wait_recv()
        o_copy(2 * i + 1).wait_recv()
        at = span(i * mb, mb)
        acc = x[at, :].astype(F32) + dot(o_mine[at, :], wo[...])
        acc = acc + dot(o_peer[at, :], po[...])
        h = acc.astype(BF)
        x[at, :] = h
        acc = products(h, h.astype(F32), (0, 1, 2, 3, 4, 6))
        for c in range(dim // 256):
            pool[span(c * rows + i * mb, mb), :] = acc[:, 256 * c:256 * c + 256]
        return carry

    def mlp_far(i, carry):
        at = span(i * mb, mb)
        acc = jnp.concatenate([pool[span(c * rows + i * mb, mb), :] for c in range(dim // 256)], axis=1)
        out_ref[at, :] = products(x[at, :], acc, (5, 7)).astype(BF)
        return carry

    lax.fori_loop(0, n_mb - 2, mlp_near, 0)
    relay2("d1")
    for k in ("u0", "u1", "d0", "d1"):
        over_d2[k].wait()
    lax.fori_loop(0, n_mb - 2, mlp_far, 0)
    lax.fori_loop(n_mb - 2, n_mb, mlp_near, 0)
    lax.fori_loop(n_mb - 2, n_mb, mlp_far, 0)

    def drain(j, carry):
        o_copy(j).wait_send()
        return carry

    lax.fori_loop(0, n_win_blk, drain, 0)


def solution(mesh):
    n_seq = mesh.shape["sp"]

    def local_layer(tokens, glob_pos, rel_bias, w_query, w_key, w_value, w_query_glob, w_out, w_up, w_down):
        rows, dim = tokens.shape
        heads, n_bias = rel_bias.shape
        halo = (n_bias - 1) // 2
        loc = w_query.shape[1]
        n_glob = glob_pos.shape[0]
        n_pairs = loc // 128
        n_win = 2 * halo // 128 + 1
        scale = (loc // heads) ** -0.5
        hid = w_up.shape[1]
        n_ext = rows + 2 * halo
        half = n_glob // 2
        vm = pl.BlockSpec(memory_space=pltpu.VMEM)
        hbm = pl.BlockSpec(memory_space=pl.ANY)

        def buf(*shape, dtype=BF):
            return pltpu.VMEM(shape, dtype)

        return pl.pallas_call(
            functools.partial(layer_kernel, n_seq, scale, halo),
            name="layer",
            in_specs=[hbm, vm, vm] + [hbm] * 7,
            out_specs=vm,
            out_shape=pltpu.VMEM((rows, dim), BF),
            scratch_shapes=[
                buf(rows, dim), buf(4, dim, loc), buf(loc, dim), buf(dim, hid), buf(hid, dim),
                buf(loc, dim), buf(4, dim, hid // n_seq), buf(4, hid // n_seq, dim),
                buf(loc, rows), buf(n_ext, loc), buf(loc, n_ext), buf(n_glob, loc), buf(loc, n_glob), buf(loc, n_glob),
                buf(half, dim), buf(half, dim), buf(half, dim), buf(half, dim), buf(n_glob, dim),
                buf(loc, n_glob, dtype=F32), buf(n_pairs * 8, 2 * n_glob, dtype=F32), buf(n_pairs * 8, 2 * n_glob, dtype=F32),
                buf(2, loc // 2, n_glob, dtype=F32), buf(2, n_pairs * 4, 2 * n_glob, dtype=F32), buf(2, n_pairs * 4, 2 * n_glob, dtype=F32),
                buf(n_glob, loc),
                buf(n_pairs, n_win + 1, 128, 2 * QB, dtype=F32), buf(n_glob, QB, dtype=F32),
                buf(rows * (dim // 256), 256, dtype=F32), buf(2, GROUP, 8, 2 * QB, dtype=F32), buf(8, 2 * QB, dtype=F32),
                buf(rows, loc), buf(rows, loc),
                pltpu.SemaphoreType.DMA((37 + rows // QB,)), pltpu.SemaphoreType.DMA((37 + rows // QB,)),
                pltpu.SemaphoreType.DMA((32,))],
            compiler_params=pltpu.CompilerParams(vmem_limit_bytes=627 * 10**5, collective_id=0, has_side_effects=True),
        )(tokens, glob_pos[None, :], rel_bias, w_query, w_key, w_value, w_query_glob, w_out, w_up, w_down)

    row_spec = P(("batch", "sp"), None)
    col_spec = P(None, "tp")
    head_spec = P("tp", None)
    in_specs = (row_spec, P("batch"), head_spec, col_spec, col_spec, col_spec, col_spec, head_spec, col_spec, head_spec)
    return jax.shard_map(local_layer, mesh=mesh, in_specs=in_specs, out_specs=row_spec, check_vma=False)
```
